8 devices in a mesh: dp: 2 (over z, y), sp: 4 (over x, core).
Axes of the slice: x: 2, y: 2, z: 1, core: 2. Of those that a mesh axis runs over, the one named last changes fastest.
Arguments:
- hidden: bfloat16 [8192, 2048], P(('dp', 'sp')), parts along dimension 0
- grad_out: bfloat16 [8192, 2048], P(('dp', 'sp')), parts along dimension 0
- positions: int32 [8192], P(('dp', 'sp')), parts along dimension 0
- doc_ids: int32 [8192], P(('dp', 'sp')), parts along dimension 0
- w_q: bfloat16 [2048, 2048], replicated
- w_k: bfloat16 [2048, 256], replicated
- w_v: bfloat16 [2048, 256], replicated
- w_o: bfloat16 [2048, 2048], replicated
Outputs:
- output 1: bfloat16 [8192, 2048], P(('dp', 'sp')), parts along dimension 0
- output 2: bfloat16 [8192, 2048], P(('dp', 'sp')), parts along dimension 0
- output 3: float32 [4096, 2048], P('dp'), parts along dimension 0
- output 4: float32 [4096, 256], P('dp'), parts along dimension 0
- output 5: float32 [4096, 256], P('dp'), parts along dimension 0
- output 6: float32 [4096, 2048], P('dp'), parts along dimension 0
There are 2 independent parts. The reference program is written for one: setup_inputs(seed, part) draws one part's arguments, and reference() takes and returns one part's arrays. A program takes and returns all parts, laid end to end along the dimension named above; an argument that names none is the same for every part.
All inputs are finite; a program needn't handle non-finite values.
Results may differ from the reference program's by a relative error of at most 0.0116802.
Values are sent between devices in bfloat16 or wider.
A program may use at most 1 GiB of HBM per device.

```python
import jax
import jax.numpy as jnp
from jax import lax

D = 2048
HEADS = 16
KV_HEADS = 2
HEAD = 128
SEQ = 4096

ROPE_THETA = 500000.0
ROPE_FACTOR = 8.0
ROPE_LOW = 1.0
ROPE_HIGH = 4.0
ROPE_OLD_CTX = 8192.0
SCORE_LIMIT = 32 * 1024 * 1024
NEG_BIG = -1.0e30


def draw_layout(layout_key):
    cut_key, start_key = jax.random.split(layout_key)
    cut_points = jnp.sort(jax.random.randint(cut_key, (2,), SEQ // 8, SEQ - SEQ // 8))
    token_idx = jnp.arange(SEQ, dtype=jnp.int32)
    doc_ids = jnp.sum(token_idx[:, None] >= cut_points[None, :], axis=1).astype(jnp.int32)
    bounds = jnp.concatenate([jnp.zeros((1,), jnp.int32), cut_points.astype(jnp.int32)])
    starts = jax.random.randint(start_key, (3,), 0, SEQ)
    positions = (starts[doc_ids] + token_idx - bounds[doc_ids]).astype(jnp.int32)
    return positions, doc_ids


def setup_inputs(seed: int = 0, part: int = 0) -> dict:
    part_key = jax.random.fold_in(jax.random.key(seed), part)
    hid_key, grad_key, layout_key = jax.random.split(part_key, 3)
    weight_keys = jax.random.split(jax.random.key(seed + 1), 4)
    hidden = jax.random.normal(hid_key, (SEQ, D), jnp.float32).astype(jnp.bfloat16)
    grad_out = jax.random.normal(grad_key, (SEQ, D), jnp.float32).astype(jnp.bfloat16)
    positions, doc_ids = draw_layout(layout_key)
    in_scale = D ** -0.5
    w_q = (jax.random.normal(weight_keys[0], (D, HEADS * HEAD), jnp.float32) * in_scale).astype(jnp.bfloat16)
    w_k = (jax.random.normal(weight_keys[1], (D, KV_HEADS * HEAD), jnp.float32) * in_scale).astype(jnp.bfloat16)
    w_v = (jax.random.normal(weight_keys[2], (D, KV_HEADS * HEAD), jnp.float32) * in_scale).astype(jnp.bfloat16)
    w_o = (jax.random.normal(weight_keys[3], (HEADS * HEAD, D), jnp.float32) * (HEADS * HEAD) ** -0.5).astype(jnp.bfloat16)
    return {"hidden": hidden, "grad_out": grad_out, "positions": positions, "doc_ids": doc_ids, "w_q": w_q, "w_k": w_k, "w_v": w_v, "w_o": w_o}


def rope_freqs():
    half_idx = jnp.arange(HEAD // 2, dtype=jnp.float32)
    inv_freq = jnp.power(ROPE_THETA, -2.0 * half_idx / HEAD)
    wavelen = 2.0 * jnp.pi / inv_freq
    smooth = (ROPE_OLD_CTX / wavelen - ROPE_LOW) / (ROPE_HIGH - ROPE_LOW)
    mixed_freq = (1.0 - smooth) * inv_freq / ROPE_FACTOR + smooth * inv_freq
    scaled = jnp.where(wavelen > ROPE_OLD_CTX / ROPE_LOW, inv_freq / ROPE_FACTOR, mixed_freq)
    return jnp.where(wavelen < ROPE_OLD_CTX / ROPE_HIGH, inv_freq, scaled)


def rope_tables(pos_vec):
    angles = pos_vec.astype(jnp.float32)[:, None] * rope_freqs()[None, :]
    return jnp.cos(angles)[:, None, :], jnp.sin(angles)[:, None, :]


def rotate(values, cos_tab, sin_tab):
    half_dim = values.shape[-1] // 2
    first_half = values[..., :half_dim]
    second_half = values[..., half_dim:]
    return jnp.concatenate([first_half * cos_tab - second_half * sin_tab, second_half * cos_tab + first_half * sin_tab], axis=-1)


def block_rows(n_query, head_count, n_keys):
    block_len = n_query
    while block_len % 16 == 0 and head_count * block_len * n_keys > SCORE_LIMIT:
        block_len = block_len // 2
    return block_len


def block_probs(q_blk, k_all, pos_blk, doc_blk, pos_all, doc_all):
    scores = jnp.einsum("qhgd,shd->hgqs", q_blk, k_all) * HEAD ** -0.5
    allowed = (pos_all[None, :] <= pos_blk[:, None]) & (doc_all[None, :] == doc_blk[:, None])
    scores = jnp.where(allowed, scores, NEG_BIG)
    row_peak = jnp.max(scores, axis=-1, keepdims=True)
    exp_vals = jnp.exp(scores - row_peak)
    return exp_vals / jnp.sum(exp_vals, axis=-1, keepdims=True)


def reference(hidden, grad_out, positions, doc_ids, w_q, w_k, w_v, w_o):
    group_size = HEADS // KV_HEADS
    score_scale = HEAD ** -0.5
    cos_tab, sin_tab = rope_tables(positions)
    q_pre = jnp.dot(hidden, w_q, preferred_element_type=jnp.float32).reshape(SEQ, HEADS, HEAD)
    k_pre = jnp.dot(hidden, w_k, preferred_element_type=jnp.float32).reshape(SEQ, KV_HEADS, HEAD)
    v_pre = jnp.dot(hidden, w_v, preferred_element_type=jnp.float32).reshape(SEQ, KV_HEADS, HEAD)
    q_rot = rotate(q_pre, cos_tab, sin_tab).astype(jnp.bfloat16).astype(jnp.float32)
    k_rot = rotate(k_pre, cos_tab, sin_tab).astype(jnp.bfloat16).astype(jnp.float32)
    v_val = v_pre.astype(jnp.bfloat16).astype(jnp.float32)
    block_len = block_rows(SEQ, HEADS, SEQ)
    n_blocks = SEQ // block_len
    q_blocks = q_rot.reshape(n_blocks, block_len, KV_HEADS, group_size, HEAD)
    pos_blocks = positions.reshape(n_blocks, block_len)
    doc_blocks = doc_ids.reshape(n_blocks, block_len)

    def fwd_block(block_in):
        q_blk, pos_blk, doc_blk = block_in
        prob_f32 = block_probs(q_blk, k_rot, pos_blk, doc_blk, positions, doc_ids)
        prob_bf = prob_f32.astype(jnp.bfloat16).astype(jnp.float32)
        return jnp.einsum("hgqs,shd->qhgd", prob_bf, v_val).astype(jnp.bfloat16)

    context = lax.map(fwd_block, (q_blocks, pos_blocks, doc_blocks)).reshape(SEQ, HEADS * HEAD)
    attn_out = jnp.dot(context, w_o, preferred_element_type=jnp.float32).astype(jnp.bfloat16)

    d_ctx = jnp.dot(grad_out, w_o.T, preferred_element_type=jnp.float32).astype(jnp.bfloat16)
    grad_wo = jnp.dot(context.T, grad_out, preferred_element_type=jnp.float32)
    d_ctx_blocks = d_ctx.astype(jnp.float32).reshape(n_blocks, block_len, KV_HEADS, group_size, HEAD)

    def bwd_block(acc_pair, block_in):
        dk_acc, dv_acc = acc_pair
        q_blk, dctx_blk, pos_blk, doc_blk = block_in
        prob_f32 = block_probs(q_blk, k_rot, pos_blk, doc_blk, positions, doc_ids)
        prob_bf = prob_f32.astype(jnp.bfloat16).astype(jnp.float32)
        d_prob = jnp.einsum("qhgd,shd->hgqs", dctx_blk, v_val)
        row_dot = jnp.sum(prob_f32 * d_prob, axis=-1, keepdims=True)
        d_score = (prob_f32 * (d_prob - row_dot) * score_scale).astype(jnp.bfloat16).astype(jnp.float32)
        dq_blk = jnp.einsum("hgqs,shd->qhgd", d_score, k_rot).astype(jnp.bfloat16)
        dk_acc = dk_acc + jnp.einsum("hgqs,qhgd->shd", d_score, q_blk)
        dv_acc = dv_acc + jnp.einsum("hgqs,qhgd->shd", prob_bf, dctx_blk)
        return (dk_acc, dv_acc), dq_blk

    zero_acc = jnp.zeros((SEQ, KV_HEADS, HEAD), jnp.float32)
    (dk_acc, dv_acc), dq_blocks = lax.scan(bwd_block, (zero_acc, zero_acc), (q_blocks, d_ctx_blocks, pos_blocks, doc_blocks))
    dq_rot = dq_blocks.reshape(SEQ, HEADS, HEAD).astype(jnp.float32)
    dq_pre = rotate(dq_rot, cos_tab, -sin_tab).astype(jnp.bfloat16).reshape(SEQ, HEADS * HEAD)
    dk_rot = dk_acc.astype(jnp.bfloat16).astype(jnp.float32)
    dk_pre = rotate(dk_rot, cos_tab, -sin_tab).astype(jnp.bfloat16).reshape(SEQ, KV_HEADS * HEAD)
    dv_pre = dv_acc.astype(jnp.bfloat16).reshape(SEQ, KV_HEADS * HEAD)
    grad_hidden = (jnp.dot(dq_pre, w_q.T, preferred_element_type=jnp.float32) + jnp.dot(dk_pre, w_k.T, preferred_element_type=jnp.float32) + jnp.dot(dv_pre, w_v.T, preferred_element_type=jnp.float32)).astype(jnp.bfloat16)
    grad_wq = jnp.dot(hidden.T, dq_pre, preferred_element_type=jnp.float32)
    grad_wk = jnp.dot(hidden.T, dk_pre, preferred_element_type=jnp.float32)
    grad_wv = jnp.dot(hidden.T, dv_pre, preferred_element_type=jnp.float32)
    return attn_out, grad_hidden, grad_wq, grad_wk, grad_wv, grad_wo
```

```python
import functools

import jax
import jax.numpy as jnp
from jax import lax
from jax.experimental import pallas as pl
from jax.experimental.pallas import tpu as pltpu
from jax.sharding import PartitionSpec as P

HEAD = 128
ROPE_THETA = 500000.0
ROPE_FACTOR = 8.0
ROPE_LOW = 1.0
ROPE_HIGH = 4.0
ROPE_OLD_CTX = 8192.0
NEG_BIG = -1.0e30
SCALE = HEAD ** -0.5
LOG2E = 1.4426950408889634

PAIR = 2
WIDE = PAIR * HEAD
BQ = 256
BK = 512
ALIGN = 128
BF = jnp.bfloat16
F32 = jnp.float32


def rope_freqs():
    half_idx = jnp.arange(HEAD // 2, dtype=F32)
    inv_freq = jnp.power(ROPE_THETA, -2.0 * half_idx / HEAD)
    wavelen = 2.0 * jnp.pi / inv_freq
    smooth = (ROPE_OLD_CTX / wavelen - ROPE_LOW) / (ROPE_HIGH - ROPE_LOW)
    mixed_freq = (1.0 - smooth) * inv_freq / ROPE_FACTOR + smooth * inv_freq
    scaled = jnp.where(wavelen > ROPE_OLD_CTX / ROPE_LOW, inv_freq / ROPE_FACTOR, mixed_freq)
    return jnp.where(wavelen < ROPE_OLD_CTX / ROPE_HIGH, inv_freq, scaled)


def rope_tables(pos_vec):
    angles = pos_vec.astype(F32)[:, None] * rope_freqs()[None, :]
    cos_half, sin_half = jnp.cos(angles), jnp.sin(angles)
    return jnp.concatenate([cos_half, cos_half], axis=-1), jnp.concatenate([-sin_half, sin_half], axis=-1)


def dot_nn(a, b):
    return lax.dot_general(a, b, (((1,), (0,)), ((), ())), preferred_element_type=F32)


def dot_nt(a, b):
    return lax.dot_general(a, b, (((1,), (1,)), ((), ())), preferred_element_type=F32)


def swap_halves(v):
    return pltpu.roll(v, HEAD // 2, 1)


def cost(flops, nbytes, trans=0):
    return pl.CostEstimate(flops=int(flops), bytes_accessed=int(nbytes), transcendentals=int(trans))


def params(**kw):
    return pltpu.CompilerParams(vmem_limit_bytes=60 * 1024 * 1024, **kw)


def kv_kernel(s_ref, x_ref, wk_ref, wv_ref, cos_ref, sin_ref, *rest):
    out_ref = rest[-1]
    x = x_ref[...]
    k = dot_nn(x, wk_ref[...])
    k = k * cos_ref[...] + swap_halves(k) * sin_ref[...]
    out_ref[:, :HEAD] = k.astype(BF)
    out_ref[:, HEAD:] = dot_nn(x, wv_ref[...]).astype(BF)


def kv_proj(sel, x, w_k, w_v, cos_t, sin_t, prev):
    tokens, width = x.shape
    half = tokens // 2
    extra = [] if prev is None else [prev]
    return pl.pallas_call(
        kv_kernel,
        grid_spec=pltpu.PrefetchScalarGridSpec(
            num_scalar_prefetch=1,
            grid=(2,),
            in_specs=[
                pl.BlockSpec((half, width), lambda m, s: (m, 0)),
                pl.BlockSpec((width, HEAD), lambda m, s: (0, s[0])),
                pl.BlockSpec((width, HEAD), lambda m, s: (0, s[0])),
                pl.BlockSpec((half, HEAD), lambda m, s: (s[1] * 2 + m, 0)),
                pl.BlockSpec((half, HEAD), lambda m, s: (s[1] * 2 + m, 0)),
            ] + [pl.BlockSpec(memory_space=pl.ANY)] * len(extra),
            out_specs=pl.BlockSpec((half, 2 * HEAD), lambda m, s: (s[1] * 2 + m, 0)),
        ),
        out_shape=jax.ShapeDtypeStruct((2 * tokens, 2 * HEAD), BF),
        input_output_aliases={} if prev is None else {6: 0},
        compiler_params=params(),
        cost_estimate=cost(2 * tokens * width * 2 * HEAD, tokens * width * 2),
        name="kv_proj",
    )(sel, x, w_k, w_v, cos_t, sin_t, *extra)


def q_kernel(s_ref, x_ref, wq_ref, cos_ref, sin_ref, *rest):
    out_ref = rest[-1]
    q = dot_nn(x_ref[...], wq_ref[...])
    for h in range(PAIR):
        part = q[:, h * HEAD:(h + 1) * HEAD]
        out_ref[:, h * HEAD:(h + 1) * HEAD] = (part * cos_ref[...] + swap_halves(part) * sin_ref[...]).astype(BF)


def q_proj(sel, x, w_q, cos_t, sin_t, prev):
    tokens, width = x.shape
    cols = w_q.shape[1] // 2
    n = cols // WIDE
    extra = [] if prev is None else [prev]
    return pl.pallas_call(
        q_kernel,
        grid_spec=pltpu.PrefetchScalarGridSpec(
            num_scalar_prefetch=1,
            grid=(n,),
            in_specs=[
                pl.BlockSpec((tokens, width), lambda j, s: (0, 0)),
                pl.BlockSpec((width, WIDE), lambda j, s: (0, s[0] * n + j)),
                pl.BlockSpec((tokens, HEAD), lambda j, s: (s[1], 0)),
                pl.BlockSpec((tokens, HEAD), lambda j, s: (s[1], 0)),
            ] + [pl.BlockSpec(memory_space=pl.ANY)] * len(extra),
            out_specs=pl.BlockSpec((tokens, WIDE), lambda j, s: (s[1], j)),
        ),
        out_shape=jax.ShapeDtypeStruct((2 * tokens, cols), BF),
        input_output_aliases={} if prev is None else {5: 0},
        compiler_params=params(),
        cost_estimate=cost(2 * tokens * width * cols, tokens * width * 2 + cols * width * 2),
        name="q_proj",
    )(sel, x, w_q, cos_t, sin_t, *extra)


def dctx_kernel(s_ref, g_ref, wo_ref, *rest):
    out_ref = rest[-1]
    out_ref[...] = dot_nt(g_ref[...], wo_ref[...]).astype(BF)


def dctx_proj(sel, g, w_o, prev):
    tokens, width = g.shape
    cols = w_o.shape[0] // 2
    n = cols // WIDE
    extra = [] if prev is None else [prev]
    return pl.pallas_call(
        dctx_kernel,
        grid_spec=pltpu.PrefetchScalarGridSpec(
            num_scalar_prefetch=1,
            grid=(n,),
            in_specs=[
                pl.BlockSpec((tokens, width), lambda j, s: (0, 0)),
                pl.BlockSpec((WIDE, width), lambda j, s: (s[0] * n + j, 0)),
            ] + [pl.BlockSpec(memory_space=pl.ANY)] * len(extra),
            out_specs=pl.BlockSpec((tokens, WIDE), lambda j, s: (s[1], j)),
        ),
        out_shape=jax.ShapeDtypeStruct((2 * tokens, cols), BF),
        input_output_aliases={} if prev is None else {3: 0},
        compiler_params=params(),
        cost_estimate=cost(2 * tokens * width * cols, tokens * width * 2 + cols * width * 2),
        name="dctx_proj",
    )(sel, g, w_o, *extra)


def flip_kernel(x_ref, out_ref):
    out_ref[...] = x_ref[...].T


def flip(x):
    rows, cols = x.shape
    step = 512
    return pl.pallas_call(
        flip_kernel,
        grid=(cols // step,),
        in_specs=[pl.BlockSpec((rows, step), lambda n: (0, n))],
        out_specs=pl.BlockSpec((step, rows), lambda n: (n, 0)),
        out_shape=jax.ShapeDtypeStruct((cols, rows), x.dtype),
        compiler_params=params(),
        cost_estimate=cost(rows * cols * 512, rows * cols * 4),
        name="flip",
    )(x)


def attn_kernel(first, lo_ref, nb_ref, q_ref, do_ref, qdoc_ref, kdoc_ref, cos_ref, sin_ref, kvp_ref, kvc_ref, *rest):
    if first:
        act_ref, ctxt_ref, dk_ref, dv_ref = rest[:4]
        scratch = rest[4:]
    else:
        dk_in, dv_in, act_ref, ctxt_ref, dk_ref, dv_ref = rest[:6]
        scratch = rest[6:]
    k_s, v_s, s_s, dp_s, m_s, l_s, d_s, qd_s, ctx_s, dq_s, q_s, do_s, qt_s, dot_s = scratch
    i = pl.program_id(0)
    chip_len = kvc_ref.shape[0]

    @pl.when(i == 0)
    def _():
        k_s[:chip_len, :] = kvp_ref[:, :HEAD]
        v_s[:chip_len, :] = kvp_ref[:, HEAD:]
        k_s[chip_len:2 * chip_len, :] = kvc_ref[:, :HEAD]
        v_s[chip_len:2 * chip_len, :] = kvc_ref[:, HEAD:]
        k_s[2 * chip_len:, :] = jnp.zeros((BK, HEAD), BF)
        v_s[2 * chip_len:, :] = jnp.zeros((BK, HEAD), BF)
        if first:
            dk_ref[...] = jnp.zeros_like(dk_ref)
            dv_ref[...] = jnp.zeros_like(dv_ref)
        else:
            dk_ref[...] = dk_in[...]
            dv_ref[...] = dv_in[...]

    for h in range(PAIR):
        rows = slice(h * BQ, (h + 1) * BQ)
        cols = slice(h * HEAD, (h + 1) * HEAD)
        q_s[rows, :] = q_ref[:, cols]
        do_s[rows, :] = do_ref[:, cols]
        qt_s[:, rows] = q_ref[:, cols].T
        dot_s[:, rows] = do_ref[:, cols].T
    qd_s[...] = jnp.broadcast_to(qdoc_ref[...], (BQ, HEAD))
    m_s[...] = jnp.full(m_s.shape, NEG_BIG, F32)
    l_s[...] = jnp.zeros(l_s.shape, F32)
    d_s[...] = jnp.zeros(d_s.shape, F32)
    ctx_s[...] = jnp.zeros(ctx_s.shape, F32)
    dq_s[...] = jnp.zeros(dq_s.shape, F32)
    lo = lo_ref[i]
    n_blocks = nb_ref[i]
    lanes = BK // HEAD

    def fold(v, op):
        out = v[:, :HEAD]
        for n in range(1, lanes):
            out = op(out, v[:, n * HEAD:(n + 1) * HEAD])
        return out

    def spread(v):
        return jnp.concatenate([v] * lanes, axis=1)

    def offset(b):
        return pl.multiple_of(lo + b * BK, ALIGN)

    def scores(b, carry):
        off = offset(b)
        s = dot_nt(q_s[...], k_s[pl.ds(off, BK), :])
        key = off + lax.broadcasted_iota(jnp.int32, (BQ, BK), 1)
        query = chip_len + i * BQ + lax.broadcasted_iota(jnp.int32, (BQ, BK), 0)
        keep = (key <= query) & (kdoc_ref[:, pl.ds(off, BK)] == spread(qd_s[...]))
        for h in range(PAIR):
            rows = slice(h * BQ, (h + 1) * BQ)
            sh = jnp.where(keep, s[rows, :], NEG_BIG)
            s_s[b, rows, :] = sh
            m_s[rows, :] = jnp.maximum(m_s[rows, :], fold(sh, jnp.maximum))
        return carry

    lax.fori_loop(0, n_blocks, scores, 0)
    m_s[...] = jnp.broadcast_to(jnp.max(m_s[...], axis=1, keepdims=True), m_s.shape)

    def weights(b, carry):
        dp = dot_nt(do_s[...], v_s[pl.ds(offset(b), BK), :])
        e = jnp.exp2((s_s[b] - spread(m_s[...])) * (SCALE * LOG2E))
        s_s[b] = e
        dp_s[b] = dp
        l_s[...] += fold(e, jnp.add)
        d_s[...] += fold(e * dp, jnp.add)
        return carry

    lax.fori_loop(0, n_blocks, weights, 0)
    inv = 1.0 / jnp.sum(l_s[...], axis=1, keepdims=True)
    delta = jnp.sum(d_s[...], axis=1, keepdims=True) * inv
    l_s[...] = jnp.broadcast_to(inv, l_s.shape)
    d_s[...] = jnp.broadcast_to(delta, d_s.shape)

    def grads(b, carry):
        off = offset(b)
        p = s_s[b] * spread(l_s[...])
        pb = p.astype(BF)
        ds = (p * (dp_s[b] - spread(d_s[...])) * SCALE).astype(BF)
        ctx_s[...] += dot_nn(pb, v_s[pl.ds(off, BK), :])
        dq_s[...] += dot_nn(ds, k_s[pl.ds(off, BK), :])
        dv_ref[:, pl.ds(off, BK)] += dot_nn(dot_s[...], pb)
        dk_ref[:, pl.ds(off, BK)] += dot_nn(qt_s[...], ds)
        return carry

    lax.fori_loop(0, n_blocks, grads, 0)
    for h in range(PAIR):
        rows = slice(h * BQ, (h + 1) * BQ)
        cols = slice(h * HEAD, (h + 1) * HEAD)
        ctx = ctx_s[rows, :].astype(BF)
        act_ref[0, :, cols] = ctx
        ctxt_ref[cols, :] = ctx.T
        dq = dq_s[rows, :].astype(BF).astype(F32)
        act_ref[1, :, cols] = (dq * cos_ref[...] - swap_halves(dq) * sin_ref[...]).astype(BF)


def attention(chunk, lo, n_blocks, q, dctx, qdoc, kdoc, cos_t, sin_t, kv_prev, kv_chip, acc):
    chip_len = q.shape[0]
    padded = 2 * chip_len + BK
    max_blocks = 2 * chip_len // BK + 1
    rows = PAIR * BQ
    first = acc is None
    full = lambda shape: pl.BlockSpec(shape, lambda i, *s: (0,) * len(shape))
    acc_shape = jax.ShapeDtypeStruct((HEAD, padded), F32)
    pairs = chip_len * chip_len * PAIR
    return pl.pallas_call(
        functools.partial(attn_kernel, first),
        grid_spec=pltpu.PrefetchScalarGridSpec(
            num_scalar_prefetch=2,
            grid=(chip_len // BQ,),
            in_specs=[
                pl.BlockSpec((BQ, WIDE), lambda i, *s: (i, chunk)),
                pl.BlockSpec((BQ, WIDE), lambda i, *s: (i, chunk)),
                pl.BlockSpec((BQ, 1), lambda i, *s: (i, 0)),
                full((1, padded)),
                pl.BlockSpec((BQ, HEAD), lambda i, *s: (i, 0)),
                pl.BlockSpec((BQ, HEAD), lambda i, *s: (i, 0)),
                full((chip_len, 2 * HEAD)),
                full((chip_len, 2 * HEAD)),
            ] + ([] if first else [full((HEAD, padded))] * 2),
            out_specs=[
                pl.BlockSpec((2, BQ, WIDE), lambda i, *s: (0, i, 0)),
                pl.BlockSpec((WIDE, BQ), lambda i, *s: (0, i)),
                full((HEAD, padded)),
                full((HEAD, padded)),
            ],
            scratch_shapes=[
                pltpu.VMEM((padded, HEAD), BF),
                pltpu.VMEM((padded, HEAD), BF),
                pltpu.VMEM((max_blocks, rows, BK), F32),
                pltpu.VMEM((max_blocks, rows, BK), F32),
                pltpu.VMEM((rows, HEAD), F32),
                pltpu.VMEM((rows, HEAD), F32),
                pltpu.VMEM((rows, HEAD), F32),
                pltpu.VMEM((BQ, HEAD), jnp.int32),
                pltpu.VMEM((rows, HEAD), F32),
                pltpu.VMEM((rows, HEAD), F32),
                pltpu.VMEM((rows, HEAD), BF),
                pltpu.VMEM((rows, HEAD), BF),
                pltpu.VMEM((HEAD, rows), BF),
                pltpu.VMEM((HEAD, rows), BF),
            ],
        ),
        out_shape=[
            jax.ShapeDtypeStruct((2, chip_len, WIDE), BF),
            jax.ShapeDtypeStruct((WIDE, chip_len), BF),
            acc_shape,
            acc_shape,
        ],
        input_output_aliases={} if first else {10: 2, 11: 3},
        compiler_params=params(),
        cost_estimate=cost(pairs * HEAD * 2 * 6, 12 * 1024 * 1024, pairs),
        name="attention",
    )(lo, n_blocks, q, dctx, qdoc, kdoc, cos_t, sin_t, kv_prev, kv_chip, *([] if first else acc))


def kv_finish_kernel(dk_ref, dv_ref, far_ref, cos_ref, sin_ref, out_ref):
    dk = (dk_ref[...] + far_ref[0].astype(F32)).astype(BF).astype(F32).T
    dv = (dv_ref[...] + far_ref[1].astype(F32)).T
    out_ref[:, :HEAD] = (dk * cos_ref[...] - swap_halves(dk) * sin_ref[...]).astype(BF)
    out_ref[:, HEAD:] = dv.astype(BF)


def kv_finish(dk, dv, far, cos_t, sin_t):
    chip_len = cos_t.shape[0]
    step = 512
    skip = chip_len // step
    return pl.pallas_call(
        kv_finish_kernel,
        grid=(chip_len // step,),
        in_specs=[
            pl.BlockSpec((HEAD, step), lambda t: (0, skip + t)),
            pl.BlockSpec((HEAD, step), lambda t: (0, skip + t)),
            pl.BlockSpec((2, HEAD, step), lambda t: (0, 0, t)),
            pl.BlockSpec((step, HEAD), lambda t: (t, 0)),
            pl.BlockSpec((step, HEAD), lambda t: (t, 0)),
        ],
        out_specs=pl.BlockSpec((step, 2 * HEAD), lambda t: (t, 0)),
        out_shape=jax.ShapeDtypeStruct((chip_len, 2 * HEAD), BF),
        compiler_params=params(),
        cost_estimate=cost(chip_len * HEAD * 64, chip_len * HEAD * 16),
        name="kv_finish",
    )(dk, dv, far, cos_t, sin_t)


def wgrad_kernel(s_ref, xt_own, xt_oth, act_ref, g_own, g_oth, ctxt_ref, out_ref):
    tokens = xt_own.shape[1]
    own = pl.ds(pl.multiple_of(s_ref[0] * tokens, tokens), tokens)
    oth = pl.ds(pl.multiple_of((1 - s_ref[0]) * tokens, tokens), tokens)
    out_ref[0] = (dot_nn(xt_own[...], act_ref[0, own, :]) + dot_nn(xt_oth[...], act_ref[0, oth, :])).astype(BF)
    gwo = (dot_nn(ctxt_ref[:, own], g_own[...]) + dot_nn(ctxt_ref[:, oth], g_oth[...])).astype(BF)
    for n in range(gwo.shape[1] // WIDE):
        out_ref[1, n * WIDE:(n + 1) * WIDE, :] = gwo[:, n * WIDE:(n + 1) * WIDE]


def wgrad(core, xt_own, xt_oth, act, g_own, g_oth, ctxt):
    width, tokens = xt_own.shape
    step = 512
    return pl.pallas_call(
        wgrad_kernel,
        grid_spec=pltpu.PrefetchScalarGridSpec(
            num_scalar_prefetch=1,
            grid=(width // step,),
            in_specs=[
                pl.BlockSpec((step, tokens), lambda n, s: (n, 0)),
                pl.BlockSpec((step, tokens), lambda n, s: (n, 0)),
                pl.BlockSpec((1, 2 * tokens, WIDE), lambda n, s: (1, 0, 0)),
                pl.BlockSpec((tokens, step), lambda n, s: (0, n)),
                pl.BlockSpec((tokens, step), lambda n, s: (0, n)),
                pl.BlockSpec((WIDE, 2 * tokens), lambda n, s: (0, 0)),
            ],
            out_specs=pl.BlockSpec((2, step, WIDE), lambda n, s: (0, n, 0)),
        ),
        out_shape=jax.ShapeDtypeStruct((2, width, WIDE), BF),
        compiler_params=params(),
        cost_estimate=cost(8 * tokens * width * WIDE, 8 * tokens * width),
        name="wgrad",
    )(core, xt_own, xt_oth, act, g_own, g_oth, ctxt)


def kvgrad_kernel(s_ref, xt_own, xt_oth, dkv_ref, out_ref):
    tokens = xt_own.shape[1]
    own = pl.ds(pl.multiple_of(s_ref[0] * tokens, tokens), tokens)
    oth = pl.ds(pl.multiple_of((1 - s_ref[0]) * tokens, tokens), tokens)
    out_ref[...] = (dot_nn(xt_own[...], dkv_ref[own, :]) + dot_nn(xt_oth[...], dkv_ref[oth, :])).astype(BF)


def kvgrad(core, xt_own, xt_oth, dkv):
    width, tokens = xt_own.shape
    step = 512
    return pl.pallas_call(
        kvgrad_kernel,
        grid_spec=pltpu.PrefetchScalarGridSpec(
            num_scalar_prefetch=1,
            grid=(width // step,),
            in_specs=[
                pl.BlockSpec((step, tokens), lambda n, s: (n, 0)),
                pl.BlockSpec((step, tokens), lambda n, s: (n, 0)),
                pl.BlockSpec((2 * tokens, 2 * HEAD), lambda n, s: (0, 0)),
            ],
            out_specs=pl.BlockSpec((step, 2 * HEAD), lambda n, s: (n, 0)),
        ),
        out_shape=jax.ShapeDtypeStruct((width, 2 * HEAD), BF),
        compiler_params=params(),
        cost_estimate=cost(4 * tokens * width * 2 * HEAD, 4 * tokens * width),
        name="kvgrad",
    )(core, xt_own, xt_oth, dkv)


def combine_kernel(s_ref, a_ref, b_ref, c_ref, d_ref, *rest):
    gq_ref, go_ref = rest[-2:]

    def put(u_ref, v_ref):
        gq_ref[...] = u_ref[0].astype(F32) + v_ref[0].astype(F32)
        for n in range(u_ref.shape[1] // WIDE):
            rows = slice(n * WIDE, (n + 1) * WIDE)
            go_ref[:, rows] = u_ref[1, rows, :].astype(F32) + v_ref[1, rows, :].astype(F32)

    @pl.when(pl.program_id(0) == 0)
    def _():
        put(a_ref, b_ref)

    @pl.when(pl.program_id(0) == 1)
    def _():
        put(c_ref, d_ref)


def combine(core, chunk, n_chunks, parts, prev):
    width = parts[0].shape[1]
    step = 512
    last = width // step - 1
    near = pl.BlockSpec((2, step, WIDE), lambda w, r, s: (0, r + w * (last - r), 0))
    far = pl.BlockSpec((2, step, WIDE), lambda w, r, s: (0, r * w, 0))

    def place(w, s):
        return (s[0] + w - 2 * s[0] * w) * n_chunks + chunk

    shape = jax.ShapeDtypeStruct((width, 2 * n_chunks * WIDE), F32)
    shape_o = jax.ShapeDtypeStruct((2 * n_chunks * WIDE, width), F32)
    extra = [] if prev is None else list(prev)
    return pl.pallas_call(
        combine_kernel,
        grid_spec=pltpu.PrefetchScalarGridSpec(
            num_scalar_prefetch=1,
            grid=(2, width // step),
            in_specs=[near, near, far, far] + [pl.BlockSpec(memory_space=pl.ANY)] * len(extra),
            out_specs=[
                pl.BlockSpec((step, WIDE), lambda w, r, s: (r, place(w, s))),
                pl.BlockSpec((WIDE, step), lambda w, r, s: (place(w, s), r)),
            ],
        ),
        out_shape=[shape, shape_o],
        input_output_aliases={} if prev is None else {5: 0, 6: 1},
        compiler_params=params(),
        cost_estimate=cost(16 * width * WIDE * 64, 32 * width * WIDE),
        name="combine",
    )(core, *parts, *extra)


def fill_heads(core, own_refs, oth_refs, lhs):
    n = len(own_refs)
    for j in range(n):
        lhs[:, pl.ds(pl.multiple_of((core * n + j) * WIDE, WIDE), WIDE)] = own_refs[j][0]
        lhs[:, pl.ds(pl.multiple_of(((1 - core) * n + j) * WIDE, WIDE), WIDE)] = oth_refs[j][0]


def attn_out_kernel(n, s_ref, *refs):
    own_refs, oth_refs = refs[:n], refs[n:2 * n]
    wo_ref, out_ref, lhs = refs[2 * n:]

    @pl.when(pl.program_id(0) == 0)
    def _():
        fill_heads(s_ref[0], own_refs, oth_refs, lhs)

    out_ref[...] = dot_nn(lhs[...], wo_ref[...]).astype(BF)


def attn_out(core, own, oth, w_o):
    n = len(own)
    tokens = own[0].shape[1] // 2
    heads, width = w_o.shape
    step = 512
    return pl.pallas_call(
        functools.partial(attn_out_kernel, n),
        grid_spec=pltpu.PrefetchScalarGridSpec(
            num_scalar_prefetch=1,
            grid=(width // step,),
            in_specs=[pl.BlockSpec((1, tokens, WIDE), lambda k, s: (0, s[0], 0))] * (2 * n)
            + [pl.BlockSpec((heads, step), lambda k, s: (0, k))],
            out_specs=pl.BlockSpec((tokens, step), lambda k, s: (0, k)),
            scratch_shapes=[pltpu.VMEM((tokens, heads), BF)],
        ),
        out_shape=jax.ShapeDtypeStruct((tokens, width), BF),
        compiler_params=params(),
        cost_estimate=cost(2 * tokens * heads * width, 2 * heads * width + 4 * tokens * width),
        name="attn_out",
    )(core, *own, *oth, w_o)


def hidden_kernel(n, s_ref, *refs):
    own_refs, oth_refs = refs[:n], refs[n:2 * n]
    kv_own, kv_oth, wq_ref, wk_ref, wv_ref, out_ref, lhs, klhs, vlhs = refs[2 * n:]
    core = s_ref[0]

    @pl.when(pl.program_id(0) == 0)
    def _():
        fill_heads(core, own_refs, oth_refs, lhs)
        for place, ref in ((core, kv_own), (1 - core, kv_oth)):
            where = pl.ds(pl.multiple_of(place * HEAD, HEAD), HEAD)
            klhs[:, where] = ref[:, :HEAD]
            vlhs[:, where] = ref[:, HEAD:]

    out_ref[...] = (
        dot_nt(lhs[...], wq_ref[...]) + dot_nt(klhs[...], wk_ref[...]) + dot_nt(vlhs[...], wv_ref[...])
    ).astype(BF)


def grad_hidden(core, own, oth, kv_own, kv_oth, w_q, w_k, w_v):
    n = len(own)
    tokens = own[0].shape[1] // 2
    width, heads = w_q.shape
    kv_cols = w_k.shape[1]
    step = 512
    return pl.pallas_call(
        functools.partial(hidden_kernel, n),
        grid_spec=pltpu.PrefetchScalarGridSpec(
            num_scalar_prefetch=1,
            grid=(width // step,),
            in_specs=[pl.BlockSpec((1, tokens, WIDE), lambda k, s: (1, s[0], 0))] * (2 * n)
            + [pl.BlockSpec((tokens, 2 * HEAD), lambda k, s: (s[0], 0))] * 2
            + [
                pl.BlockSpec((step, heads), lambda k, s: (k, 0)),
                pl.BlockSpec((step, kv_cols), lambda k, s: (k, 0)),
                pl.BlockSpec((step, kv_cols), lambda k, s: (k, 0)),
            ],
            out_specs=pl.BlockSpec((tokens, step), lambda k, s: (0, k)),
            scratch_shapes=[
                pltpu.VMEM((tokens, heads), BF),
                pltpu.VMEM((tokens, kv_cols), BF),
                pltpu.VMEM((tokens, kv_cols), BF),
            ],
        ),
        out_shape=jax.ShapeDtypeStruct((tokens, width), BF),
        compiler_params=params(),
        cost_estimate=cost(2 * tokens * (heads + 2 * kv_cols) * width, 2 * heads * width + 4 * tokens * width),
        name="grad_hidden",
    )(core, *own, *oth, kv_own, kv_oth, w_q, w_k, w_v)


def solution(mesh):
    n_dev = mesh.shape["sp"]
    n_chunks = 4
    near_perm = [(d, d ^ 1) for d in range(n_dev)]
    far_perm = [(d, d ^ 2) for d in range(n_dev)]
    down_perm = [(0, 2), (1, 3)]
    up_perm = [(2, 0), (3, 1)]

    def near(v):
        return lax.ppermute(v, "sp", near_perm)

    def far(v):
        return lax.ppermute(v, "sp", far_perm)

    def device_step(hidden, grad_out, positions, doc_ids, w_q, w_k, w_v, w_o):
        tokens = hidden.shape[0]
        chip_len = 2 * tokens
        assert n_chunks == w_q.shape[1] // (2 * WIDE)
        place = lax.axis_index("sp")
        core_id, chip_id = place % 2, place // 2
        core = core_id.astype(jnp.int32)[None]
        sel_own = jnp.stack([core_id, core_id]).astype(jnp.int32)
        sel_oth = jnp.stack([core_id, 1 - core_id]).astype(jnp.int32)

        pos_doc = jnp.stack([positions, doc_ids])
        pos_doc_oth = near(pos_doc)
        x_oth = near(hidden)
        g_oth = near(grad_out)
        pos_doc = jnp.where(
            core_id == 0,
            jnp.concatenate([pos_doc, pos_doc_oth], axis=1),
            jnp.concatenate([pos_doc_oth, pos_doc], axis=1),
        )
        doc_chip = pos_doc[1]
        doc_far = far(doc_chip)
        cos_t, sin_t = rope_tables(pos_doc[0])

        heads_doc = doc_chip[::BQ]
        lo = jnp.sum(doc_chip[None, :] < heads_doc[:, None], axis=1, dtype=jnp.int32)
        lo_far = jnp.sum(doc_far[None, :] < heads_doc[:, None], axis=1, dtype=jnp.int32)
        lo = lo + jnp.where(chip_id == 0, chip_len, lo_far)
        lo = lo // ALIGN * ALIGN
        end = chip_len + BQ * (1 + jnp.arange(chip_len // BQ, dtype=jnp.int32))
        n_blocks = (end - lo + BK - 1) // BK
        kdoc = jnp.concatenate([doc_far, doc_chip, jnp.zeros((BK,), jnp.int32)])[None, :]
        qdoc = doc_chip[:, None]

        kv = kv_proj(sel_own, hidden, w_k, w_v, cos_t, sin_t, None)
        kv = kv_proj(sel_oth, x_oth, w_k, w_v, cos_t, sin_t, kv)
        kv_prev = lax.ppermute(kv, "sp", down_perm)
        q = q_proj(sel_own, hidden, w_q, cos_t, sin_t, None)
        grad_late, x_late = lax.optimization_barrier((kv, grad_out, x_oth))[1:]
        dctx = dctx_proj(sel_own, grad_late, w_o, None)
        q = q_proj(sel_oth, x_late, w_q, cos_t, sin_t, q)
        dctx = dctx_proj(sel_oth, g_oth, w_o, dctx)
        xt_own, xt_oth = flip(hidden), flip(x_late)

        acc = None
        acts, acts_oth, sums = [], [], None
        for j in range(n_chunks):
            act, ctxt, dk, dv = attention(j, lo, n_blocks, q, dctx, qdoc, kdoc, cos_t, sin_t, kv_prev, kv, acc)
            acc = (dk, dv)
            acts.append(act)
            acts_oth.append(near(act))
            if j == n_chunks - 1:
                dkv_up = jnp.stack([dk[:, :chip_len], dv[:, :chip_len]]).astype(BF)
                dkv_far = lax.ppermute(dkv_up, "sp", up_perm)
            part = wgrad(core, xt_own, xt_oth, act, grad_out, g_oth, ctxt)
            part_far = far(part)
            part_near = near(part)
            acc = lax.optimization_barrier((dk, dv, part))[:2]
            part_far_near = near(part_far)
            sums = combine(core, j, n_chunks, (part, part_far, part_near, part_far_near), sums)
        grad_wq, grad_wo = sums

        dkv = kv_finish(dk, dv, dkv_far, cos_t, sin_t)
        dkv_oth = near(dkv)
        kv_part = kvgrad(core, xt_own, xt_oth, dkv)
        kv_part_far = far(kv_part)
        kv_sum = kv_part.astype(F32) + kv_part_far.astype(F32)
        kv_sum_oth = near(kv_sum)

        def pick(cols):
            a, b = kv_sum[:, cols], kv_sum_oth[:, cols]
            return jnp.where(core_id == 0, jnp.concatenate([a, b], axis=1), jnp.concatenate([b, a], axis=1))

        grad_wk, grad_wv = pick(slice(0, HEAD)), pick(slice(HEAD, 2 * HEAD))
        out = attn_out(core, acts, acts_oth, w_o)
        g_hidden = grad_hidden(core, acts, acts_oth, dkv, dkv_oth, w_q, w_k, w_v)
        return out, g_hidden, grad_wq, grad_wk, grad_wv, grad_wo

    tok_spec = P(("dp", "sp"), None)
    vec_spec = P(("dp", "sp"))
    rep_spec = P(None, None)
    part_spec = P("dp", None)

    return jax.shard_map(
        device_step,
        mesh=mesh,
        in_specs=(tok_spec, tok_spec, vec_spec, vec_spec, rep_spec, rep_spec, rep_spec, rep_spec),
        out_specs=(tok_spec, tok_spec, part_spec, part_spec, part_spec, part_spec),
        check_vma=False,
    )
```

```python
import functools

import jax
import jax.numpy as jnp
from jax import lax
from jax.experimental import pallas as pl
from jax.experimental.pallas import tpu as pltpu
from jax.sharding import PartitionSpec as P

HEAD = 128
ROPE_THETA = 500000.0
ROPE_FACTOR = 8.0
ROPE_LOW = 1.0
ROPE_HIGH = 4.0
ROPE_OLD_CTX = 8192.0
NEG_BIG = -1.0e30
SCALE = HEAD ** -0.5
LOG2E = 1.4426950408889634

PAIR = 2
WIDE = PAIR * HEAD
BQ = 512
BK = 512
ALIGN = 128
BF = jnp.bfloat16
F32 = jnp.float32


def rope_freqs():
    half_idx = jnp.arange(HEAD // 2, dtype=F32)
    inv_freq = jnp.power(ROPE_THETA, -2.0 * half_idx / HEAD)
    wavelen = 2.0 * jnp.pi / inv_freq
    smooth = (ROPE_OLD_CTX / wavelen - ROPE_LOW) / (ROPE_HIGH - ROPE_LOW)
    mixed_freq = (1.0 - smooth) * inv_freq / ROPE_FACTOR + smooth * inv_freq
    scaled = jnp.where(wavelen > ROPE_OLD_CTX / ROPE_LOW, inv_freq / ROPE_FACTOR, mixed_freq)
    return jnp.where(wavelen < ROPE_OLD_CTX / ROPE_HIGH, inv_freq, scaled)


def rope_table(pos_vec):
    angles = pos_vec.astype(F32)[:, None] * rope_freqs()[None, :]
    return jnp.concatenate([jnp.cos(angles), jnp.sin(angles)], axis=-1)


def dot_nn(a, b):
    return lax.dot_general(a, b, (((1,), (0,)), ((), ())), preferred_element_type=F32)


def dot_nt(a, b):
    return lax.dot_general(a, b, (((1,), (1,)), ((), ())), preferred_element_type=F32)


def swap_halves(v):
    return pltpu.roll(v, HEAD // 2, 1)


def spread_table(tab):
    low = lax.broadcasted_iota(jnp.int32, tab.shape, 1) < HEAD // 2
    other = swap_halves(tab)
    return jnp.where(low, tab, other), jnp.where(low, -other, tab)


def cost(flops, nbytes, trans=0):
    return pl.CostEstimate(flops=int(flops), bytes_accessed=int(nbytes), transcendentals=int(trans))


def params(**kw):
    return pltpu.CompilerParams(vmem_limit_bytes=62 * 1024 * 1024, **kw)


def span(index, size):
    return pl.ds(pl.multiple_of(index * size, size), size)


def kv_kernel(s_ref, x_ref, wk_ref, wv_ref, tab_ref, out_ref, w_s):
    @pl.when(pl.program_id(0) == 0)
    def _():
        w_s[:, :HEAD] = wk_ref[...]
        w_s[:, HEAD:] = wv_ref[...]

    kv = dot_nn(x_ref[...], w_s[...])
    cos_t, sin_t = spread_table(tab_ref[...])
    k = kv[:, :HEAD]
    out_ref[:, :HEAD] = (k * cos_t + swap_halves(k) * sin_t).astype(BF)
    out_ref[:, HEAD:] = kv[:, HEAD:].astype(BF)


def kv_proj(core, x, w_k, w_v, tab):
    tokens, width = x.shape
    step = tokens // 4
    return pl.pallas_call(
        kv_kernel,
        grid_spec=pltpu.PrefetchScalarGridSpec(
            num_scalar_prefetch=1,
            grid=(tokens // step,),
            in_specs=[
                pl.BlockSpec((step, width), lambda m, s: (m, 0)),
                pl.BlockSpec((width, HEAD), lambda m, s: (0, s[0])),
                pl.BlockSpec((width, HEAD), lambda m, s: (0, s[0])),
                pl.BlockSpec((step, HEAD), lambda m, s: (m, 0)),
            ],
            out_specs=pl.BlockSpec((step, 2 * HEAD), lambda m, s: (m, 0)),
            scratch_shapes=[pltpu.VMEM((width, 2 * HEAD), BF)],
        ),
        out_shape=jax.ShapeDtypeStruct((tokens, 2 * HEAD), BF),
        compiler_params=params(),
        cost_estimate=cost(2 * tokens * width * 2 * HEAD, tokens * width * 2),
        name="kv_proj",
    )(core, x, w_k, w_v, tab)


def q_kernel(s_ref, x_ref, wq_ref, tab_ref, *rest):
    out_ref = rest[-1]
    q = dot_nn(x_ref[...], wq_ref[...])
    cos_t, sin_t = spread_table(tab_ref[...])
    for h in range(wq_ref.shape[1] // HEAD):
        part = q[:, h * HEAD:(h + 1) * HEAD]
        out_ref[:, h * HEAD:(h + 1) * HEAD] = (part * cos_t + swap_halves(part) * sin_t).astype(BF)


def q_proj(sel, x, w_q, tab, prev):
    tokens, width = x.shape
    cols = w_q.shape[1] // 2
    step = 512
    rows = tokens // 2
    n = cols // step
    extra = [] if prev is None else [prev]
    return pl.pallas_call(
        q_kernel,
        grid_spec=pltpu.PrefetchScalarGridSpec(
            num_scalar_prefetch=1,
            grid=(n, 2),
            in_specs=[
                pl.BlockSpec((rows, width), lambda j, m, s: (m, 0)),
                pl.BlockSpec((width, step), lambda j, m, s: (0, s[0] * n + j)),
                pl.BlockSpec((rows, HEAD), lambda j, m, s: (m, 0)),
            ] + [pl.BlockSpec(memory_space=pl.ANY)] * len(extra),
            out_specs=pl.BlockSpec((rows, step), lambda j, m, s: (s[1] * 2 + m, j)),
        ),
        out_shape=jax.ShapeDtypeStruct((2 * tokens, cols), BF),
        input_output_aliases={} if prev is None else {4: 0},
        compiler_params=params(),
        cost_estimate=cost(2 * tokens * width * cols, tokens * width * 2 + cols * width * 2),
        name="q_proj",
    )(sel, x, w_q, tab, *extra)


def dctx_kernel(s_ref, g_ref, wo_ref, *rest):
    out_ref = rest[-1]
    out_ref[...] = dot_nt(g_ref[...], wo_ref[...]).astype(BF)


def dctx_proj(sel, g, w_o, prev):
    tokens, width = g.shape
    cols = w_o.shape[0] // 2
    step = 512
    rows = tokens // 2
    n = cols // step
    extra = [] if prev is None else [prev]
    return pl.pallas_call(
        dctx_kernel,
        grid_spec=pltpu.PrefetchScalarGridSpec(
            num_scalar_prefetch=1,
            grid=(n, 2),
            in_specs=[
                pl.BlockSpec((rows, width), lambda j, m, s: (m, 0)),
                pl.BlockSpec((step, width), lambda j, m, s: (s[0] * n + j, 0)),
            ] + [pl.BlockSpec(memory_space=pl.ANY)] * len(extra),
            out_specs=pl.BlockSpec((rows, step), lambda j, m, s: (s[1] * 2 + m, j)),
        ),
        out_shape=jax.ShapeDtypeStruct((2 * tokens, cols), BF),
        input_output_aliases={} if prev is None else {3: 0},
        compiler_params=params(),
        cost_estimate=cost(2 * tokens * width * cols, tokens * width * 2 + cols * width * 2),
        name="dctx_proj",
    )(sel, g, w_o, *extra)


def attn_kernel(
    core_ref, lo_ref, nb_ref, q_ref, do_ref, kdoc_ref, tab_own, tab_oth, kvp_own, kvp_oth, kvc_own, kvc_oth,
    act_ref, actt_ref, dkv_ref,
    k_s, v_s, s_s, dp_s, m_s, l_s, d_s, qd_s, ctx_s, dq_s, q_s, do_s, qt_s, dot_s, tab_s, dk_s, dv_s,
):
    i = pl.program_id(0)
    tokens = kvc_own.shape[0]
    chip_len = 2 * tokens
    core = core_ref[0]

    @pl.when(i == 0)
    def _():
        for base, place, ref in ((0, core, kvp_own), (0, 1 - core, kvp_oth), (2, core, kvc_own), (2, 1 - core, kvc_oth)):
            where = span(base + place, tokens)
            k_s[where, :] = ref[:, :HEAD]
            v_s[where, :] = ref[:, HEAD:]
        k_s[2 * chip_len:, :] = jnp.zeros((BK, HEAD), BF)
        v_s[2 * chip_len:, :] = jnp.zeros((BK, HEAD), BF)
        tab_s[span(core, tokens), :] = tab_own[...]
        tab_s[span(1 - core, tokens), :] = tab_oth[...]
        dk_s[...] = jnp.zeros_like(dk_s)
        dv_s[...] = jnp.zeros_like(dv_s)

    for h in range(PAIR):
        rows = slice(h * BQ, (h + 1) * BQ)
        cols = slice(h * HEAD, (h + 1) * HEAD)
        q_s[rows, :] = q_ref[:, cols]
        do_s[rows, :] = do_ref[:, cols]
        qt_s[:, rows] = q_ref[:, cols].T
        dot_s[:, rows] = do_ref[:, cols].T
    qdoc = kdoc_ref[:, pl.ds(pl.multiple_of(chip_len + i * BQ, BQ), BQ)]
    qd_s[...] = jnp.broadcast_to(qdoc, (HEAD, BQ)).T
    m_s[...] = jnp.full(m_s.shape, NEG_BIG, F32)
    l_s[...] = jnp.zeros(l_s.shape, F32)
    d_s[...] = jnp.zeros(d_s.shape, F32)
    ctx_s[...] = jnp.zeros(ctx_s.shape, F32)
    dq_s[...] = jnp.zeros(dq_s.shape, F32)
    lo = lo_ref[i]
    n_blocks = nb_ref[i]
    lanes = BK // HEAD

    def fold(v, op):
        out = v[:, :HEAD]
        for n in range(1, lanes):
            out = op(out, v[:, n * HEAD:(n + 1) * HEAD])
        return out

    def spread(v):
        return jnp.concatenate([v] * lanes, axis=1)

    def offset(b):
        return pl.multiple_of(lo + b * BK, ALIGN)

    def scores(b, carry):
        off = offset(b)
        s = dot_nt(q_s[...], k_s[pl.ds(off, BK), :])
        key = off + lax.broadcasted_iota(jnp.int32, (BQ, BK), 1)
        query = chip_len + i * BQ + lax.broadcasted_iota(jnp.int32, (BQ, BK), 0)
        keep = (key <= query) & (kdoc_ref[:, pl.ds(off, BK)] == spread(qd_s[...]))
        for h in range(PAIR):
            rows = slice(h * BQ, (h + 1) * BQ)
            sh = jnp.where(keep, s[rows, :], NEG_BIG)
            s_s[b, rows, :] = sh
            m_s[rows, :] = jnp.maximum(m_s[rows, :], fold(sh, jnp.maximum))
        return carry

    lax.fori_loop(0, n_blocks, scores, 0)
    m_s[...] = jnp.broadcast_to(jnp.max(m_s[...], axis=1, keepdims=True), m_s.shape)

    def weights(b, carry):
        dp = dot_nt(do_s[...], v_s[pl.ds(offset(b), BK), :])
        e = jnp.exp2((s_s[b] - spread(m_s[...])) * (SCALE * LOG2E))
        s_s[b] = e
        dp_s[b] = dp
        l_s[...] += fold(e, jnp.add)
        d_s[...] += fold(e * dp, jnp.add)
        return carry

    lax.fori_loop(0, n_blocks, weights, 0)
    inv = 1.0 / jnp.sum(l_s[...], axis=1, keepdims=True)
    delta = jnp.sum(d_s[...], axis=1, keepdims=True) * inv
    l_s[...] = jnp.broadcast_to(inv, l_s.shape)
    d_s[...] = jnp.broadcast_to(delta, d_s.shape)

    def grads(b, carry):
        off = offset(b)
        p = s_s[b] * spread(l_s[...])
        pb = p.astype(BF)
        ds = (p * (dp_s[b] - spread(d_s[...])) * SCALE).astype(BF)
        ctx_s[...] += dot_nn(pb, v_s[pl.ds(off, BK), :])
        dq_s[...] += dot_nn(ds, k_s[pl.ds(off, BK), :])
        dv_s[:, pl.ds(off, BK)] += dot_nn(dot_s[...], pb)
        dk_s[:, pl.ds(off, BK)] += dot_nn(qt_s[...], ds)
        return carry

    lax.fori_loop(0, n_blocks, grads, 0)
    cos_t, sin_t = spread_table(tab_s[span(i, BQ), :])
    for h in range(PAIR):
        rows = slice(h * BQ, (h + 1) * BQ)
        cols = slice(h * HEAD, (h + 1) * HEAD)
        ctx = ctx_s[rows, :].astype(BF)
        act_ref[0, :, cols] = ctx
        actt_ref[0, cols, :] = ctx.T
        dq = dq_s[rows, :].astype(BF).astype(F32)
        dq = (dq * cos_t - swap_halves(dq) * sin_t).astype(BF)
        act_ref[1, :, cols] = dq
        actt_ref[1, cols, :] = dq.T

    @pl.when(i == pl.num_programs(0) - 1)
    def _():
        dkv_ref[0] = dk_s[:, :2 * chip_len].astype(BF)
        dkv_ref[1] = dv_s[:, :2 * chip_len].astype(BF)


def attention(chunk, core, lo, n_blocks, q, dctx, kdoc, tab_own, tab_oth, kv_prev, kv_chip):
    chip_len = q.shape[0]
    tokens = chip_len // 2
    padded = 2 * chip_len + BK
    max_blocks = 2 * chip_len // BK + 1
    rows = PAIR * BQ
    full = lambda shape: pl.BlockSpec(shape, lambda i, *s: (0,) * len(shape))
    pairs = chip_len * chip_len * PAIR
    return pl.pallas_call(
        attn_kernel,
        grid_spec=pltpu.PrefetchScalarGridSpec(
            num_scalar_prefetch=3,
            grid=(chip_len // BQ,),
            in_specs=[
                pl.BlockSpec((BQ, WIDE), lambda i, *s: (i, chunk)),
                pl.BlockSpec((BQ, WIDE), lambda i, *s: (i, chunk)),
                full((1, padded)),
            ] + [full((tokens, HEAD))] * 2 + [full((tokens, 2 * HEAD))] * 4,
            out_specs=[
                pl.BlockSpec((2, BQ, WIDE), lambda i, *s: (0, i, 0)),
                pl.BlockSpec((2, WIDE, BQ), lambda i, *s: (0, 0, i)),
                full((2, HEAD, 2 * chip_len)),
            ],
            scratch_shapes=[
                pltpu.VMEM((padded, HEAD), BF),
                pltpu.VMEM((padded, HEAD), BF),
                pltpu.VMEM((max_blocks, rows, BK), F32),
                pltpu.VMEM((max_blocks, rows, BK), F32),
                pltpu.VMEM((rows, HEAD), F32),
                pltpu.VMEM((rows, HEAD), F32),
                pltpu.VMEM((rows, HEAD), F32),
                pltpu.VMEM((BQ, HEAD), jnp.int32),
                pltpu.VMEM((rows, HEAD), F32),
                pltpu.VMEM((rows, HEAD), F32),
                pltpu.VMEM((rows, HEAD), BF),
                pltpu.VMEM((rows, HEAD), BF),
                pltpu.VMEM((HEAD, rows), BF),
                pltpu.VMEM((HEAD, rows), BF),
                pltpu.VMEM((chip_len, HEAD), F32),
                pltpu.VMEM((HEAD, padded), F32),
                pltpu.VMEM((HEAD, padded), F32),
            ],
        ),
        out_shape=[
            jax.ShapeDtypeStruct((2, chip_len, WIDE), BF),
            jax.ShapeDtypeStruct((2, WIDE, chip_len), BF),
            jax.ShapeDtypeStruct((2, HEAD, 2 * chip_len), BF),
        ],
        compiler_params=params(),
        cost_estimate=cost(pairs * HEAD * 2 * 8, 12 * 1024 * 1024, pairs),
        name="attention",
    )(core, lo, n_blocks, q, dctx, kdoc, tab_own, tab_oth, *kv_prev, *kv_chip)


def kv_finish_kernel(n, s_ref, *refs):
    far_ref, tab_own, tab_oth, out_ref, outt_ref, tab_s = refs[n:]
    tokens = tab_own.shape[0]
    step = out_ref.shape[0]

    @pl.when(pl.program_id(0) == 0)
    def _():
        tab_s[span(s_ref[0], tokens), :] = tab_own[...]
        tab_s[span(1 - s_ref[0], tokens), :] = tab_oth[...]

    total = far_ref[...].astype(F32)
    for ref in refs[:n]:
        total = total + ref[...].astype(F32)
    cos_t, sin_t = spread_table(tab_s[span(pl.program_id(0), step), :])
    dk = total[0].astype(BF).astype(F32).T
    dk = (dk * cos_t - swap_halves(dk) * sin_t).astype(BF)
    dvt = total[1].astype(BF)
    out_ref[:, :HEAD] = dk
    out_ref[:, HEAD:] = dvt.T
    outt_ref[:HEAD, :] = dk.T
    outt_ref[HEAD:, :] = dvt


def kv_finish(core, parts, far, tab_own, tab_oth):
    tokens = tab_own.shape[0]
    chip_len = 2 * tokens
    step = 512
    skip = chip_len // step
    return pl.pallas_call(
        functools.partial(kv_finish_kernel, len(parts)),
        grid_spec=pltpu.PrefetchScalarGridSpec(
            num_scalar_prefetch=1,
            grid=(chip_len // step,),
            in_specs=[pl.BlockSpec((2, HEAD, step), lambda t, s: (0, 0, skip + t))] * len(parts)
            + [
                pl.BlockSpec((2, HEAD, step), lambda t, s: (0, 0, t)),
                pl.BlockSpec((tokens, HEAD), lambda t, s: (0, 0)),
                pl.BlockSpec((tokens, HEAD), lambda t, s: (0, 0)),
            ],
            out_specs=[
                pl.BlockSpec((step, 2 * HEAD), lambda t, s: (t, 0)),
                pl.BlockSpec((2 * HEAD, step), lambda t, s: (0, t)),
            ],
            scratch_shapes=[pltpu.VMEM((chip_len, HEAD), F32)],
        ),
        out_shape=[
            jax.ShapeDtypeStruct((chip_len, 2 * HEAD), BF),
            jax.ShapeDtypeStruct((2 * HEAD, chip_len), BF),
        ],
        compiler_params=params(),
        cost_estimate=cost(chip_len * HEAD * 64, chip_len * HEAD * 16),
        name="kv_finish",
    )(core, *parts, far, tab_own, tab_oth)


def wgrad_kernel(s_ref, actt_ref, x_own, x_oth, g_own, g_oth, out_ref):
    tokens = x_own.shape[0]
    own, oth = span(s_ref[0], tokens), span(1 - s_ref[0], tokens)
    out_ref[0] = (dot_nn(actt_ref[1, :, own], x_own[...]) + dot_nn(actt_ref[1, :, oth], x_oth[...])).astype(BF)
    out_ref[1] = (dot_nn(actt_ref[0, :, own], g_own[...]) + dot_nn(actt_ref[0, :, oth], g_oth[...])).astype(BF)


def wgrad(core, actt, x_own, x_oth, g_own, g_oth):
    tokens, width = x_own.shape
    step = 512
    piece = pl.BlockSpec((tokens, step), lambda n, s: (0, n))
    return pl.pallas_call(
        wgrad_kernel,
        grid_spec=pltpu.PrefetchScalarGridSpec(
            num_scalar_prefetch=1,
            grid=(width // step,),
            in_specs=[pl.BlockSpec((2, WIDE, 2 * tokens), lambda n, s: (0, 0, 0)), piece, piece, piece, piece],
            out_specs=pl.BlockSpec((2, WIDE, step), lambda n, s: (0, 0, n)),
        ),
        out_shape=jax.ShapeDtypeStruct((2, WIDE, width), BF),
        compiler_params=params(),
        cost_estimate=cost(8 * tokens * width * WIDE, 8 * tokens * width),
        name="wgrad",
    )(core, actt, x_own, x_oth, g_own, g_oth)


def kvgrad_kernel(s_ref, dkvt_ref, x_own, x_oth, out_ref):
    tokens = x_own.shape[0]
    own, oth = span(s_ref[0], tokens), span(1 - s_ref[0], tokens)
    out_ref[...] = (dot_nn(dkvt_ref[:, own], x_own[...]) + dot_nn(dkvt_ref[:, oth], x_oth[...])).astype(BF)


def kvgrad(core, dkvt, x_own, x_oth):
    tokens, width = x_own.shape
    step = 512
    piece = pl.BlockSpec((tokens, step), lambda n, s: (0, n))
    return pl.pallas_call(
        kvgrad_kernel,
        grid_spec=pltpu.PrefetchScalarGridSpec(
            num_scalar_prefetch=1,
            grid=(width // step,),
            in_specs=[pl.BlockSpec((2 * HEAD, 2 * tokens), lambda n, s: (0, 0)), piece, piece],
            out_specs=pl.BlockSpec((2 * HEAD, step), lambda n, s: (0, n)),
        ),
        out_shape=jax.ShapeDtypeStruct((2 * HEAD, width), BF),
        compiler_params=params(),
        cost_estimate=cost(4 * tokens * width * 2 * HEAD, 4 * tokens * width),
        name="kvgrad",
    )(core, dkvt, x_own, x_oth)


def kv_combine_kernel(s_ref, a_ref, b_ref, c_ref, d_ref, gk_ref, gv_ref):
    for place, u_ref, v_ref in ((s_ref[0], a_ref, b_ref), (1 - s_ref[0], c_ref, d_ref)):
        total = u_ref[...].astype(F32) + v_ref[...].astype(F32)
        where = span(place, HEAD)
        gk_ref[:, where] = total[:HEAD, :].T
        gv_ref[:, where] = total[HEAD:, :].T


def kv_combine(core, parts):
    rows, width = parts[0].shape
    step = 512
    out = jax.ShapeDtypeStruct((width, rows), F32)
    return pl.pallas_call(
        kv_combine_kernel,
        grid_spec=pltpu.PrefetchScalarGridSpec(
            num_scalar_prefetch=1,
            grid=(width // step,),
            in_specs=[pl.BlockSpec((rows, step), lambda n, s: (0, n))] * 4,
            out_specs=[pl.BlockSpec((step, rows), lambda n, s: (n, 0))] * 2,
        ),
        out_shape=[out, out],
        compiler_params=params(),
        cost_estimate=cost(16 * width * rows * 16, 16 * width * rows),
        name="kv_combine",
    )(core, *parts)


def combine_kernel(s_ref, a_ref, b_ref, c_ref, d_ref, *rest):
    gq_ref, go_ref = rest[-2:]

    def put(u_ref, v_ref):
        gq_ref[...] = (u_ref[0].astype(F32) + v_ref[0].astype(F32)).T
        go_ref[...] = u_ref[1].astype(F32) + v_ref[1].astype(F32)

    @pl.when(pl.program_id(0) == 0)
    def _():
        put(a_ref, b_ref)

    @pl.when(pl.program_id(0) == 1)
    def _():
        put(c_ref, d_ref)


def combine(core, chunk, n_chunks, parts, prev):
    width = parts[0].shape[2]
    step = 512
    last = width // step - 1
    near = pl.BlockSpec((2, WIDE, step), lambda w, r, s: (0, 0, r + w * (last - r)))
    far = pl.BlockSpec((2, WIDE, step), lambda w, r, s: (0, 0, r * w))

    def place(w, s):
        return (s[0] + w - 2 * s[0] * w) * n_chunks + chunk

    shape = jax.ShapeDtypeStruct((width, 2 * n_chunks * WIDE), F32)
    shape_o = jax.ShapeDtypeStruct((2 * n_chunks * WIDE, width), F32)
    extra = [] if prev is None else list(prev)
    return pl.pallas_call(
        combine_kernel,
        grid_spec=pltpu.PrefetchScalarGridSpec(
            num_scalar_prefetch=1,
            grid=(2, width // step),
            in_specs=[near, near, far, far] + [pl.BlockSpec(memory_space=pl.ANY)] * len(extra),
            out_specs=[
                pl.BlockSpec((step, WIDE), lambda w, r, s: (r, place(w, s))),
                pl.BlockSpec((WIDE, step), lambda w, r, s: (place(w, s), r)),
            ],
        ),
        out_shape=[shape, shape_o],
        input_output_aliases={} if prev is None else {5: 0, 6: 1},
        compiler_params=params(),
        cost_estimate=cost(16 * width * WIDE * 64, 32 * width * WIDE),
        name="combine",
    )(core, *parts, *extra)


def fill_heads(core, own_refs, oth_refs, lhs):
    n = len(own_refs)
    for j in range(n):
        lhs[:, pl.ds(pl.multiple_of((core * n + j) * WIDE, WIDE), WIDE)] = own_refs[j][0]
        lhs[:, pl.ds(pl.multiple_of(((1 - core) * n + j) * WIDE, WIDE), WIDE)] = oth_refs[j][0]


def attn_out_kernel(n, s_ref, *refs):
    own_refs, oth_refs = refs[:n], refs[n:2 * n]
    wo_ref, out_ref, lhs = refs[2 * n:]

    @pl.when(pl.program_id(0) == 0)
    def _():
        fill_heads(s_ref[0], own_refs, oth_refs, lhs)

    out_ref[...] = dot_nn(lhs[...], wo_ref[...]).astype(BF)


def attn_out(core, own, oth, w_o):
    n = len(own)
    tokens = own[0].shape[1] // 2
    heads, width = w_o.shape
    step = 512
    return pl.pallas_call(
        functools.partial(attn_out_kernel, n),
        grid_spec=pltpu.PrefetchScalarGridSpec(
            num_scalar_prefetch=1,
            grid=(width // step,),
            in_specs=[pl.BlockSpec((1, tokens, WIDE), lambda k, s: (0, s[0], 0))] * (2 * n)
            + [pl.BlockSpec((heads, step), lambda k, s: (0, k))],
            out_specs=pl.BlockSpec((tokens, step), lambda k, s: (0, k)),
            scratch_shapes=[pltpu.VMEM((tokens, heads), BF)],
        ),
        out_shape=jax.ShapeDtypeStruct((tokens, width), BF),
        compiler_params=params(),
        cost_estimate=cost(2 * tokens * heads * width, 2 * heads * width + 4 * tokens * width),
        name="attn_out",
    )(core, *own, *oth, w_o)


def hidden_kernel(n, s_ref, *refs):
    own_refs, oth_refs = refs[:n], refs[n:2 * n]
    kv_own, kv_oth, wq_ref, wk_ref, wv_ref, out_ref, lhs, klhs, vlhs = refs[2 * n:]
    core = s_ref[0]

    @pl.when(pl.program_id(0) == 0)
    def _():
        fill_heads(core, own_refs, oth_refs, lhs)
        for place, ref in ((core, kv_own), (1 - core, kv_oth)):
            where = pl.ds(pl.multiple_of(place * HEAD, HEAD), HEAD)
            klhs[:, where] = ref[:, :HEAD]
            vlhs[:, where] = ref[:, HEAD:]

    out_ref[...] = (
        dot_nt(lhs[...], wq_ref[...]) + dot_nt(klhs[...], wk_ref[...]) + dot_nt(vlhs[...], wv_ref[...])
    ).astype(BF)


def grad_hidden(core, own, oth, kv_own, kv_oth, w_q, w_k, w_v):
    n = len(own)
    tokens = own[0].shape[1] // 2
    width, heads = w_q.shape
    kv_cols = w_k.shape[1]
    step = 512
    return pl.pallas_call(
        functools.partial(hidden_kernel, n),
        grid_spec=pltpu.PrefetchScalarGridSpec(
            num_scalar_prefetch=1,
            grid=(width // step,),
            in_specs=[pl.BlockSpec((1, tokens, WIDE), lambda k, s: (1, s[0], 0))] * (2 * n)
            + [pl.BlockSpec((tokens, 2 * HEAD), lambda k, s: (s[0], 0))] * 2
            + [
                pl.BlockSpec((step, heads), lambda k, s: (k, 0)),
                pl.BlockSpec((step, kv_cols), lambda k, s: (k, 0)),
                pl.BlockSpec((step, kv_cols), lambda k, s: (k, 0)),
            ],
            out_specs=pl.BlockSpec((tokens, step), lambda k, s: (0, k)),
            scratch_shapes=[
                pltpu.VMEM((tokens, heads), BF),
                pltpu.VMEM((tokens, kv_cols), BF),
                pltpu.VMEM((tokens, kv_cols), BF),
            ],
        ),
        out_shape=jax.ShapeDtypeStruct((tokens, width), BF),
        compiler_params=params(),
        cost_estimate=cost(2 * tokens * (heads + 2 * kv_cols) * width, 2 * heads * width + 4 * tokens * width),
        name="grad_hidden",
    )(core, *own, *oth, kv_own, kv_oth, w_q, w_k, w_v)


def solution(mesh):
    n_dev = mesh.shape["sp"]
    n_chunks = 4
    near_perm = [(d, d ^ 1) for d in range(n_dev)]
    far_perm = [(d, d ^ 2) for d in range(n_dev)]
    down_perm = [(0, 2), (1, 3)]
    up_perm = [(2, 0), (3, 1)]

    def near(v):
        return lax.ppermute(v, "sp", near_perm)

    def far(v):
        return lax.ppermute(v, "sp", far_perm)

    def device_step(hidden, grad_out, positions, doc_ids, w_q, w_k, w_v, w_o):
        tokens = hidden.shape[0]
        chip_len = 2 * tokens
        assert n_chunks == w_q.shape[1] // (2 * WIDE)
        place = lax.axis_index("sp")
        core_id, chip_id = place & 1, place >> 1
        core = core_id.astype(jnp.int32)[None]
        sel_own = jnp.stack([core_id, core_id]).astype(jnp.int32)
        sel_oth = jnp.stack([core_id, 1 - core_id]).astype(jnp.int32)

        doc_oth = near(doc_ids)
        x_oth = near(hidden)
        g_oth = near(grad_out)
        tab_own = rope_table(positions)
        tab_oth = near(tab_own)
        kv_own = kv_proj(core, hidden, w_k, w_v, tab_own)
        kvp_own = lax.ppermute(kv_own, "sp", down_perm)
        q = q_proj(sel_own, hidden, w_q, tab_own, None)
        doc_chip = jnp.where(
            core_id == 0, jnp.concatenate([doc_ids, doc_oth]), jnp.concatenate([doc_oth, doc_ids])
        )
        doc_far = far(doc_chip)
        kv_oth = kv_proj(core, x_oth, w_k, w_v, tab_oth)
        kvp_oth = lax.ppermute(kv_oth, "sp", down_perm)
        dctx = dctx_proj(sel_own, grad_out, w_o, None)
        q = q_proj(sel_oth, x_oth, w_q, tab_oth, q)
        dctx = dctx_proj(sel_oth, g_oth, w_o, dctx)

        heads_doc = doc_chip[::BQ]
        lo = jnp.sum(doc_chip[None, :] < heads_doc[:, None], axis=1, dtype=jnp.int32)
        lo_far = jnp.sum(doc_far[None, :] < heads_doc[:, None], axis=1, dtype=jnp.int32)
        lo = lo + jnp.where(chip_id == 0, chip_len, lo_far)
        lo = (lo >> (ALIGN.bit_length() - 1)) << (ALIGN.bit_length() - 1)
        end = chip_len + BQ * (1 + jnp.arange(chip_len // BQ, dtype=jnp.int32))
        n_blocks = (end - lo + BK - 1) >> (BK.bit_length() - 1)
        kdoc = jnp.concatenate([doc_far, doc_chip, jnp.zeros((BK,), jnp.int32)])[None, :]

        acts, acts_oth, dkvs, sums = [], [], [], None
        q_in = q
        for j in range(n_chunks):
            act, actt, dkv = attention(
                j, core, lo, n_blocks, q_in, dctx, kdoc, tab_own, tab_oth, (kvp_own, kvp_oth), (kv_own, kv_oth)
            )
            acts.append(act)
            dkvs.append(dkv)
            if j == n_chunks - 1:
                dkv_up = sum(d[:, :, :chip_len].astype(F32) for d in dkvs).astype(BF)
                dkv_far = lax.ppermute(dkv_up, "sp", up_perm)
            acts_oth.append(near(act))
            part = wgrad(core, actt, hidden, x_oth, grad_out, g_oth)
            part_far = far(part)
            part_near = near(part)
            part_far_near = near(part_far)
            sums = combine(core, j, n_chunks, (part, part_far, part_near, part_far_near), sums)
        grad_wq, grad_wo = sums

        dkv, dkvt = kv_finish(core, dkvs, dkv_far, tab_own, tab_oth)
        dkv_oth = near(dkv)
        kv_part = kvgrad(core, dkvt, hidden, x_oth)
        kv_part_far = far(kv_part)
        kv_part_near = near(kv_part)
        kv_part_far_near = near(kv_part_far)
        grad_wk, grad_wv = kv_combine(core, (kv_part, kv_part_far, kv_part_near, kv_part_far_near))
        out = attn_out(core, acts, acts_oth, w_o)
        g_hidden = grad_hidden(core, acts, acts_oth, dkv, dkv_oth, w_q, w_k, w_v)
        return out, g_hidden, grad_wq, grad_wk, grad_wv, grad_wo

    tok_spec = P(("dp", "sp"), None)
    vec_spec = P(("dp", "sp"))
    rep_spec = P(None, None)
    part_spec = P("dp", None)


    return jax.shard_map(
        device_step,
        mesh=mesh,
        in_specs=(tok_spec, tok_spec, vec_spec, vec_spec, rep_spec, rep_spec, rep_spec, rep_spec),
        out_specs=(tok_spec, tok_spec, part_spec, part_spec, part_spec, part_spec),
        check_vma=False,
    )
```

```python
import functools

import jax
import jax.numpy as jnp
from jax import lax
from jax.experimental import pallas as pl
from jax.experimental.pallas import tpu as pltpu
from jax.sharding import PartitionSpec as P

HEAD = 128
ROPE_THETA = 500000.0
ROPE_FACTOR = 8.0
ROPE_LOW = 1.0
ROPE_HIGH = 4.0
ROPE_OLD_CTX = 8192.0
NEG_BIG = -1.0e30
SCALE = HEAD ** -0.5
LOG2E = 1.4426950408889634

PAIR = 2
WIDE = PAIR * HEAD
BQ = 512
BK = 512
ALIGN = 128
BF = jnp.bfloat16
F32 = jnp.float32


def rope_freqs():
    half_idx = jnp.arange(HEAD // 2, dtype=F32)
    inv_freq = jnp.power(ROPE_THETA, -2.0 * half_idx / HEAD)
    wavelen = 2.0 * jnp.pi / inv_freq
    smooth = (ROPE_OLD_CTX / wavelen - ROPE_LOW) / (ROPE_HIGH - ROPE_LOW)
    mixed_freq = (1.0 - smooth) * inv_freq / ROPE_FACTOR + smooth * inv_freq
    scaled = jnp.where(wavelen > ROPE_OLD_CTX / ROPE_LOW, inv_freq / ROPE_FACTOR, mixed_freq)
    return jnp.where(wavelen < ROPE_OLD_CTX / ROPE_HIGH, inv_freq, scaled)


def rope_table(pos_vec):
    angles = pos_vec.astype(F32)[:, None] * rope_freqs()[None, :]
    return jnp.concatenate([jnp.cos(angles), jnp.sin(angles)], axis=-1)


def dot_nn(a, b):
    return lax.dot_general(a, b, (((1,), (0,)), ((), ())), preferred_element_type=F32)


def dot_nt(a, b):
    return lax.dot_general(a, b, (((1,), (1,)), ((), ())), preferred_element_type=F32)


def swap_halves(v):
    return pltpu.roll(v, HEAD // 2, 1)


def spread_table(tab):
    low = lax.broadcasted_iota(jnp.int32, tab.shape, 1) < HEAD // 2
    other = swap_halves(tab)
    return jnp.where(low, tab, other), jnp.where(low, -other, tab)


def cost(flops, nbytes, trans=0):
    return pl.CostEstimate(flops=int(flops), bytes_accessed=int(nbytes), transcendentals=int(trans))


def params(**kw):
    return pltpu.CompilerParams(vmem_limit_bytes=67_000_000, **kw)


def by_rows(rows, body, size=16):
    def step(r, carry):
        body(span(r, size))
        return carry

    lax.fori_loop(0, rows // size, step, 0)


def span(index, size):
    return pl.ds(pl.multiple_of(index * size, size), size)


def qkv_kernel(s_ref, x_ref, wq_ref, wk_ref, wv_ref, tab_ref, *rest):
    kv_ref, q_ref, w_s = rest[-3:]

    @pl.when(pl.program_id(0) == 0)
    def _():
        w_s[:, :HEAD] = wk_ref[...]
        w_s[:, HEAD:] = wv_ref[...]

    x = x_ref[...]
    cos_t, sin_t = spread_table(tab_ref[...])
    kv = dot_nn(x, w_s[...])
    k = kv[:, :HEAD]
    kv_ref[:, :HEAD] = (k * cos_t + swap_halves(k) * sin_t).astype(BF)
    kv_ref[:, HEAD:] = kv[:, HEAD:].astype(BF)
    step = 4 * HEAD
    for n in range(wq_ref.shape[1] // step):
        q = dot_nn(x, wq_ref[:, n * step:(n + 1) * step])
        for h in range(step // HEAD):
            part = q[:, h * HEAD:(h + 1) * HEAD]
            at = n * step + h * HEAD
            q_ref[:, at:at + HEAD] = (part * cos_t + swap_halves(part) * sin_t).astype(BF)


def qkv_proj(sel, x, w_q, w_k, w_v, tab, prev):
    tokens, width = x.shape
    cols = w_q.shape[1] // 2
    rows = tokens // 2
    extra = [] if prev is None else [prev]
    return pl.pallas_call(
        qkv_kernel,
        grid_spec=pltpu.PrefetchScalarGridSpec(
            num_scalar_prefetch=1,
            grid=(2,),
            in_specs=[
                pl.BlockSpec((rows, width), lambda m, s: (m, 0)),
                pl.BlockSpec((width, cols), lambda m, s: (0, s[0])),
                pl.BlockSpec((width, HEAD), lambda m, s: (0, s[0])),
                pl.BlockSpec((width, HEAD), lambda m, s: (0, s[0])),
                pl.BlockSpec((rows, HEAD), lambda m, s: (m, 0)),
            ] + [pl.BlockSpec(memory_space=pl.ANY)] * len(extra),
            out_specs=[
                pl.BlockSpec((rows, 2 * HEAD), lambda m, s: (m, 0)),
                pl.BlockSpec((rows, cols), lambda m, s: (s[1] * 2 + m, 0)),
            ],
            scratch_shapes=[pltpu.VMEM((width, 2 * HEAD), BF)],
        ),
        out_shape=[
            jax.ShapeDtypeStruct((tokens, 2 * HEAD), BF),
            jax.ShapeDtypeStruct((2 * tokens, cols), BF),
        ],
        input_output_aliases={} if prev is None else {6: 1},
        compiler_params=params(),
        cost_estimate=cost(2 * tokens * width * (cols + 2 * HEAD), tokens * width * 2 + cols * width * 2),
        name="qkv_proj",
    )(sel, x, w_q, w_k, w_v, tab, *extra)


def dctx_kernel(s_ref, own_ref, oth_ref, wo_ref, out_ref):
    def put(ref):
        step = 4 * HEAD
        for n in range(wo_ref.shape[0] // step):
            out_ref[:, n * step:(n + 1) * step] = dot_nt(ref[...], wo_ref[n * step:(n + 1) * step, :]).astype(BF)

    @pl.when(pl.program_id(0) < 2)
    def _():
        put(own_ref)

    @pl.when(pl.program_id(0) >= 2)
    def _():
        put(oth_ref)


def dctx_proj(core, own, oth, w_o):
    tokens, width = own.shape
    cols = w_o.shape[0] // 2
    rows = tokens // 2

    def place(m, s):
        far = m // 2
        return (s[0] + far - 2 * s[0] * far) * 2 + m % 2

    return pl.pallas_call(
        dctx_kernel,
        grid_spec=pltpu.PrefetchScalarGridSpec(
            num_scalar_prefetch=1,
            grid=(4,),
            in_specs=[
                pl.BlockSpec((rows, width), lambda m, s: (jnp.minimum(m, 1), 0)),
                pl.BlockSpec((rows, width), lambda m, s: (jnp.maximum(m - 2, 0), 0)),
                pl.BlockSpec((cols, width), lambda m, s: (s[0], 0)),
            ],
            out_specs=pl.BlockSpec((rows, cols), lambda m, s: (place(m, s), 0)),
        ),
        out_shape=jax.ShapeDtypeStruct((2 * tokens, cols), BF),
        compiler_params=params(),
        cost_estimate=cost(4 * tokens * width * cols, tokens * width * 4 + cols * width * 2),
        name="dctx_proj",
    )(core, own, oth, w_o)


def attn_kernel(
    core_ref, lo_ref, nb_ref, q_ref, do_ref, kdoc_ref, tab_own, tab_oth, kvp_own, kvp_oth, kvc_own, kvc_oth,
    x_own, x_oth, g_own, g_oth, act_ref, part_ref, dkv_ref,
    k_s, v_s, s_s, dp_s, m_s, l_s, d_s, qd_s, ctx_s, dq_s, q_s, do_s, qt_s, dot_s, tab_s, dk_s, dv_s,
    x_s, g_s, at_s, w_s, init_sem, row_sem, out_sem,
):
    i = pl.program_id(0)
    tokens = kvc_own.shape[0]
    chip_len = 2 * tokens
    core = core_ref[0]
    per_half = tokens // BQ
    rows_here = span(i % per_half, BQ)

    def row_copies(x, g):
        return (
            pltpu.make_async_copy(x.at[rows_here, :], x_s, row_sem.at[0]),
            pltpu.make_async_copy(g.at[rows_here, :], g_s, row_sem.at[1]),
        )

    @pl.when(i // per_half == core)
    def _():
        for copy in row_copies(x_own, g_own):
            copy.start()

    @pl.when(i // per_half != core)
    def _():
        for copy in row_copies(x_oth, g_oth):
            copy.start()

    @pl.when(i == 0)
    def _():
        copies = []
        for base, place, ref in ((0, core, kvp_own), (0, 1 - core, kvp_oth), (2, core, kvc_own), (2, 1 - core, kvc_oth)):
            where = span(base + place, tokens)
            copies.append((ref.at[:, pl.ds(0, HEAD)], k_s.at[where, :]))
            copies.append((ref.at[:, pl.ds(HEAD, HEAD)], v_s.at[where, :]))
        copies.append((tab_own, tab_s.at[span(core, tokens), :]))
        copies.append((tab_oth, tab_s.at[span(1 - core, tokens), :]))
        copies = [pltpu.make_async_copy(src, dst, init_sem.at[n]) for n, (src, dst) in enumerate(copies)]
        for copy in copies:
            copy.start()
        k_s[2 * chip_len:, :] = jnp.zeros((BK, HEAD), BF)
        v_s[2 * chip_len:, :] = jnp.zeros((BK, HEAD), BF)

        def clear(r):
            w_s[r, :] = jnp.zeros((16, w_s.shape[1]), F32)

        def clear_kv(r):
            dk_s[r, :] = jnp.zeros((16, dk_s.shape[1]), F32)
            dv_s[r, :] = jnp.zeros((16, dv_s.shape[1]), F32)

        by_rows(w_s.shape[0], clear)
        by_rows(HEAD, clear_kv)
        for copy in copies:
            copy.wait()

    for h in range(PAIR):
        rows = slice(h * BQ, (h + 1) * BQ)
        cols = slice(h * HEAD, (h + 1) * HEAD)
        q_s[rows, :] = q_ref[:, cols]
        do_s[rows, :] = do_ref[:, cols]
        qt_s[:, rows] = q_ref[:, cols].T
        dot_s[:, rows] = do_ref[:, cols].T
    qdoc = kdoc_ref[:, pl.ds(pl.multiple_of(chip_len + i * BQ, BQ), BQ)]
    qd_s[...] = jnp.broadcast_to(qdoc, (HEAD, BQ)).T
    m_s[...] = jnp.full(m_s.shape, NEG_BIG, F32)
    l_s[...] = jnp.zeros(l_s.shape, F32)
    d_s[...] = jnp.zeros(d_s.shape, F32)
    ctx_s[...] = jnp.zeros(ctx_s.shape, F32)
    dq_s[...] = jnp.zeros(dq_s.shape, F32)
    lo = lo_ref[i]
    n_blocks = nb_ref[i]
    lanes = BK // HEAD

    def fold(v, op):
        out = v[:, :HEAD]
        for n in range(1, lanes):
            out = op(out, v[:, n * HEAD:(n + 1) * HEAD])
        return out

    def spread(v):
        return jnp.concatenate([v] * lanes, axis=1)

    def offset(b):
        return pl.multiple_of(lo + b * BK, ALIGN)

    def scores(b, carry):
        off = offset(b)
        s = dot_nt(q_s[...], k_s[pl.ds(off, BK), :])
        key = off + lax.broadcasted_iota(jnp.int32, (BQ, BK), 1)
        query = chip_len + i * BQ + lax.broadcasted_iota(jnp.int32, (BQ, BK), 0)
        keep = (key <= query) & (kdoc_ref[:, pl.ds(off, BK)] == spread(qd_s[...]))
        for h in range(PAIR):
            rows = slice(h * BQ, (h + 1) * BQ)
            sh = jnp.where(keep, s[rows, :], NEG_BIG)
            s_s[b, rows, :] = sh
            m_s[rows, :] = jnp.maximum(m_s[rows, :], fold(sh, jnp.maximum))
        return carry

    lax.fori_loop(0, n_blocks, scores, 0)
    m_s[...] = jnp.broadcast_to(jnp.max(m_s[...], axis=1, keepdims=True), m_s.shape)

    def weights(b, carry):
        dp = dot_nt(do_s[...], v_s[pl.ds(offset(b), BK), :])
        e = jnp.exp2((s_s[b] - spread(m_s[...])) * (SCALE * LOG2E))
        s_s[b] = e
        dp_s[b] = dp
        l_s[...] += fold(e, jnp.add)
        d_s[...] += fold(e * dp, jnp.add)
        return carry

    lax.fori_loop(0, n_blocks, weights, 0)
    inv = 1.0 / jnp.sum(l_s[...], axis=1, keepdims=True)
    delta = jnp.sum(d_s[...], axis=1, keepdims=True) * inv
    l_s[...] = jnp.broadcast_to(inv, l_s.shape)
    d_s[...] = jnp.broadcast_to(delta, d_s.shape)

    def grads(b, carry):
        off = offset(b)
        p = s_s[b] * spread(l_s[...])
        pb = p.astype(BF)
        ds = (p * (dp_s[b] - spread(d_s[...])) * SCALE).astype(BF)
        ctx_s[...] += dot_nn(pb, v_s[pl.ds(off, BK), :])
        dq_s[...] += dot_nn(ds, k_s[pl.ds(off, BK), :])
        dv_s[:, pl.ds(off, BK)] += dot_nn(dot_s[...], pb)
        dk_s[:, pl.ds(off, BK)] += dot_nn(qt_s[...], ds)
        return carry

    lax.fori_loop(0, n_blocks, grads, 0)
    cos_t, sin_t = spread_table(tab_s[span(i, BQ), :])
    for h in range(PAIR):
        rows = slice(h * BQ, (h + 1) * BQ)
        cols = slice(h * HEAD, (h + 1) * HEAD)
        ctx = ctx_s[rows, :].astype(BF)
        act_ref[0, :, cols] = ctx
        at_s[WIDE + h * HEAD:WIDE + (h + 1) * HEAD, :] = ctx.T
        dq = dq_s[rows, :].astype(BF).astype(F32)
        dq = (dq * cos_t - swap_halves(dq) * sin_t).astype(BF)
        act_ref[1, :, cols] = dq
        at_s[h * HEAD:(h + 1) * HEAD, :] = dq.T
    step = 4 * HEAD
    for copy in row_copies(x_own, g_own):
        copy.wait()

    def products(c, carry):
        cols = span(c, step)
        w_s[:WIDE, cols] += dot_nn(at_s[:WIDE, :], x_s[:, cols])
        w_s[WIDE:, cols] += dot_nn(at_s[WIDE:, :], g_s[:, cols])
        return carry

    lax.fori_loop(0, x_s.shape[1] // step, products, 0)

    @pl.when(i == pl.num_programs(0) - 1)
    def _():
        def narrow(r):
            x_s[r, :] = w_s[r, :].astype(BF)

        by_rows(w_s.shape[0], narrow)

        def narrow_kv(r, carry):
            rows = span(r, 16)
            for n, acc in enumerate((dk_s, dv_s)):
                for side in range(2):
                    at = pl.ds(pl.multiple_of((2 * n + side) * HEAD + r * 16, 16), 16)
                    g_s[at, :] = acc[rows, side * chip_len:(side + 1) * chip_len].astype(BF)
            return carry

        lax.fori_loop(0, HEAD // 16, narrow_kv, 0)
        copies = (
            pltpu.make_async_copy(x_s, part_ref, out_sem.at[0]),
            pltpu.make_async_copy(g_s, dkv_ref, out_sem.at[1]),
        )
        for copy in copies:
            copy.start()
        for copy in copies:
            copy.wait()


def attention(chunk, core, lo, n_blocks, q, dctx, kdoc, tabs, kv_prev, kv_chip, xs, gs):
    chip_len = q.shape[0]
    width = xs[0].shape[1]
    assert 2 * WIDE == BQ == 4 * HEAD and width == chip_len
    padded = 2 * chip_len + BK
    max_blocks = 2 * chip_len // BK
    rows = PAIR * BQ
    full = lambda shape: pl.BlockSpec(shape, lambda i, *s: (0,) * len(shape))
    pairs = chip_len * chip_len * PAIR
    return pl.pallas_call(
        attn_kernel,
        grid_spec=pltpu.PrefetchScalarGridSpec(
            num_scalar_prefetch=3,
            grid=(chip_len // BQ,),
            in_specs=[
                pl.BlockSpec((BQ, WIDE), lambda i, *s: (i, chunk)),
                pl.BlockSpec((BQ, WIDE), lambda i, *s: (i, chunk)),
                full((1, padded)),
            ] + [pl.BlockSpec(memory_space=pl.ANY)] * 10,
            out_specs=[
                pl.BlockSpec((2, BQ, WIDE), lambda i, *s: (0, i, 0)),
                pl.BlockSpec(memory_space=pl.ANY),
                pl.BlockSpec(memory_space=pl.ANY),
            ],
            scratch_shapes=[
                pltpu.VMEM((padded, HEAD), BF),
                pltpu.VMEM((padded, HEAD), BF),
                pltpu.VMEM((max_blocks, rows, BK), F32),
                pltpu.VMEM((max_blocks, rows, BK), F32),
                pltpu.VMEM((rows, HEAD), F32),
                pltpu.VMEM((rows, HEAD), F32),
                pltpu.VMEM((rows, HEAD), F32),
                pltpu.VMEM((BQ, HEAD), jnp.int32),
                pltpu.VMEM((rows, HEAD), F32),
                pltpu.VMEM((rows, HEAD), F32),
                pltpu.VMEM((rows, HEAD), BF),
                pltpu.VMEM((rows, HEAD), BF),
                pltpu.VMEM((HEAD, rows), BF),
                pltpu.VMEM((HEAD, rows), BF),
                pltpu.VMEM((chip_len, HEAD), F32),
                pltpu.VMEM((HEAD, padded), F32),
                pltpu.VMEM((HEAD, padded), F32),
                pltpu.VMEM((BQ, width), BF),
                pltpu.VMEM((BQ, width), BF),
                pltpu.VMEM((2 * WIDE, BQ), BF),
                pltpu.VMEM((2 * WIDE, width), F32),
                pltpu.SemaphoreType.DMA((10,)),
                pltpu.SemaphoreType.DMA((2,)),
                pltpu.SemaphoreType.DMA((2,)),
            ],
        ),
        out_shape=[
            jax.ShapeDtypeStruct((2, chip_len, WIDE), BF),
            jax.ShapeDtypeStruct((2 * WIDE, width), BF),
            jax.ShapeDtypeStruct((4 * HEAD, chip_len), BF),
        ],
        compiler_params=params(),
        cost_estimate=cost(pairs * HEAD * 2 * 8, 12 * 1024 * 1024, pairs),
        name="attention",
    )(core, lo, n_blocks, q, dctx, kdoc, *tabs, *kv_prev, *kv_chip, *xs, *gs)


def kv_finish_kernel(n, s_ref, *refs):
    far_ref, tab_own, tab_oth, out_ref, outt_ref, tab_s = refs[n:]
    tokens = tab_own.shape[0]
    step = out_ref.shape[0]

    @pl.when(pl.program_id(0) == 0)
    def _():
        tab_s[span(s_ref[0], tokens), :] = tab_own[...]
        tab_s[span(1 - s_ref[0], tokens), :] = tab_oth[...]

    total = far_ref[...].astype(F32)
    for ref in refs[:n]:
        total = total + ref[:, 0].astype(F32)
    cos_t, sin_t = spread_table(tab_s[span(pl.program_id(0), step), :])
    dk = total[0].astype(BF).astype(F32).T
    dk = (dk * cos_t - swap_halves(dk) * sin_t).astype(BF)
    dvt = total[1].astype(BF)
    out_ref[:, :HEAD] = dk
    out_ref[:, HEAD:] = dvt.T
    outt_ref[:HEAD, :] = dk.T
    outt_ref[HEAD:, :] = dvt


def kv_finish(core, parts, far, tab_own, tab_oth):
    tokens = tab_own.shape[0]
    chip_len = 2 * tokens
    step = 512
    return pl.pallas_call(
        functools.partial(kv_finish_kernel, len(parts)),
        grid_spec=pltpu.PrefetchScalarGridSpec(
            num_scalar_prefetch=1,
            grid=(chip_len // step,),
            in_specs=[pl.BlockSpec((2, 1, HEAD, step), lambda t, s: (0, 1, 0, t))] * len(parts)
            + [
                pl.BlockSpec((2, HEAD, step), lambda t, s: (0, 0, t)),
                pl.BlockSpec((tokens, HEAD), lambda t, s: (0, 0)),
                pl.BlockSpec((tokens, HEAD), lambda t, s: (0, 0)),
            ],
            out_specs=[
                pl.BlockSpec((step, 2 * HEAD), lambda t, s: (t, 0)),
                pl.BlockSpec((2 * HEAD, step), lambda t, s: (0, t)),
            ],
            scratch_shapes=[pltpu.VMEM((chip_len, HEAD), F32)],
        ),
        out_shape=[
            jax.ShapeDtypeStruct((chip_len, 2 * HEAD), BF),
            jax.ShapeDtypeStruct((2 * HEAD, chip_len), BF),
        ],
        compiler_params=params(),
        cost_estimate=cost(chip_len * HEAD * 64, chip_len * HEAD * 16),
        name="kv_finish",
    )(core, *parts, far, tab_own, tab_oth)


def kvgrad_kernel(s_ref, dkvt_ref, x_own, x_oth, out_ref):
    tokens = x_own.shape[0]
    own, oth = span(s_ref[0], tokens), span(1 - s_ref[0], tokens)
    out_ref[...] = (dot_nn(dkvt_ref[:, own], x_own[...]) + dot_nn(dkvt_ref[:, oth], x_oth[...])).astype(BF)


def kvgrad(core, dkvt, x_own, x_oth):
    tokens, width = x_own.shape
    step = 512
    piece = pl.BlockSpec((tokens, step), lambda n, s: (0, n))
    return pl.pallas_call(
        kvgrad_kernel,
        grid_spec=pltpu.PrefetchScalarGridSpec(
            num_scalar_prefetch=1,
            grid=(width // step,),
            in_specs=[pl.BlockSpec((2 * HEAD, 2 * tokens), lambda n, s: (0, 0)), piece, piece],
            out_specs=pl.BlockSpec((2 * HEAD, step), lambda n, s: (0, n)),
        ),
        out_shape=jax.ShapeDtypeStruct((2 * HEAD, width), BF),
        compiler_params=params(),
        cost_estimate=cost(4 * tokens * width * 2 * HEAD, 4 * tokens * width),
        name="kvgrad",
    )(core, dkvt, x_own, x_oth)


def kv_combine_kernel(s_ref, a_ref, b_ref, c_ref, d_ref, gk_ref, gv_ref):
    for place, u_ref, v_ref in ((s_ref[0], a_ref, b_ref), (1 - s_ref[0], c_ref, d_ref)):
        total = u_ref[...].astype(F32) + v_ref[...].astype(F32)
        where = span(place, HEAD)
        gk_ref[:, where] = total[:HEAD, :].T
        gv_ref[:, where] = total[HEAD:, :].T


def kv_combine(core, parts):
    rows, width = parts[0].shape
    step = 512
    out = jax.ShapeDtypeStruct((width, rows), F32)
    return pl.pallas_call(
        kv_combine_kernel,
        grid_spec=pltpu.PrefetchScalarGridSpec(
            num_scalar_prefetch=1,
            grid=(width // step,),
            in_specs=[pl.BlockSpec((rows, step), lambda n, s: (0, n))] * 4,
            out_specs=[pl.BlockSpec((step, rows), lambda n, s: (n, 0))] * 2,
        ),
        out_shape=[out, out],
        compiler_params=params(),
        cost_estimate=cost(16 * width * rows * 16, 16 * width * rows),
        name="kv_combine",
    )(core, *parts)


def combine_kernel(s_ref, a_ref, b_ref, c_ref, d_ref, *rest):
    gq_ref, go_ref = rest[-2:]

    def put(u_ref, v_ref):
        gq_ref[...] = (u_ref[0].astype(F32) + v_ref[0].astype(F32)).T
        go_ref[...] = u_ref[1].astype(F32) + v_ref[1].astype(F32)

    @pl.when(pl.program_id(0) == 0)
    def _():
        put(a_ref, b_ref)

    @pl.when(pl.program_id(0) == 1)
    def _():
        put(c_ref, d_ref)


def combine(core, chunk, n_chunks, parts, prev):
    width = parts[0].shape[2]
    step = 512
    last = width // step - 1
    near = pl.BlockSpec((2, WIDE, step), lambda w, r, s: (0, 0, r + w * (last - r)))
    far = pl.BlockSpec((2, WIDE, step), lambda w, r, s: (0, 0, r * w))

    def place(w, s):
        return (s[0] + w - 2 * s[0] * w) * n_chunks + chunk

    shape = jax.ShapeDtypeStruct((width, 2 * n_chunks * WIDE), F32)
    shape_o = jax.ShapeDtypeStruct((2 * n_chunks * WIDE, width), F32)
    extra = [] if prev is None else list(prev)
    return pl.pallas_call(
        combine_kernel,
        grid_spec=pltpu.PrefetchScalarGridSpec(
            num_scalar_prefetch=1,
            grid=(2, width // step),
            in_specs=[near, near, far, far] + [pl.BlockSpec(memory_space=pl.ANY)] * len(extra),
            out_specs=[
                pl.BlockSpec((step, WIDE), lambda w, r, s: (r, place(w, s))),
                pl.BlockSpec((WIDE, step), lambda w, r, s: (place(w, s), r)),
            ],
        ),
        out_shape=[shape, shape_o],
        input_output_aliases={} if prev is None else {5: 0, 6: 1},
        compiler_params=params(),
        cost_estimate=cost(16 * width * WIDE * 64, 32 * width * WIDE),
        name="combine",
    )(core, *parts, *extra)


def fill_heads(core, own_refs, oth_refs, lhs):
    n = len(own_refs)
    for j in range(n):
        lhs[:, pl.ds(pl.multiple_of((core * n + j) * WIDE, WIDE), WIDE)] = own_refs[j][0]
        lhs[:, pl.ds(pl.multiple_of(((1 - core) * n + j) * WIDE, WIDE), WIDE)] = oth_refs[j][0]


def attn_out_kernel(n, s_ref, *refs):
    own_refs, oth_refs = refs[:n], refs[n:2 * n]
    wo_ref, out_ref, lhs = refs[2 * n:]

    @pl.when(pl.program_id(0) == 0)
    def _():
        fill_heads(s_ref[0], own_refs, oth_refs, lhs)

    out_ref[...] = dot_nn(lhs[...], wo_ref[...]).astype(BF)


def attn_out(core, own, oth, w_o):
    n = len(own)
    tokens = own[0].shape[1] // 2
    heads, width = w_o.shape
    step = 512
    return pl.pallas_call(
        functools.partial(attn_out_kernel, n),
        grid_spec=pltpu.PrefetchScalarGridSpec(
            num_scalar_prefetch=1,
            grid=(width // step,),
            in_specs=[pl.BlockSpec((1, tokens, WIDE), lambda k, s: (0, s[0], 0))] * (2 * n)
            + [pl.BlockSpec((heads, step), lambda k, s: (0, k))],
            out_specs=pl.BlockSpec((tokens, step), lambda k, s: (0, k)),
            scratch_shapes=[pltpu.VMEM((tokens, heads), BF)],
        ),
        out_shape=jax.ShapeDtypeStruct((tokens, width), BF),
        compiler_params=params(),
        cost_estimate=cost(2 * tokens * heads * width, 2 * heads * width + 4 * tokens * width),
        name="attn_out",
    )(core, *own, *oth, w_o)


def hidden_kernel(n, s_ref, *refs):
    own_refs, oth_refs = refs[:n], refs[n:2 * n]
    kv_own, kv_oth, wq_ref, wk_ref, wv_ref, out_ref, lhs, klhs, vlhs = refs[2 * n:]
    core = s_ref[0]

    @pl.when(pl.program_id(0) == 0)
    def _():
        fill_heads(core, own_refs, oth_refs, lhs)
        for place, ref in ((core, kv_own), (1 - core, kv_oth)):
            where = pl.ds(pl.multiple_of(place * HEAD, HEAD), HEAD)
            klhs[:, where] = ref[:, :HEAD]
            vlhs[:, where] = ref[:, HEAD:]

    out_ref[...] = (
        dot_nt(lhs[...], wq_ref[...]) + dot_nt(klhs[...], wk_ref[...]) + dot_nt(vlhs[...], wv_ref[...])
    ).astype(BF)


def grad_hidden(core, own, oth, kv_own, kv_oth, w_q, w_k, w_v):
    n = len(own)
    tokens = own[0].shape[1] // 2
    width, heads = w_q.shape
    kv_cols = w_k.shape[1]
    step = 512
    return pl.pallas_call(
        functools.partial(hidden_kernel, n),
        grid_spec=pltpu.PrefetchScalarGridSpec(
            num_scalar_prefetch=1,
            grid=(width // step,),
            in_specs=[pl.BlockSpec((1, tokens, WIDE), lambda k, s: (1, s[0], 0))] * (2 * n)
            + [pl.BlockSpec((tokens, 2 * HEAD), lambda k, s: (s[0], 0))] * 2
            + [
                pl.BlockSpec((step, heads), lambda k, s: (k, 0)),
                pl.BlockSpec((step, kv_cols), lambda k, s: (k, 0)),
                pl.BlockSpec((step, kv_cols), lambda k, s: (k, 0)),
            ],
            out_specs=pl.BlockSpec((tokens, step), lambda k, s: (0, k)),
            scratch_shapes=[
                pltpu.VMEM((tokens, heads), BF),
                pltpu.VMEM((tokens, kv_cols), BF),
                pltpu.VMEM((tokens, kv_cols), BF),
            ],
        ),
        out_shape=jax.ShapeDtypeStruct((tokens, width), BF),
        compiler_params=params(),
        cost_estimate=cost(2 * tokens * (heads + 2 * kv_cols) * width, 2 * heads * width + 4 * tokens * width),
        name="grad_hidden",
    )(core, *own, *oth, kv_own, kv_oth, w_q, w_k, w_v)


def solution(mesh):
    n_dev = mesh.shape["sp"]
    n_chunks = 4
    near_perm = [(d, d ^ 1) for d in range(n_dev)]
    far_perm = [(d, d ^ 2) for d in range(n_dev)]
    down_perm = [(0, 2), (1, 3)]
    up_perm = [(2, 0), (3, 1)]

    def near(v):
        return lax.ppermute(v, "sp", near_perm)

    def far(v):
        return lax.ppermute(v, "sp", far_perm)

    def device_step(hidden, grad_out, positions, doc_ids, w_q, w_k, w_v, w_o):
        tokens = hidden.shape[0]
        chip_len = 2 * tokens
        assert n_chunks == w_q.shape[1] // (2 * WIDE)
        place = lax.axis_index("sp")
        core_id, chip_id = place & 1, place >> 1
        core = core_id.astype(jnp.int32)[None]
        sel_own = jnp.stack([core_id, core_id]).astype(jnp.int32)
        sel_oth = jnp.stack([core_id, 1 - core_id]).astype(jnp.int32)

        doc_oth = near(doc_ids)
        x_oth = near(hidden)
        g_oth = near(grad_out)
        tab_own = rope_table(positions)
        tab_oth = near(tab_own)
        kv_own, q = qkv_proj(sel_own, hidden, w_q, w_k, w_v, tab_own, None)
        kvp_own = lax.ppermute(kv_own, "sp", down_perm)
        doc_chip = jnp.where(
            core_id == 0, jnp.concatenate([doc_ids, doc_oth]), jnp.concatenate([doc_oth, doc_ids])
        )
        doc_far = far(doc_chip)
        kv_oth, q = qkv_proj(sel_oth, x_oth, w_q, w_k, w_v, tab_oth, q)
        kvp_oth = lax.ppermute(kv_oth, "sp", down_perm)
        dctx = dctx_proj(core, grad_out, g_oth, w_o)

        heads_doc = doc_chip[::BQ]
        lo = jnp.sum(doc_chip[None, :] < heads_doc[:, None], axis=1, dtype=jnp.int32)
        lo_far = jnp.sum(doc_far[None, :] < heads_doc[:, None], axis=1, dtype=jnp.int32)
        lo = lo + jnp.where(chip_id == 0, chip_len, lo_far)
        lo = (lo >> (ALIGN.bit_length() - 1)) << (ALIGN.bit_length() - 1)
        end = chip_len + BQ * (1 + jnp.arange(chip_len // BQ, dtype=jnp.int32))
        n_blocks = (end - lo + BK - 1) >> (BK.bit_length() - 1)
        kdoc = jnp.concatenate([doc_far, doc_chip, jnp.zeros((BK,), jnp.int32)])[None, :]

        acts, acts_oth, dkvs, sums = [], [], [], None
        for j in range(n_chunks):
            act, part, dkv = attention(
                j, core, lo, n_blocks, q, dctx, kdoc, (tab_own, tab_oth), (kvp_own, kvp_oth), (kv_own, kv_oth),
                (hidden, x_oth), (grad_out, g_oth),
            )
            part = part.reshape(2, WIDE, -1)
            acts.append(act)
            dkvs.append(dkv.reshape(2, 2, HEAD, chip_len))
            if j == n_chunks - 1:
                dkv_up = sum(d[:, 0].astype(F32) for d in dkvs).astype(BF)
                dkv_far = lax.ppermute(dkv_up, "sp", up_perm)
            acts_oth.append(near(act))
            part_far = far(part)
            part_near = near(part)
            part_far_near = near(part_far)
            sums = combine(core, j, n_chunks, (part, part_far, part_near, part_far_near), sums)
        grad_wq, grad_wo = sums

        dkv, dkvt = kv_finish(core, dkvs, dkv_far, tab_own, tab_oth)
        dkv_oth = near(dkv)
        kv_part = kvgrad(core, dkvt, hidden, x_oth)
        kv_part_far = far(kv_part)
        kv_part_near = near(kv_part)
        kv_part_far_near = near(kv_part_far)
        grad_wk, grad_wv = kv_combine(core, (kv_part, kv_part_far, kv_part_near, kv_part_far_near))
        out = attn_out(core, acts, acts_oth, w_o)
        g_hidden = grad_hidden(core, acts, acts_oth, dkv, dkv_oth, w_q, w_k, w_v)
        return out, g_hidden, grad_wq, grad_wk, grad_wv, grad_wo

    tok_spec = P(("dp", "sp"), None)
    vec_spec = P(("dp", "sp"))
    rep_spec = P(None, None)
    part_spec = P("dp", None)


    return jax.shard_map(
        device_step,
        mesh=mesh,
        in_specs=(tok_spec, tok_spec, vec_spec, vec_spec, rep_spec, rep_spec, rep_spec, rep_spec),
        out_specs=(tok_spec, tok_spec, part_spec, part_spec, part_spec, part_spec),
        check_vma=False,
    )
```

```python
import functools

import jax
import jax.numpy as jnp
from jax import lax
from jax.experimental import pallas as pl
from jax.experimental.pallas import tpu as pltpu
from jax.sharding import PartitionSpec as P

HEAD = 128
ROPE_THETA = 500000.0
ROPE_FACTOR = 8.0
ROPE_LOW = 1.0
ROPE_HIGH = 4.0
ROPE_OLD_CTX = 8192.0
NEG_BIG = -1.0e30
SCALE = HEAD ** -0.5
LOG2E = 1.4426950408889634

PAIR = 2
WIDE = PAIR * HEAD
BQ = 512
BK = 512
ALIGN = 128
BF = jnp.bfloat16
F32 = jnp.float32


def rope_freqs():
    half_idx = jnp.arange(HEAD // 2, dtype=F32)
    inv_freq = jnp.power(ROPE_THETA, -2.0 * half_idx / HEAD)
    wavelen = 2.0 * jnp.pi / inv_freq
    smooth = (ROPE_OLD_CTX / wavelen - ROPE_LOW) / (ROPE_HIGH - ROPE_LOW)
    mixed_freq = (1.0 - smooth) * inv_freq / ROPE_FACTOR + smooth * inv_freq
    scaled = jnp.where(wavelen > ROPE_OLD_CTX / ROPE_LOW, inv_freq / ROPE_FACTOR, mixed_freq)
    return jnp.where(wavelen < ROPE_OLD_CTX / ROPE_HIGH, inv_freq, scaled)


def rope_table(pos_vec):
    angles = pos_vec.astype(F32)[:, None] * rope_freqs()[None, :]
    return jnp.concatenate([jnp.cos(angles), jnp.sin(angles)], axis=-1)


def dot_nn(a, b):
    return lax.dot_general(a, b, (((1,), (0,)), ((), ())), preferred_element_type=F32)


def dot_nt(a, b):
    return lax.dot_general(a, b, (((1,), (1,)), ((), ())), preferred_element_type=F32)


def swap_halves(v):
    return pltpu.roll(v, HEAD // 2, 1)


def spread_table(tab):
    low = lax.broadcasted_iota(jnp.int32, tab.shape, 1) < HEAD // 2
    other = swap_halves(tab)
    return jnp.where(low, tab, other), jnp.where(low, -other, tab)


def cost(flops, nbytes, trans=0):
    return pl.CostEstimate(flops=int(flops), bytes_accessed=int(nbytes), transcendentals=int(trans))


def params(**kw):
    return pltpu.CompilerParams(vmem_limit_bytes=67_000_000, **kw)


def by_rows(rows, body, size=16):
    def step(r, carry):
        body(span(r, size))
        return carry

    lax.fori_loop(0, rows // size, step, 0)


def span(index, size):
    return pl.ds(pl.multiple_of(index * size, size), size)


def qkv_kernel(s_ref, x_ref, wq_ref, wk_ref, wv_ref, tab_ref, *rest):
    kv_ref, q_ref, w_s = rest[-3:]

    @pl.when(pl.program_id(0) == 0)
    def _():
        w_s[:, :HEAD] = wk_ref[...]
        w_s[:, HEAD:] = wv_ref[...]

    x = x_ref[...]
    cos_t, sin_t = spread_table(tab_ref[...])
    kv = dot_nn(x, w_s[...])
    k = kv[:, :HEAD]
    kv_ref[:, :HEAD] = (k * cos_t + swap_halves(k) * sin_t).astype(BF)
    kv_ref[:, HEAD:] = kv[:, HEAD:].astype(BF)
    step = 4 * HEAD
    for n in range(wq_ref.shape[1] // step):
        q = dot_nn(x, wq_ref[:, n * step:(n + 1) * step])
        for h in range(step // HEAD):
            part = q[:, h * HEAD:(h + 1) * HEAD]
            at = n * step + h * HEAD
            q_ref[:, at:at + HEAD] = (part * cos_t + swap_halves(part) * sin_t).astype(BF)


def qkv_proj(sel, x, w_q, w_k, w_v, tab, prev):
    tokens, width = x.shape
    cols = w_q.shape[1] // 2
    rows = tokens // 2
    extra = [] if prev is None else [prev]
    return pl.pallas_call(
        qkv_kernel,
        grid_spec=pltpu.PrefetchScalarGridSpec(
            num_scalar_prefetch=1,
            grid=(2,),
            in_specs=[
                pl.BlockSpec((rows, width), lambda m, s: (m, 0)),
                pl.BlockSpec((width, cols), lambda m, s: (0, s[0])),
                pl.BlockSpec((width, HEAD), lambda m, s: (0, s[0])),
                pl.BlockSpec((width, HEAD), lambda m, s: (0, s[0])),
                pl.BlockSpec((rows, HEAD), lambda m, s: (m, 0)),
            ] + [pl.BlockSpec(memory_space=pl.ANY)] * len(extra),
            out_specs=[
                pl.BlockSpec((rows, 2 * HEAD), lambda m, s: (m, 0)),
                pl.BlockSpec((rows, cols), lambda m, s: (s[1] * 2 + m, 0)),
            ],
            scratch_shapes=[pltpu.VMEM((width, 2 * HEAD), BF)],
        ),
        out_shape=[
            jax.ShapeDtypeStruct((tokens, 2 * HEAD), BF),
            jax.ShapeDtypeStruct((2 * tokens, cols), BF),
        ],
        input_output_aliases={} if prev is None else {6: 1},
        compiler_params=params(),
        cost_estimate=cost(2 * tokens * width * (cols + 2 * HEAD), tokens * width * 2 + cols * width * 2),
        name="qkv_proj",
    )(sel, x, w_q, w_k, w_v, tab, *extra)


def dctx_kernel(s_ref, own_ref, oth_ref, wo_ref, out_ref):
    def put(ref):
        step = 4 * HEAD
        for n in range(wo_ref.shape[0] // step):
            out_ref[:, n * step:(n + 1) * step] = dot_nt(ref[...], wo_ref[n * step:(n + 1) * step, :]).astype(BF)

    @pl.when(pl.program_id(0) < 2)
    def _():
        put(own_ref)

    @pl.when(pl.program_id(0) >= 2)
    def _():
        put(oth_ref)


def dctx_proj(core, own, oth, w_o):
    tokens, width = own.shape
    cols = w_o.shape[0] // 2
    rows = tokens // 2

    def place(m, s):
        far = m // 2
        return (s[0] + far - 2 * s[0] * far) * 2 + m % 2

    return pl.pallas_call(
        dctx_kernel,
        grid_spec=pltpu.PrefetchScalarGridSpec(
            num_scalar_prefetch=1,
            grid=(4,),
            in_specs=[
                pl.BlockSpec((rows, width), lambda m, s: (jnp.minimum(m, 1), 0)),
                pl.BlockSpec((rows, width), lambda m, s: (jnp.maximum(m - 2, 0), 0)),
                pl.BlockSpec((cols, width), lambda m, s: (s[0], 0)),
            ],
            out_specs=pl.BlockSpec((rows, cols), lambda m, s: (place(m, s), 0)),
        ),
        out_shape=jax.ShapeDtypeStruct((2 * tokens, cols), BF),
        compiler_params=params(),
        cost_estimate=cost(4 * tokens * width * cols, tokens * width * 4 + cols * width * 2),
        name="dctx_proj",
    )(core, own, oth, w_o)


def attn_kernel(
    core_ref, lo_ref, nb_ref, q_ref, do_ref, kdoc_ref, tab_own, tab_oth, kvp_own, kvp_oth, kvc_own, kvc_oth,
    x_own, x_oth, g_own, g_oth, act_ref, part_ref, dkv_ref,
    k_s, v_s, s_s, dp_s, m_s, l_s, d_s, qd_s, ctx_s, dq_s, q_s, do_s, qt_s, dot_s, tab_s, dk_s, dv_s,
    x_s, g_s, at_s, w_s, init_sem, row_sem, out_sem,
):
    i = pl.program_id(0)
    tokens = kvc_own.shape[0]
    chip_len = 2 * tokens
    core = core_ref[0]
    per_half = tokens // BQ
    rows_here = span(i % per_half, BQ)

    def row_copies(x, g):
        return (
            pltpu.make_async_copy(x.at[rows_here, :], x_s, row_sem.at[0]),
            pltpu.make_async_copy(g.at[rows_here, :], g_s, row_sem.at[1]),
        )

    def init_copies():
        moves = []
        for base, place, ref in ((0, core, kvp_own), (0, 1 - core, kvp_oth), (2, core, kvc_own), (2, 1 - core, kvc_oth)):
            moves.append((ref.at[:, pl.ds(0, HEAD)], k_s.at[span(base + place, tokens), :]))
        for base, place, ref in ((0, core, kvp_own), (0, 1 - core, kvp_oth), (2, core, kvc_own), (2, 1 - core, kvc_oth)):
            moves.append((ref.at[:, pl.ds(HEAD, HEAD)], v_s.at[span(base + place, tokens), :]))
        moves.append((tab_own, tab_s.at[span(core, tokens), :]))
        moves.append((tab_oth, tab_s.at[span(1 - core, tokens), :]))
        return [pltpu.make_async_copy(src, dst, init_sem.at[n]) for n, (src, dst) in enumerate(moves)]

    def arrive(first, last):
        @pl.when(i == 0)
        def _():
            for copy in init_copies()[first:last]:
                copy.wait()

    @pl.when(i == 0)
    def _():
        for copy in init_copies():
            copy.start()
        k_s[2 * chip_len:, :] = jnp.zeros((BK, HEAD), BF)
        v_s[2 * chip_len:, :] = jnp.zeros((BK, HEAD), BF)

        def clear(r):
            w_s[r, :] = jnp.zeros((16, w_s.shape[1]), F32)

        def clear_kv(r):
            dk_s[r, :] = jnp.zeros((16, dk_s.shape[1]), F32)
            dv_s[r, :] = jnp.zeros((16, dv_s.shape[1]), F32)

        by_rows(w_s.shape[0], clear)
        by_rows(HEAD, clear_kv)

    @pl.when(i // per_half == core)
    def _():
        for copy in row_copies(x_own, g_own):
            copy.start()

    @pl.when(i // per_half != core)
    def _():
        for copy in row_copies(x_oth, g_oth):
            copy.start()

    for h in range(PAIR):
        rows = slice(h * BQ, (h + 1) * BQ)
        cols = slice(h * HEAD, (h + 1) * HEAD)
        q_s[rows, :] = q_ref[:, cols]
        do_s[rows, :] = do_ref[:, cols]
        qt_s[:, rows] = q_ref[:, cols].T
        dot_s[:, rows] = do_ref[:, cols].T
    qdoc = kdoc_ref[:, pl.ds(pl.multiple_of(chip_len + i * BQ, BQ), BQ)]
    qd_s[...] = jnp.broadcast_to(qdoc, (HEAD, BQ)).T
    m_s[...] = jnp.full(m_s.shape, NEG_BIG, F32)
    l_s[...] = jnp.zeros(l_s.shape, F32)
    d_s[...] = jnp.zeros(d_s.shape, F32)
    ctx_s[...] = jnp.zeros(ctx_s.shape, F32)
    dq_s[...] = jnp.zeros(dq_s.shape, F32)
    lo = lo_ref[i]
    n_blocks = nb_ref[i]
    lanes = BK // HEAD

    def fold(v, op):
        out = v[:, :HEAD]
        for n in range(1, lanes):
            out = op(out, v[:, n * HEAD:(n + 1) * HEAD])
        return out

    def spread(v):
        return jnp.concatenate([v] * lanes, axis=1)

    def offset(b):
        return pl.multiple_of(lo + b * BK, ALIGN)

    def scores(b, carry):
        off = offset(b)
        s = dot_nt(q_s[...], k_s[pl.ds(off, BK), :])
        key = off + lax.broadcasted_iota(jnp.int32, (BQ, BK), 1)
        query = chip_len + i * BQ + lax.broadcasted_iota(jnp.int32, (BQ, BK), 0)
        keep = (key <= query) & (kdoc_ref[:, pl.ds(off, BK)] == spread(qd_s[...]))
        for h in range(PAIR):
            rows = slice(h * BQ, (h + 1) * BQ)
            sh = jnp.where(keep, s[rows, :], NEG_BIG)
            s_s[b, rows, :] = sh
            m_s[rows, :] = jnp.maximum(m_s[rows, :], fold(sh, jnp.maximum))
        return carry

    arrive(0, 4)
    lax.fori_loop(0, n_blocks, scores, 0)
    m_s[...] = jnp.broadcast_to(jnp.max(m_s[...], axis=1, keepdims=True), m_s.shape)

    def weights(b, carry):
        dp = dot_nt(do_s[...], v_s[pl.ds(offset(b), BK), :])
        e = jnp.exp2((s_s[b] - spread(m_s[...])) * (SCALE * LOG2E))
        s_s[b] = e
        dp_s[b] = dp
        l_s[...] += fold(e, jnp.add)
        d_s[...] += fold(e * dp, jnp.add)
        return carry

    arrive(4, 10)
    lax.fori_loop(0, n_blocks, weights, 0)
    inv = 1.0 / jnp.sum(l_s[...], axis=1, keepdims=True)
    delta = jnp.sum(d_s[...], axis=1, keepdims=True) * inv
    l_s[...] = jnp.broadcast_to(inv, l_s.shape)
    d_s[...] = jnp.broadcast_to(delta, d_s.shape)

    def grads(b, carry):
        off = offset(b)
        p = s_s[b] * spread(l_s[...])
        pb = p.astype(BF)
        ds = (p * (dp_s[b] - spread(d_s[...])) * SCALE).astype(BF)
        ctx_s[...] += dot_nn(pb, v_s[pl.ds(off, BK), :])
        dq_s[...] += dot_nn(ds, k_s[pl.ds(off, BK), :])
        dv_s[:, pl.ds(off, BK)] += dot_nn(dot_s[...], pb)
        dk_s[:, pl.ds(off, BK)] += dot_nn(qt_s[...], ds)
        return carry

    lax.fori_loop(0, n_blocks, grads, 0)
    cos_t, sin_t = spread_table(tab_s[span(i, BQ), :])
    for h in range(PAIR):
        rows = slice(h * BQ, (h + 1) * BQ)
        cols = slice(h * HEAD, (h + 1) * HEAD)
        ctx = ctx_s[rows, :].astype(BF)
        act_ref[0, :, cols] = ctx
        at_s[WIDE + h * HEAD:WIDE + (h + 1) * HEAD, :] = ctx.T
        dq = dq_s[rows, :].astype(BF).astype(F32)
        dq = (dq * cos_t - swap_halves(dq) * sin_t).astype(BF)
        act_ref[1, :, cols] = dq
        at_s[h * HEAD:(h + 1) * HEAD, :] = dq.T
    step = 4 * HEAD
    for copy in row_copies(x_own, g_own):
        copy.wait()

    def products(c, carry):
        cols = span(c, step)
        w_s[:WIDE, cols] += dot_nn(at_s[:WIDE, :], x_s[:, cols])
        w_s[WIDE:, cols] += dot_nn(at_s[WIDE:, :], g_s[:, cols])
        return carry

    lax.fori_loop(0, x_s.shape[1] // step, products, 0)

    @pl.when(i == pl.num_programs(0) - 1)
    def _():
        def narrow(r):
            x_s[r, :] = w_s[r, :].astype(BF)

        by_rows(w_s.shape[0], narrow)
        part_copy = pltpu.make_async_copy(x_s, part_ref, out_sem.at[0])
        part_copy.start()

        def narrow_kv(r, carry):
            rows = span(r, 16)
            for n, acc in enumerate((dk_s, dv_s)):
                for side in range(2):
                    at = pl.ds(pl.multiple_of((2 * n + side) * HEAD + r * 16, 16), 16)
                    g_s[at, :] = acc[rows, side * chip_len:(side + 1) * chip_len].astype(BF)
            return carry

        lax.fori_loop(0, HEAD // 16, narrow_kv, 0)
        dkv_copy = pltpu.make_async_copy(g_s, dkv_ref, out_sem.at[1])
        dkv_copy.start()
        part_copy.wait()
        dkv_copy.wait()


def attention(chunk, core, lo, n_blocks, q, dctx, kdoc, tabs, kv_prev, kv_chip, xs, gs):
    chip_len = q.shape[0]
    width = xs[0].shape[1]
    assert 2 * WIDE == BQ == 4 * HEAD and width == chip_len
    padded = 2 * chip_len + BK
    max_blocks = 2 * chip_len // BK
    rows = PAIR * BQ
    full = lambda shape: pl.BlockSpec(shape, lambda i, *s: (0,) * len(shape))
    pairs = chip_len * chip_len * PAIR
    return pl.pallas_call(
        attn_kernel,
        grid_spec=pltpu.PrefetchScalarGridSpec(
            num_scalar_prefetch=3,
            grid=(chip_len // BQ,),
            in_specs=[
                pl.BlockSpec((BQ, WIDE), lambda i, *s: (i, chunk)),
                pl.BlockSpec((BQ, WIDE), lambda i, *s: (i, chunk)),
                full((1, padded)),
            ] + [pl.BlockSpec(memory_space=pl.ANY)] * 10,
            out_specs=[
                pl.BlockSpec((2, BQ, WIDE), lambda i, *s: (0, i, 0)),
                pl.BlockSpec(memory_space=pl.ANY),
                pl.BlockSpec(memory_space=pl.ANY),
            ],
            scratch_shapes=[
                pltpu.VMEM((padded, HEAD), BF),
                pltpu.VMEM((padded, HEAD), BF),
                pltpu.VMEM((max_blocks, rows, BK), F32),
                pltpu.VMEM((max_blocks, rows, BK), F32),
                pltpu.VMEM((rows, HEAD), F32),
                pltpu.VMEM((rows, HEAD), F32),
                pltpu.VMEM((rows, HEAD), F32),
                pltpu.VMEM((BQ, HEAD), jnp.int32),
                pltpu.VMEM((rows, HEAD), F32),
                pltpu.VMEM((rows, HEAD), F32),
                pltpu.VMEM((rows, HEAD), BF),
                pltpu.VMEM((rows, HEAD), BF),
                pltpu.VMEM((HEAD, rows), BF),
                pltpu.VMEM((HEAD, rows), BF),
                pltpu.VMEM((chip_len, HEAD), F32),
                pltpu.VMEM((HEAD, padded), F32),
                pltpu.VMEM((HEAD, padded), F32),
                pltpu.VMEM((BQ, width), BF),
                pltpu.VMEM((BQ, width), BF),
                pltpu.VMEM((2 * WIDE, BQ), BF),
                pltpu.VMEM((2 * WIDE, width), F32),
                pltpu.SemaphoreType.DMA((10,)),
                pltpu.SemaphoreType.DMA((2,)),
                pltpu.SemaphoreType.DMA((2,)),
            ],
        ),
        out_shape=[
            jax.ShapeDtypeStruct((2, chip_len, WIDE), BF),
            jax.ShapeDtypeStruct((2 * WIDE, width), BF),
            jax.ShapeDtypeStruct((4 * HEAD, chip_len), BF),
        ],
        compiler_params=params(),
        cost_estimate=cost(pairs * HEAD * 2 * 8, 12 * 1024 * 1024, pairs),
        name="attention",
    )(core, lo, n_blocks, q, dctx, kdoc, *tabs, *kv_prev, *kv_chip, *xs, *gs)


def kv_finish_kernel(n, s_ref, *refs):
    far_ref, tab_own, tab_oth, out_ref, outt_ref, tab_s = refs[n:]
    tokens = tab_own.shape[0]
    step = out_ref.shape[0]

    @pl.when(pl.program_id(0) == 0)
    def _():
        tab_s[span(s_ref[0], tokens), :] = tab_own[...]
        tab_s[span(1 - s_ref[0], tokens), :] = tab_oth[...]

    total = far_ref[...].astype(F32)
    for ref in refs[:n]:
        total = total + ref[:, 0].astype(F32)
    cos_t, sin_t = spread_table(tab_s[span(pl.program_id(0), step), :])
    dk = total[0].astype(BF).astype(F32).T
    dk = (dk * cos_t - swap_halves(dk) * sin_t).astype(BF)
    dvt = total[1].astype(BF)
    out_ref[:, :HEAD] = dk
    out_ref[:, HEAD:] = dvt.T
    outt_ref[:HEAD, :] = dk.T
    outt_ref[HEAD:, :] = dvt


def kv_finish(core, parts, far, tab_own, tab_oth):
    tokens = tab_own.shape[0]
    chip_len = 2 * tokens
    step = 512
    return pl.pallas_call(
        functools.partial(kv_finish_kernel, len(parts)),
        grid_spec=pltpu.PrefetchScalarGridSpec(
            num_scalar_prefetch=1,
            grid=(chip_len // step,),
            in_specs=[pl.BlockSpec((2, 1, HEAD, step), lambda t, s: (0, 1, 0, t))] * len(parts)
            + [
                pl.BlockSpec((2, HEAD, step), lambda t, s: (0, 0, t)),
                pl.BlockSpec((tokens, HEAD), lambda t, s: (0, 0)),
                pl.BlockSpec((tokens, HEAD), lambda t, s: (0, 0)),
            ],
            out_specs=[
                pl.BlockSpec((step, 2 * HEAD), lambda t, s: (t, 0)),
                pl.BlockSpec((2 * HEAD, step), lambda t, s: (0, t)),
            ],
            scratch_shapes=[pltpu.VMEM((chip_len, HEAD), F32)],
        ),
        out_shape=[
            jax.ShapeDtypeStruct((chip_len, 2 * HEAD), BF),
            jax.ShapeDtypeStruct((2 * HEAD, chip_len), BF),
        ],
        compiler_params=params(),
        cost_estimate=cost(chip_len * HEAD * 64, chip_len * HEAD * 16),
        name="kv_finish",
    )(core, *parts, far, tab_own, tab_oth)


def kvgrad_kernel(s_ref, dkvt_ref, x_own, x_oth, out_ref):
    tokens = x_own.shape[0]
    own, oth = span(s_ref[0], tokens), span(1 - s_ref[0], tokens)
    out_ref[...] = (dot_nn(dkvt_ref[:, own], x_own[...]) + dot_nn(dkvt_ref[:, oth], x_oth[...])).astype(BF)


def kvgrad(core, dkvt, x_own, x_oth):
    tokens, width = x_own.shape
    step = 512
    piece = pl.BlockSpec((tokens, step), lambda n, s: (0, n))
    return pl.pallas_call(
        kvgrad_kernel,
        grid_spec=pltpu.PrefetchScalarGridSpec(
            num_scalar_prefetch=1,
            grid=(width // step,),
            in_specs=[pl.BlockSpec((2 * HEAD, 2 * tokens), lambda n, s: (0, 0)), piece, piece],
            out_specs=pl.BlockSpec((2 * HEAD, step), lambda n, s: (0, n)),
        ),
        out_shape=jax.ShapeDtypeStruct((2 * HEAD, width), BF),
        compiler_params=params(),
        cost_estimate=cost(4 * tokens * width * 2 * HEAD, 4 * tokens * width),
        name="kvgrad",
    )(core, dkvt, x_own, x_oth)


def kv_combine_kernel(s_ref, a_ref, b_ref, c_ref, d_ref, gk_ref, gv_ref):
    for place, u_ref, v_ref in ((s_ref[0], a_ref, b_ref), (1 - s_ref[0], c_ref, d_ref)):
        total = u_ref[...].astype(F32) + v_ref[...].astype(F32)
        where = span(place, HEAD)
        gk_ref[:, where] = total[:HEAD, :].T
        gv_ref[:, where] = total[HEAD:, :].T


def kv_combine(core, parts):
    rows, width = parts[0].shape
    step = 512
    out = jax.ShapeDtypeStruct((width, rows), F32)
    return pl.pallas_call(
        kv_combine_kernel,
        grid_spec=pltpu.PrefetchScalarGridSpec(
            num_scalar_prefetch=1,
            grid=(width // step,),
            in_specs=[pl.BlockSpec((rows, step), lambda n, s: (0, n))] * 4,
            out_specs=[pl.BlockSpec((step, rows), lambda n, s: (n, 0))] * 2,
        ),
        out_shape=[out, out],
        compiler_params=params(),
        cost_estimate=cost(16 * width * rows * 16, 16 * width * rows),
        name="kv_combine",
    )(core, *parts)


def combine_kernel(s_ref, a_ref, b_ref, c_ref, d_ref, *rest):
    gq_ref, go_ref = rest[-2:]

    def put(u_ref, v_ref):
        gq_ref[...] = (u_ref[0].astype(F32) + v_ref[0].astype(F32)).T
        go_ref[...] = u_ref[1].astype(F32) + v_ref[1].astype(F32)

    @pl.when(pl.program_id(0) == 0)
    def _():
        put(a_ref, b_ref)

    @pl.when(pl.program_id(0) == 1)
    def _():
        put(c_ref, d_ref)


def combine(core, chunk, n_chunks, parts, prev):
    width = parts[0].shape[2]
    step = 512
    last = width // step - 1
    near = pl.BlockSpec((2, WIDE, step), lambda w, r, s: (0, 0, r + w * (last - r)))
    far = pl.BlockSpec((2, WIDE, step), lambda w, r, s: (0, 0, r * w))

    def place(w, s):
        return (s[0] + w - 2 * s[0] * w) * n_chunks + chunk

    shape = jax.ShapeDtypeStruct((width, 2 * n_chunks * WIDE), F32)
    shape_o = jax.ShapeDtypeStruct((2 * n_chunks * WIDE, width), F32)
    extra = [] if prev is None else list(prev)
    return pl.pallas_call(
        combine_kernel,
        grid_spec=pltpu.PrefetchScalarGridSpec(
            num_scalar_prefetch=1,
            grid=(2, width // step),
            in_specs=[near, near, far, far] + [pl.BlockSpec(memory_space=pl.ANY)] * len(extra),
            out_specs=[
                pl.BlockSpec((step, WIDE), lambda w, r, s: (r, place(w, s))),
                pl.BlockSpec((WIDE, step), lambda w, r, s: (place(w, s), r)),
            ],
        ),
        out_shape=[shape, shape_o],
        input_output_aliases={} if prev is None else {5: 0, 6: 1},
        compiler_params=params(),
        cost_estimate=cost(16 * width * WIDE * 64, 32 * width * WIDE),
        name="combine",
    )(core, *parts, *extra)


def fill_heads(core, own_refs, oth_refs, lhs):
    n = len(own_refs)
    for j in range(n):
        lhs[:, pl.ds(pl.multiple_of((core * n + j) * WIDE, WIDE), WIDE)] = own_refs[j][0]
        lhs[:, pl.ds(pl.multiple_of(((1 - core) * n + j) * WIDE, WIDE), WIDE)] = oth_refs[j][0]


def attn_out_kernel(n, s_ref, *refs):
    own_refs, oth_refs = refs[:n], refs[n:2 * n]
    wo_ref, out_ref, lhs = refs[2 * n:]

    @pl.when(pl.program_id(0) == 0)
    def _():
        fill_heads(s_ref[0], own_refs, oth_refs, lhs)

    out_ref[...] = dot_nn(lhs[...], wo_ref[...]).astype(BF)


def attn_out(core, own, oth, w_o):
    n = len(own)
    tokens = own[0].shape[1] // 2
    heads, width = w_o.shape
    step = 512
    return pl.pallas_call(
        functools.partial(attn_out_kernel, n),
        grid_spec=pltpu.PrefetchScalarGridSpec(
            num_scalar_prefetch=1,
            grid=(width // step,),
            in_specs=[pl.BlockSpec((1, tokens, WIDE), lambda k, s: (0, s[0], 0))] * (2 * n)
            + [pl.BlockSpec((heads, step), lambda k, s: (0, k))],
            out_specs=pl.BlockSpec((tokens, step), lambda k, s: (0, k)),
            scratch_shapes=[pltpu.VMEM((tokens, heads), BF)],
        ),
        out_shape=jax.ShapeDtypeStruct((tokens, width), BF),
        compiler_params=params(),
        cost_estimate=cost(2 * tokens * heads * width, 2 * heads * width + 4 * tokens * width),
        name="attn_out",
    )(core, *own, *oth, w_o)


def hidden_kernel(n, s_ref, *refs):
    own_refs, oth_refs = refs[:n], refs[n:2 * n]
    kv_own, kv_oth, wq_ref, wk_ref, wv_ref, out_ref, lhs, klhs, vlhs = refs[2 * n:]
    core = s_ref[0]

    @pl.when(pl.program_id(0) == 0)
    def _():
        fill_heads(core, own_refs, oth_refs, lhs)
        for place, ref in ((core, kv_own), (1 - core, kv_oth)):
            where = pl.ds(pl.multiple_of(place * HEAD, HEAD), HEAD)
            klhs[:, where] = ref[:, :HEAD]
            vlhs[:, where] = ref[:, HEAD:]

    out_ref[...] = (
        dot_nt(lhs[...], wq_ref[...]) + dot_nt(klhs[...], wk_ref[...]) + dot_nt(vlhs[...], wv_ref[...])
    ).astype(BF)


def grad_hidden(core, own, oth, kv_own, kv_oth, w_q, w_k, w_v):
    n = len(own)
    tokens = own[0].shape[1] // 2
    width, heads = w_q.shape
    kv_cols = w_k.shape[1]
    step = 512
    return pl.pallas_call(
        functools.partial(hidden_kernel, n),
        grid_spec=pltpu.PrefetchScalarGridSpec(
            num_scalar_prefetch=1,
            grid=(width // step,),
            in_specs=[pl.BlockSpec((1, tokens, WIDE), lambda k, s: (1, s[0], 0))] * (2 * n)
            + [pl.BlockSpec((tokens, 2 * HEAD), lambda k, s: (s[0], 0))] * 2
            + [
                pl.BlockSpec((step, heads), lambda k, s: (k, 0)),
                pl.BlockSpec((step, kv_cols), lambda k, s: (k, 0)),
                pl.BlockSpec((step, kv_cols), lambda k, s: (k, 0)),
            ],
            out_specs=pl.BlockSpec((tokens, step), lambda k, s: (0, k)),
            scratch_shapes=[
                pltpu.VMEM((tokens, heads), BF),
                pltpu.VMEM((tokens, kv_cols), BF),
                pltpu.VMEM((tokens, kv_cols), BF),
            ],
        ),
        out_shape=jax.ShapeDtypeStruct((tokens, width), BF),
        compiler_params=params(),
        cost_estimate=cost(2 * tokens * (heads + 2 * kv_cols) * width, 2 * heads * width + 4 * tokens * width),
        name="grad_hidden",
    )(core, *own, *oth, kv_own, kv_oth, w_q, w_k, w_v)


def solution(mesh):
    n_dev = mesh.shape["sp"]
    n_chunks = 4
    near_perm = [(d, d ^ 1) for d in range(n_dev)]
    far_perm = [(d, d ^ 2) for d in range(n_dev)]
    down_perm = [(0, 2), (1, 3)]
    up_perm = [(2, 0), (3, 1)]

    def near(v):
        return lax.ppermute(v, "sp", near_perm)

    def far(v):
        return lax.ppermute(v, "sp", far_perm)

    def device_step(hidden, grad_out, positions, doc_ids, w_q, w_k, w_v, w_o):
        tokens = hidden.shape[0]
        chip_len = 2 * tokens
        assert n_chunks == w_q.shape[1] // (2 * WIDE)
        place = lax.axis_index("sp")
        core_id, chip_id = place & 1, place >> 1
        core = core_id.astype(jnp.int32)[None]
        sel_own = jnp.stack([core_id, core_id]).astype(jnp.int32)
        sel_oth = jnp.stack([core_id, 1 - core_id]).astype(jnp.int32)

        doc_oth = near(doc_ids)
        doc_far = far(doc_ids)
        doc_far_oth = lax.ppermute(doc_ids, "sp", [(d, d ^ 3) for d in range(n_dev)])
        x_oth = near(hidden)
        g_oth = near(grad_out)
        tab_own = rope_table(positions)
        tab_oth = near(tab_own)
        kv_own, q = qkv_proj(sel_own, hidden, w_q, w_k, w_v, tab_own, None)
        kvp_own = lax.ppermute(kv_own, "sp", down_perm)

        def in_order(own, oth):
            return jnp.where(core_id == 0, jnp.concatenate([own, oth]), jnp.concatenate([oth, own]))

        doc_chip, doc_far = in_order(doc_ids, doc_oth), in_order(doc_far, doc_far_oth)
        kv_oth, q = qkv_proj(sel_oth, x_oth, w_q, w_k, w_v, tab_oth, q)
        kvp_oth = lax.ppermute(kv_oth, "sp", down_perm)
        dctx = dctx_proj(core, grad_out, g_oth, w_o)

        heads_doc = doc_chip[::BQ]
        lo = jnp.sum(doc_chip[None, :] < heads_doc[:, None], axis=1, dtype=jnp.int32)
        lo_far = jnp.sum(doc_far[None, :] < heads_doc[:, None], axis=1, dtype=jnp.int32)
        lo = lo + jnp.where(chip_id == 0, chip_len, lo_far)
        lo = (lo >> (ALIGN.bit_length() - 1)) << (ALIGN.bit_length() - 1)
        end = chip_len + BQ * (1 + jnp.arange(chip_len // BQ, dtype=jnp.int32))
        n_blocks = (end - lo + BK - 1) >> (BK.bit_length() - 1)
        kdoc = jnp.concatenate([doc_far, doc_chip, jnp.zeros((BK,), jnp.int32)])[None, :]

        acts, acts_oth, dkvs, sums = [], [], [], None
        for j in range(n_chunks):
            act, part, dkv = attention(
                j, core, lo, n_blocks, q, dctx, kdoc, (tab_own, tab_oth), (kvp_own, kvp_oth), (kv_own, kv_oth),
                (hidden, x_oth), (grad_out, g_oth),
            )
            part = part.reshape(2, WIDE, -1)
            acts.append(act)
            dkvs.append(dkv.reshape(2, 2, HEAD, chip_len))
            if j == n_chunks - 1:
                dkv_up = sum(d[:, 0].astype(F32) for d in dkvs).astype(BF)
                dkv_far = lax.ppermute(dkv_up, "sp", up_perm)
            acts_oth.append(near(act))
            part_far = far(part)
            part_near = near(part)
            part_far_near = near(part_far)
            sums = combine(core, j, n_chunks, (part, part_far, part_near, part_far_near), sums)
        grad_wq, grad_wo = sums

        dkv, dkvt = kv_finish(core, dkvs, dkv_far, tab_own, tab_oth)
        dkv_oth = near(dkv)
        kv_part = kvgrad(core, dkvt, hidden, x_oth)
        kv_part_far = far(kv_part)
        kv_part_near = near(kv_part)
        kv_part_far_near = near(kv_part_far)
        grad_wk, grad_wv = kv_combine(core, (kv_part, kv_part_far, kv_part_near, kv_part_far_near))
        out = attn_out(core, acts, acts_oth, w_o)
        g_hidden = grad_hidden(core, acts, acts_oth, dkv, dkv_oth, w_q, w_k, w_v)
        return out, g_hidden, grad_wq, grad_wk, grad_wv, grad_wo

    tok_spec = P(("dp", "sp"), None)
    vec_spec = P(("dp", "sp"))
    rep_spec = P(None, None)
    part_spec = P("dp", None)


    return jax.shard_map(
        device_step,
        mesh=mesh,
        in_specs=(tok_spec, tok_spec, vec_spec, vec_spec, rep_spec, rep_spec, rep_spec, rep_spec),
        out_specs=(tok_spec, tok_spec, part_spec, part_spec, part_spec, part_spec),
        check_vma=False,
    )
```

```python
import functools

import jax
import jax.numpy as jnp
from jax import lax
from jax.experimental import pallas as pl
from jax.experimental.pallas import tpu as pltpu
from jax.sharding import PartitionSpec as P

HEAD = 128
ROPE_THETA = 500000.0
ROPE_FACTOR = 8.0
ROPE_LOW = 1.0
ROPE_HIGH = 4.0
ROPE_OLD_CTX = 8192.0
NEG_BIG = -1.0e30
SCALE = HEAD ** -0.5
LOG2E = 1.4426950408889634

PAIR = 2
WIDE = PAIR * HEAD
BQ = 512
BK = 512
ALIGN = 128
BF = jnp.bfloat16
F32 = jnp.float32


def rope_freqs():
    half_idx = jnp.arange(HEAD // 2, dtype=F32)
    inv_freq = jnp.power(ROPE_THETA, -2.0 * half_idx / HEAD)
    wavelen = 2.0 * jnp.pi / inv_freq
    smooth = (ROPE_OLD_CTX / wavelen - ROPE_LOW) / (ROPE_HIGH - ROPE_LOW)
    mixed_freq = (1.0 - smooth) * inv_freq / ROPE_FACTOR + smooth * inv_freq
    scaled = jnp.where(wavelen > ROPE_OLD_CTX / ROPE_LOW, inv_freq / ROPE_FACTOR, mixed_freq)
    return jnp.where(wavelen < ROPE_OLD_CTX / ROPE_HIGH, inv_freq, scaled)


def rope_table(pos_vec):
    angles = pos_vec.astype(F32)[:, None] * rope_freqs()[None, :]
    return jnp.concatenate([jnp.cos(angles), jnp.sin(angles)], axis=-1)


def dot_nn(a, b):
    return lax.dot_general(a, b, (((1,), (0,)), ((), ())), preferred_element_type=F32)


def dot_nt(a, b):
    return lax.dot_general(a, b, (((1,), (1,)), ((), ())), preferred_element_type=F32)


def swap_halves(v):
    return pltpu.roll(v, HEAD // 2, 1)


def spread_table(tab):
    low = lax.broadcasted_iota(jnp.int32, tab.shape, 1) < HEAD // 2
    other = swap_halves(tab)
    return jnp.where(low, tab, other), jnp.where(low, -other, tab)


def cost(flops, nbytes, trans=0):
    return pl.CostEstimate(flops=int(flops), bytes_accessed=int(nbytes), transcendentals=int(trans))


def params(**kw):
    return pltpu.CompilerParams(vmem_limit_bytes=67_000_000, **kw)


def by_rows(rows, body, size=16):
    def step(r, carry):
        body(span(r, size))
        return carry

    lax.fori_loop(0, rows // size, step, 0)


def span(index, size):
    return pl.ds(pl.multiple_of(index * size, size), size)


def qkv_kernel(s_ref, x_ref, wk_ref, wv_ref, wq_ref, tab_ref, *rest):
    kv_ref, q_ref, w_s = rest[-3:]

    @pl.when(pl.program_id(0) == 0)
    def _():
        w_s[:, :HEAD] = wk_ref[...]
        w_s[:, HEAD:2 * HEAD] = wv_ref[...]
        w_s[:, 2 * HEAD:] = wq_ref[...]

    out = dot_nn(x_ref[...], w_s[...])
    cos_t, sin_t = spread_table(tab_ref[...])

    def turned(n):
        part = out[:, n * HEAD:(n + 1) * HEAD]
        return (part * cos_t + swap_halves(part) * sin_t).astype(BF)

    kv_ref[:, :HEAD] = turned(0)
    kv_ref[:, HEAD:] = out[:, HEAD:2 * HEAD].astype(BF)
    for h in range(PAIR):
        q_ref[:, h * HEAD:(h + 1) * HEAD] = turned(2 + h)


def qkv_proj(sel, x, w_q, w_k, w_v, tab, prev):
    tokens, width = x.shape
    n = w_q.shape[1] // 2 // WIDE
    rows = tokens // 4
    extra = [] if prev is None else [prev]
    return pl.pallas_call(
        qkv_kernel,
        grid_spec=pltpu.PrefetchScalarGridSpec(
            num_scalar_prefetch=1,
            grid=(4,),
            in_specs=[
                pl.BlockSpec((rows, width), lambda m, s: (m, 0)),
                pl.BlockSpec((width, HEAD), lambda m, s: (0, s[0])),
                pl.BlockSpec((width, HEAD), lambda m, s: (0, s[0])),
                pl.BlockSpec((width, WIDE), lambda m, s: (0, s[0] * n)),
                pl.BlockSpec((rows, HEAD), lambda m, s: (m, 0)),
            ] + [pl.BlockSpec(memory_space=pl.ANY)] * len(extra),
            out_specs=[
                pl.BlockSpec((rows, 2 * HEAD), lambda m, s: (m, 0)),
                pl.BlockSpec((rows, WIDE), lambda m, s: (s[1] * 4 + m, 0)),
            ],
            scratch_shapes=[pltpu.VMEM((width, 2 * HEAD + WIDE), BF)],
        ),
        out_shape=[
            jax.ShapeDtypeStruct((tokens, 2 * HEAD), BF),
            jax.ShapeDtypeStruct((2 * tokens, WIDE), BF),
        ],
        input_output_aliases={} if prev is None else {6: 1},
        compiler_params=params(),
        cost_estimate=cost(2 * tokens * width * (WIDE + 2 * HEAD), tokens * width * 2),
        name="qkv_proj",
    )(sel, x, w_k, w_v, w_q, tab, *extra)


def by_half(rows_per_step, width, steps=2):
    own = pl.BlockSpec((rows_per_step, width), lambda m, s: (jnp.minimum(m, steps - 1), 0))
    oth = pl.BlockSpec((rows_per_step, width), lambda m, s: (jnp.maximum(m - steps, 0), 0))

    def place(m, s):
        far = m // steps
        return (s[0] + far - 2 * s[0] * far) * steps + m % steps

    return own, oth, place


def on_half(put, own_refs, oth_refs, steps=2):
    @pl.when(pl.program_id(0) < steps)
    def _():
        put(*own_refs)

    @pl.when(pl.program_id(0) >= steps)
    def _():
        put(*oth_refs)


def q_rest_kernel(n, s_ref, own_ref, oth_ref, tab_own, tab_oth, *rest):
    w_refs, (out_ref, w_s) = rest[:n], rest[n:]

    @pl.when(pl.program_id(0) == 0)
    def _():
        for r in range(n):
            w_s[:, r * WIDE:(r + 1) * WIDE] = w_refs[r][...]

    def put(ref, tab_ref):
        cos_t, sin_t = spread_table(tab_ref[...])
        q = dot_nn(ref[...], w_s[...])
        for h in range(q.shape[1] // HEAD):
            part = q[:, h * HEAD:(h + 1) * HEAD]
            out_ref[:, h * HEAD:(h + 1) * HEAD] = (part * cos_t + swap_halves(part) * sin_t).astype(BF)

    on_half(put, (own_ref, tab_own), (oth_ref, tab_oth))


def q_rest(core, own, oth, tab_own, tab_oth, w_q):
    tokens, width = own.shape
    chunks = w_q.shape[1] // 2 // WIDE
    n = chunks - 1
    rows = tokens // 2
    spec_own, spec_oth, place = by_half(rows, width)
    t_own, t_oth, _ = by_half(rows, HEAD)
    return pl.pallas_call(
        functools.partial(q_rest_kernel, n),
        grid_spec=pltpu.PrefetchScalarGridSpec(
            num_scalar_prefetch=1,
            grid=(4,),
            in_specs=[spec_own, spec_oth, t_own, t_oth] + [
                pl.BlockSpec((width, WIDE), lambda m, s, r=r: (0, s[0] * chunks + 1 + r)) for r in range(n)
            ],
            out_specs=pl.BlockSpec((rows, n * WIDE), lambda m, s: (place(m, s), 0)),
            scratch_shapes=[pltpu.VMEM((width, n * WIDE), BF)],
        ),
        out_shape=jax.ShapeDtypeStruct((2 * tokens, n * WIDE), BF),
        compiler_params=params(),
        cost_estimate=cost(4 * tokens * width * n * WIDE, tokens * width * 4),
        name="q_rest",
    )(core, own, oth, tab_own, tab_oth, *([w_q] * n))


def dctx_kernel(n, s_ref, own_ref, oth_ref, *rest):
    w_refs, (out_ref, w_s) = rest[:n], rest[n:]

    @pl.when(pl.program_id(0) == 0)
    def _():
        for r in range(n):
            w_s[r * WIDE:(r + 1) * WIDE, :] = w_refs[r][...]

    def put(ref):
        out_ref[...] = dot_nt(ref[...], w_s[...]).astype(BF)

    on_half(put, (own_ref,), (oth_ref,))


def dctx_proj(core, own, oth, w_o, first, n):
    tokens, width = own.shape
    chunks = w_o.shape[0] // 2 // WIDE
    rows = tokens // 2
    spec_own, spec_oth, place = by_half(rows, width)
    return pl.pallas_call(
        functools.partial(dctx_kernel, n),
        grid_spec=pltpu.PrefetchScalarGridSpec(
            num_scalar_prefetch=1,
            grid=(4,),
            in_specs=[spec_own, spec_oth] + [
                pl.BlockSpec((WIDE, width), lambda m, s, r=r: (s[0] * chunks + first + r, 0)) for r in range(n)
            ],
            out_specs=pl.BlockSpec((rows, n * WIDE), lambda m, s: (place(m, s), 0)),
            scratch_shapes=[pltpu.VMEM((n * WIDE, width), BF)],
        ),
        out_shape=jax.ShapeDtypeStruct((2 * tokens, n * WIDE), BF),
        compiler_params=params(),
        cost_estimate=cost(4 * tokens * width * n * WIDE, tokens * width * 4),
        name="dctx_proj",
    )(core, own, oth, *([w_o] * n))


def attn_kernel(
    core_ref, lo_ref, nb_ref, q_ref, do_ref, kdoc_ref, tab_own, tab_oth, kvp_own, kvp_oth, kvc_own, kvc_oth,
    x_own, x_oth, g_own, g_oth, act_ref, part_ref, dkv_ref,
    k_s, v_s, s_s, dp_s, m_s, l_s, d_s, qd_s, ctx_s, dq_s, q_s, do_s, qt_s, dot_s, tab_s, dk_s, dv_s,
    x_s, g_s, at_s, w_s, init_sem, row_sem, out_sem,
):
    i = pl.program_id(0)
    tokens = kvc_own.shape[0]
    chip_len = 2 * tokens
    core = core_ref[0]
    per_half = tokens // BQ
    rows_here = span(i % per_half, BQ)

    def row_copies(x, g):
        return (
            pltpu.make_async_copy(x.at[rows_here, :], x_s, row_sem.at[0]),
            pltpu.make_async_copy(g.at[rows_here, :], g_s, row_sem.at[1]),
        )

    def init_copies():
        moves = []
        for base, place, ref in ((0, core, kvp_own), (0, 1 - core, kvp_oth), (2, core, kvc_own), (2, 1 - core, kvc_oth)):
            moves.append((ref.at[:, pl.ds(0, HEAD)], k_s.at[span(base + place, tokens), :]))
        for base, place, ref in ((0, core, kvp_own), (0, 1 - core, kvp_oth), (2, core, kvc_own), (2, 1 - core, kvc_oth)):
            moves.append((ref.at[:, pl.ds(HEAD, HEAD)], v_s.at[span(base + place, tokens), :]))
        moves.append((tab_own, tab_s.at[span(core, tokens), :]))
        moves.append((tab_oth, tab_s.at[span(1 - core, tokens), :]))
        return [pltpu.make_async_copy(src, dst, init_sem.at[n]) for n, (src, dst) in enumerate(moves)]

    def arrive(first, last):
        @pl.when(i == 0)
        def _():
            for copy in init_copies()[first:last]:
                copy.wait()

    @pl.when(i == 0)
    def _():
        for copy in init_copies():
            copy.start()
        k_s[2 * chip_len:, :] = jnp.zeros((BK, HEAD), BF)
        v_s[2 * chip_len:, :] = jnp.zeros((BK, HEAD), BF)

        def clear(r):
            w_s[r, :] = jnp.zeros((16, w_s.shape[1]), F32)

        def clear_kv(r):
            dk_s[r, :] = jnp.zeros((16, dk_s.shape[1]), F32)
            dv_s[r, :] = jnp.zeros((16, dv_s.shape[1]), F32)

        by_rows(w_s.shape[0], clear)
        by_rows(HEAD, clear_kv)

    @pl.when(i // per_half == core)
    def _():
        for copy in row_copies(x_own, g_own):
            copy.start()

    @pl.when(i // per_half != core)
    def _():
        for copy in row_copies(x_oth, g_oth):
            copy.start()

    for h in range(PAIR):
        rows = slice(h * BQ, (h + 1) * BQ)
        cols = slice(h * HEAD, (h + 1) * HEAD)
        q_s[rows, :] = q_ref[:, cols]
        do_s[rows, :] = do_ref[:, cols]
        qt_s[:, rows] = q_ref[:, cols].T
        dot_s[:, rows] = do_ref[:, cols].T
    qdoc = kdoc_ref[:, pl.ds(pl.multiple_of(chip_len + i * BQ, BQ), BQ)]
    qd_s[...] = jnp.broadcast_to(qdoc, (HEAD, BQ)).T
    m_s[...] = jnp.full(m_s.shape, NEG_BIG, F32)
    l_s[...] = jnp.zeros(l_s.shape, F32)
    d_s[...] = jnp.zeros(d_s.shape, F32)
    ctx_s[...] = jnp.zeros(ctx_s.shape, F32)
    dq_s[...] = jnp.zeros(dq_s.shape, F32)
    lo = lo_ref[i]
    n_blocks = nb_ref[i]
    lanes = BK // HEAD

    def fold(v, op):
        out = v[:, :HEAD]
        for n in range(1, lanes):
            out = op(out, v[:, n * HEAD:(n + 1) * HEAD])
        return out

    def spread(v):
        return jnp.concatenate([v] * lanes, axis=1)

    def offset(b):
        return pl.multiple_of(lo + b * BK, ALIGN)

    def scores(b, carry):
        off = offset(b)
        s = dot_nt(q_s[...], k_s[pl.ds(off, BK), :])
        key = off + lax.broadcasted_iota(jnp.int32, (BQ, BK), 1)
        query = chip_len + i * BQ + lax.broadcasted_iota(jnp.int32, (BQ, BK), 0)
        keep = (key <= query) & (kdoc_ref[:, pl.ds(off, BK)] == spread(qd_s[...]))
        for h in range(PAIR):
            rows = slice(h * BQ, (h + 1) * BQ)
            sh = jnp.where(keep, s[rows, :], NEG_BIG)
            s_s[b, rows, :] = sh
            m_s[rows, :] = jnp.maximum(m_s[rows, :], fold(sh, jnp.maximum))
        return carry

    arrive(0, 4)
    lax.fori_loop(0, n_blocks, scores, 0)
    m_s[...] = jnp.broadcast_to(jnp.max(m_s[...], axis=1, keepdims=True), m_s.shape)

    def weights(b, carry):
        dp = dot_nt(do_s[...], v_s[pl.ds(offset(b), BK), :])
        e = jnp.exp2((s_s[b] - spread(m_s[...])) * (SCALE * LOG2E))
        s_s[b] = e
        dp_s[b] = dp
        l_s[...] += fold(e, jnp.add)
        d_s[...] += fold(e * dp, jnp.add)
        return carry

    arrive(4, 10)
    lax.fori_loop(0, n_blocks, weights, 0)
    inv = 1.0 / jnp.sum(l_s[...], axis=1, keepdims=True)
    delta = jnp.sum(d_s[...], axis=1, keepdims=True) * inv
    l_s[...] = jnp.broadcast_to(inv, l_s.shape)
    d_s[...] = jnp.broadcast_to(delta, d_s.shape)

    def grads(b, carry):
        off = offset(b)
        p = s_s[b] * spread(l_s[...])
        pb = p.astype(BF)
        ds = (p * (dp_s[b] - spread(d_s[...])) * SCALE).astype(BF)
        ctx_s[...] += dot_nn(pb, v_s[pl.ds(off, BK), :])
        dq_s[...] += dot_nn(ds, k_s[pl.ds(off, BK), :])
        dv_s[:, pl.ds(off, BK)] += dot_nn(dot_s[...], pb)
        dk_s[:, pl.ds(off, BK)] += dot_nn(qt_s[...], ds)
        return carry

    lax.fori_loop(0, n_blocks, grads, 0)
    cos_t, sin_t = spread_table(tab_s[span(i, BQ), :])
    for h in range(PAIR):
        rows = slice(h * BQ, (h + 1) * BQ)
        cols = slice(h * HEAD, (h + 1) * HEAD)
        ctx = ctx_s[rows, :].astype(BF)
        act_ref[0, :, cols] = ctx
        at_s[WIDE + h * HEAD:WIDE + (h + 1) * HEAD, :] = ctx.T
        dq = dq_s[rows, :].astype(BF).astype(F32)
        dq = (dq * cos_t - swap_halves(dq) * sin_t).astype(BF)
        act_ref[1, :, cols] = dq
        at_s[h * HEAD:(h + 1) * HEAD, :] = dq.T
    step = 4 * HEAD
    for copy in row_copies(x_own, g_own):
        copy.wait()

    def products(c, carry):
        cols = span(c, step)
        w_s[:WIDE, cols] += dot_nn(at_s[:WIDE, :], x_s[:, cols])
        w_s[WIDE:, cols] += dot_nn(at_s[WIDE:, :], g_s[:, cols])
        return carry

    lax.fori_loop(0, x_s.shape[1] // step, products, 0)

    @pl.when(i == pl.num_programs(0) - 1)
    def _():
        def narrow(r):
            x_s[r, :] = w_s[r, :].astype(BF)

        by_rows(w_s.shape[0], narrow)
        part_copy = pltpu.make_async_copy(x_s, part_ref, out_sem.at[0])
        part_copy.start()

        def narrow_kv(r, carry):
            rows = span(r, 16)
            for n, acc in enumerate((dk_s, dv_s)):
                for side in range(2):
                    at = pl.ds(pl.multiple_of((2 * n + side) * HEAD + r * 16, 16), 16)
                    g_s[at, :] = acc[rows, side * chip_len:(side + 1) * chip_len].astype(BF)
            return carry

        lax.fori_loop(0, HEAD // 16, narrow_kv, 0)
        dkv_copy = pltpu.make_async_copy(g_s, dkv_ref, out_sem.at[1])
        dkv_copy.start()
        part_copy.wait()
        dkv_copy.wait()


def attention(chunk, core, lo, n_blocks, q, dctx, kdoc, tabs, kv_prev, kv_chip, xs, gs):
    chip_len = q.shape[0]
    width = xs[0].shape[1]
    assert 2 * WIDE == BQ == 4 * HEAD and width == chip_len
    padded = 2 * chip_len + BK
    max_blocks = 2 * chip_len // BK
    rows = PAIR * BQ
    full = lambda shape: pl.BlockSpec(shape, lambda i, *s: (0,) * len(shape))
    pairs = chip_len * chip_len * PAIR
    return pl.pallas_call(
        attn_kernel,
        grid_spec=pltpu.PrefetchScalarGridSpec(
            num_scalar_prefetch=3,
            grid=(chip_len // BQ,),
            in_specs=[
                pl.BlockSpec((BQ, WIDE), lambda i, *s: (i, chunk)),
                pl.BlockSpec((BQ, WIDE), lambda i, *s: (i, chunk)),
                full((1, padded)),
            ] + [pl.BlockSpec(memory_space=pl.ANY)] * 10,
            out_specs=[
                pl.BlockSpec((2, BQ, WIDE), lambda i, *s: (0, i, 0)),
                pl.BlockSpec(memory_space=pl.ANY),
                pl.BlockSpec(memory_space=pl.ANY),
            ],
            scratch_shapes=[
                pltpu.VMEM((padded, HEAD), BF),
                pltpu.VMEM((padded, HEAD), BF),
                pltpu.VMEM((max_blocks, rows, BK), F32),
                pltpu.VMEM((max_blocks, rows, BK), F32),
                pltpu.VMEM((rows, HEAD), F32),
                pltpu.VMEM((rows, HEAD), F32),
                pltpu.VMEM((rows, HEAD), F32),
                pltpu.VMEM((BQ, HEAD), jnp.int32),
                pltpu.VMEM((rows, HEAD), F32),
                pltpu.VMEM((rows, HEAD), F32),
                pltpu.VMEM((rows, HEAD), BF),
                pltpu.VMEM((rows, HEAD), BF),
                pltpu.VMEM((HEAD, rows), BF),
                pltpu.VMEM((HEAD, rows), BF),
                pltpu.VMEM((chip_len, HEAD), F32),
                pltpu.VMEM((HEAD, padded), F32),
                pltpu.VMEM((HEAD, padded), F32),
                pltpu.VMEM((BQ, width), BF),
                pltpu.VMEM((BQ, width), BF),
                pltpu.VMEM((2 * WIDE, BQ), BF),
                pltpu.VMEM((2 * WIDE, width), F32),
                pltpu.SemaphoreType.DMA((10,)),
                pltpu.SemaphoreType.DMA((2,)),
                pltpu.SemaphoreType.DMA((2,)),
            ],
        ),
        out_shape=[
            jax.ShapeDtypeStruct((2, chip_len, WIDE), BF),
            jax.ShapeDtypeStruct((2 * WIDE, width), BF),
            jax.ShapeDtypeStruct((4 * HEAD, chip_len), BF),
        ],
        compiler_params=params(),
        cost_estimate=cost(pairs * HEAD * 2 * 8, 12 * 1024 * 1024, pairs),
        name="attention",
    )(core, lo, n_blocks, q, dctx, kdoc, *tabs, *kv_prev, *kv_chip, *xs, *gs)


def kv_finish_kernel(n, s_ref, *refs):
    far_ref, tab_own, tab_oth, out_ref, outt_ref, tab_s = refs[n:]
    tokens = tab_own.shape[0]
    step = out_ref.shape[0]

    @pl.when(pl.program_id(0) == 0)
    def _():
        tab_s[span(s_ref[0], tokens), :] = tab_own[...]
        tab_s[span(1 - s_ref[0], tokens), :] = tab_oth[...]

    total = far_ref[...].astype(F32)
    for ref in refs[:n]:
        total = total + ref[:, 0].astype(F32)
    cos_t, sin_t = spread_table(tab_s[span(pl.program_id(0), step), :])
    dk = total[0].astype(BF).astype(F32).T
    dk = (dk * cos_t - swap_halves(dk) * sin_t).astype(BF)
    dvt = total[1].astype(BF)
    out_ref[:, :HEAD] = dk
    out_ref[:, HEAD:] = dvt.T
    outt_ref[:HEAD, :] = dk.T
    outt_ref[HEAD:, :] = dvt


def kv_finish(core, parts, far, tab_own, tab_oth):
    tokens = tab_own.shape[0]
    chip_len = 2 * tokens
    step = 512
    return pl.pallas_call(
        functools.partial(kv_finish_kernel, len(parts)),
        grid_spec=pltpu.PrefetchScalarGridSpec(
            num_scalar_prefetch=1,
            grid=(chip_len // step,),
            in_specs=[pl.BlockSpec((2, 1, HEAD, step), lambda t, s: (0, 1, 0, t))] * len(parts)
            + [
                pl.BlockSpec((2, HEAD, step), lambda t, s: (0, 0, t)),
                pl.BlockSpec((tokens, HEAD), lambda t, s: (0, 0)),
                pl.BlockSpec((tokens, HEAD), lambda t, s: (0, 0)),
            ],
            out_specs=[
                pl.BlockSpec((step, 2 * HEAD), lambda t, s: (t, 0)),
                pl.BlockSpec((2 * HEAD, step), lambda t, s: (0, t)),
            ],
            scratch_shapes=[pltpu.VMEM((chip_len, HEAD), F32)],
        ),
        out_shape=[
            jax.ShapeDtypeStruct((chip_len, 2 * HEAD), BF),
            jax.ShapeDtypeStruct((2 * HEAD, chip_len), BF),
        ],
        compiler_params=params(),
        cost_estimate=cost(chip_len * HEAD * 64, chip_len * HEAD * 16),
        name="kv_finish",
    )(core, *parts, far, tab_own, tab_oth)


def kvgrad_kernel(s_ref, dkvt_ref, x_own, x_oth, out_ref):
    tokens = x_own.shape[0]
    own, oth = span(s_ref[0], tokens), span(1 - s_ref[0], tokens)
    out_ref[...] = (dot_nn(dkvt_ref[:, own], x_own[...]) + dot_nn(dkvt_ref[:, oth], x_oth[...])).astype(BF)


def kvgrad(core, dkvt, x_own, x_oth):
    tokens, width = x_own.shape
    step = 512
    piece = pl.BlockSpec((tokens, step), lambda n, s: (0, n))
    return pl.pallas_call(
        kvgrad_kernel,
        grid_spec=pltpu.PrefetchScalarGridSpec(
            num_scalar_prefetch=1,
            grid=(width // step,),
            in_specs=[pl.BlockSpec((2 * HEAD, 2 * tokens), lambda n, s: (0, 0)), piece, piece],
            out_specs=pl.BlockSpec((2 * HEAD, step), lambda n, s: (0, n)),
        ),
        out_shape=jax.ShapeDtypeStruct((2 * HEAD, width), BF),
        compiler_params=params(),
        cost_estimate=cost(4 * tokens * width * 2 * HEAD, 4 * tokens * width),
        name="kvgrad",
    )(core, dkvt, x_own, x_oth)


def kv_combine_kernel(s_ref, a_ref, b_ref, c_ref, d_ref, gk_ref, gv_ref):
    for place, u_ref, v_ref in ((s_ref[0], a_ref, b_ref), (1 - s_ref[0], c_ref, d_ref)):
        total = u_ref[...].astype(F32) + v_ref[...].astype(F32)
        where = span(place, HEAD)
        gk_ref[:, where] = total[:HEAD, :].T
        gv_ref[:, where] = total[HEAD:, :].T


def kv_combine(core, parts):
    rows, width = parts[0].shape
    step = 512
    out = jax.ShapeDtypeStruct((width, rows), F32)
    return pl.pallas_call(
        kv_combine_kernel,
        grid_spec=pltpu.PrefetchScalarGridSpec(
            num_scalar_prefetch=1,
            grid=(width // step,),
            in_specs=[pl.BlockSpec((rows, step), lambda n, s: (0, n))] * 4,
            out_specs=[pl.BlockSpec((step, rows), lambda n, s: (n, 0))] * 2,
        ),
        out_shape=[out, out],
        compiler_params=params(),
        cost_estimate=cost(16 * width * rows * 16, 16 * width * rows),
        name="kv_combine",
    )(core, *parts)


def combine_kernel(s_ref, a_ref, b_ref, c_ref, d_ref, *rest):
    gq_ref, go_ref = rest[-2:]

    def put(u_ref, v_ref):
        gq_ref[...] = (u_ref[0].astype(F32) + v_ref[0].astype(F32)).T
        go_ref[...] = u_ref[1].astype(F32) + v_ref[1].astype(F32)

    @pl.when(pl.program_id(0) == 0)
    def _():
        put(a_ref, b_ref)

    @pl.when(pl.program_id(0) == 1)
    def _():
        put(c_ref, d_ref)


def combine(core, chunk, n_chunks, parts, prev):
    width = parts[0].shape[2]
    step = 512
    last = width // step - 1
    near = pl.BlockSpec((2, WIDE, step), lambda w, r, s: (0, 0, r + w * (last - r)))
    far = pl.BlockSpec((2, WIDE, step), lambda w, r, s: (0, 0, r * w))

    def place(w, s):
        return (s[0] + w - 2 * s[0] * w) * n_chunks + chunk

    shape = jax.ShapeDtypeStruct((width, 2 * n_chunks * WIDE), F32)
    shape_o = jax.ShapeDtypeStruct((2 * n_chunks * WIDE, width), F32)
    extra = [] if prev is None else list(prev)
    return pl.pallas_call(
        combine_kernel,
        grid_spec=pltpu.PrefetchScalarGridSpec(
            num_scalar_prefetch=1,
            grid=(2, width // step),
            in_specs=[near, near, far, far] + [pl.BlockSpec(memory_space=pl.ANY)] * len(extra),
            out_specs=[
                pl.BlockSpec((step, WIDE), lambda w, r, s: (r, place(w, s))),
                pl.BlockSpec((WIDE, step), lambda w, r, s: (place(w, s), r)),
            ],
        ),
        out_shape=[shape, shape_o],
        input_output_aliases={} if prev is None else {5: 0, 6: 1},
        compiler_params=params(),
        cost_estimate=cost(16 * width * WIDE * 64, 32 * width * WIDE),
        name="combine",
    )(core, *parts, *extra)


def fill_heads(core, own_refs, oth_refs, lhs):
    n = len(own_refs)
    for j in range(n):
        lhs[:, pl.ds(pl.multiple_of((core * n + j) * WIDE, WIDE), WIDE)] = own_refs[j][0]
        lhs[:, pl.ds(pl.multiple_of(((1 - core) * n + j) * WIDE, WIDE), WIDE)] = oth_refs[j][0]


def attn_out_kernel(n, s_ref, *refs):
    own_refs, oth_refs = refs[:n], refs[n:2 * n]
    wo_ref, out_ref, lhs = refs[2 * n:]

    @pl.when(pl.program_id(0) == 0)
    def _():
        fill_heads(s_ref[0], own_refs, oth_refs, lhs)

    out_ref[...] = dot_nn(lhs[...], wo_ref[...]).astype(BF)


def attn_out(core, own, oth, w_o):
    n = len(own)
    tokens = own[0].shape[1] // 2
    heads, width = w_o.shape
    step = 512
    return pl.pallas_call(
        functools.partial(attn_out_kernel, n),
        grid_spec=pltpu.PrefetchScalarGridSpec(
            num_scalar_prefetch=1,
            grid=(width // step,),
            in_specs=[pl.BlockSpec((1, tokens, WIDE), lambda k, s: (0, s[0], 0))] * (2 * n)
            + [pl.BlockSpec((heads, step), lambda k, s: (0, k))],
            out_specs=pl.BlockSpec((tokens, step), lambda k, s: (0, k)),
            scratch_shapes=[pltpu.VMEM((tokens, heads), BF)],
        ),
        out_shape=jax.ShapeDtypeStruct((tokens, width), BF),
        compiler_params=params(),
        cost_estimate=cost(2 * tokens * heads * width, 2 * heads * width + 4 * tokens * width),
        name="attn_out",
    )(core, *own, *oth, w_o)


def hidden_kernel(n, s_ref, *refs):
    own_refs, oth_refs = refs[:n], refs[n:2 * n]
    kv_own, kv_oth, wq_ref, wk_ref, wv_ref, out_ref, lhs, klhs, vlhs = refs[2 * n:]
    core = s_ref[0]

    @pl.when(pl.program_id(0) == 0)
    def _():
        fill_heads(core, own_refs, oth_refs, lhs)
        for place, ref in ((core, kv_own), (1 - core, kv_oth)):
            where = pl.ds(pl.multiple_of(place * HEAD, HEAD), HEAD)
            klhs[:, where] = ref[:, :HEAD]
            vlhs[:, where] = ref[:, HEAD:]

    out_ref[...] = (
        dot_nt(lhs[...], wq_ref[...]) + dot_nt(klhs[...], wk_ref[...]) + dot_nt(vlhs[...], wv_ref[...])
    ).astype(BF)


def grad_hidden(core, own, oth, kv_own, kv_oth, w_q, w_k, w_v):
    n = len(own)
    tokens = own[0].shape[1] // 2
    width, heads = w_q.shape
    kv_cols = w_k.shape[1]
    step = 512
    return pl.pallas_call(
        functools.partial(hidden_kernel, n),
        grid_spec=pltpu.PrefetchScalarGridSpec(
            num_scalar_prefetch=1,
            grid=(width // step,),
            in_specs=[pl.BlockSpec((1, tokens, WIDE), lambda k, s: (1, s[0], 0))] * (2 * n)
            + [pl.BlockSpec((tokens, 2 * HEAD), lambda k, s: (s[0], 0))] * 2
            + [
                pl.BlockSpec((step, heads), lambda k, s: (k, 0)),
                pl.BlockSpec((step, kv_cols), lambda k, s: (k, 0)),
                pl.BlockSpec((step, kv_cols), lambda k, s: (k, 0)),
            ],
            out_specs=pl.BlockSpec((tokens, step), lambda k, s: (0, k)),
            scratch_shapes=[
                pltpu.VMEM((tokens, heads), BF),
                pltpu.VMEM((tokens, kv_cols), BF),
                pltpu.VMEM((tokens, kv_cols), BF),
            ],
        ),
        out_shape=jax.ShapeDtypeStruct((tokens, width), BF),
        compiler_params=params(),
        cost_estimate=cost(2 * tokens * (heads + 2 * kv_cols) * width, 2 * heads * width + 4 * tokens * width),
        name="grad_hidden",
    )(core, *own, *oth, kv_own, kv_oth, w_q, w_k, w_v)


def solution(mesh):
    n_dev = mesh.shape["sp"]
    n_chunks = 4
    near_perm = [(d, d ^ 1) for d in range(n_dev)]
    far_perm = [(d, d ^ 2) for d in range(n_dev)]
    down_perm = [(0, 2), (1, 3)]
    up_perm = [(2, 0), (3, 1)]

    def near(v):
        return lax.ppermute(v, "sp", near_perm)

    def far(v):
        return lax.ppermute(v, "sp", far_perm)

    def device_step(hidden, grad_out, positions, doc_ids, w_q, w_k, w_v, w_o):
        tokens = hidden.shape[0]
        chip_len = 2 * tokens
        assert n_chunks == w_q.shape[1] // (2 * WIDE)
        place = lax.axis_index("sp")
        core_id, chip_id = place & 1, place >> 1
        core = core_id.astype(jnp.int32)[None]
        sel_own = jnp.stack([core_id, core_id]).astype(jnp.int32)
        sel_oth = jnp.stack([core_id, 1 - core_id]).astype(jnp.int32)

        doc_oth = near(doc_ids)
        doc_far = far(doc_ids)
        doc_far_oth = lax.ppermute(doc_ids, "sp", [(d, d ^ 3) for d in range(n_dev)])
        x_oth = near(hidden)
        g_oth = near(grad_out)
        tab_own = rope_table(positions)
        tab_oth = near(tab_own)
        kv_own, q_first = qkv_proj(sel_own, hidden, w_q, w_k, w_v, tab_own, None)
        kvp_own = lax.ppermute(kv_own, "sp", down_perm)

        def in_order(own, oth):
            return jnp.where(core_id == 0, jnp.concatenate([own, oth]), jnp.concatenate([oth, own]))

        doc_chip, doc_far = in_order(doc_ids, doc_oth), in_order(doc_far, doc_far_oth)
        kv_oth, q_first = qkv_proj(sel_oth, x_oth, w_q, w_k, w_v, tab_oth, q_first)
        kvp_oth = lax.ppermute(kv_oth, "sp", down_perm)
        dctx_first = dctx_proj(core, grad_out, g_oth, w_o, 0, 1)
        q_more = q_rest(core, hidden, x_oth, tab_own, tab_oth, w_q)
        dctx_more = dctx_proj(core, grad_out, g_oth, w_o, 1, n_chunks - 1)

        heads_doc = doc_chip[::BQ]
        lo = jnp.sum(doc_chip[None, :] < heads_doc[:, None], axis=1, dtype=jnp.int32)
        lo_far = jnp.sum(doc_far[None, :] < heads_doc[:, None], axis=1, dtype=jnp.int32)
        lo = lo + jnp.where(chip_id == 0, chip_len, lo_far)
        lo = (lo >> (ALIGN.bit_length() - 1)) << (ALIGN.bit_length() - 1)
        end = chip_len + BQ * (1 + jnp.arange(chip_len // BQ, dtype=jnp.int32))
        n_blocks = (end - lo + BK - 1) >> (BK.bit_length() - 1)
        kdoc = jnp.concatenate([doc_far, doc_chip, jnp.zeros((BK,), jnp.int32)])[None, :]

        acts, acts_oth, dkvs, sums = [], [], [], None
        for j in range(n_chunks):
            act, part, dkv = attention(
                max(j - 1, 0), core, lo, n_blocks, q_more if j else q_first, dctx_more if j else dctx_first, kdoc, (tab_own, tab_oth), (kvp_own, kvp_oth), (kv_own, kv_oth),
                (hidden, x_oth), (grad_out, g_oth),
            )
            part = part.reshape(2, WIDE, -1)
            acts.append(act)
            dkvs.append(dkv.reshape(2, 2, HEAD, chip_len))
            if j == n_chunks - 1:
                dkv_up = sum(d[:, 0].astype(F32) for d in dkvs).astype(BF)
                dkv_far = lax.ppermute(dkv_up, "sp", up_perm)
            acts_oth.append(near(act))
            part_far = far(part)
            part_near = near(part)
            part_far_near = near(part_far)
            sums = combine(core, j, n_chunks, (part, part_far, part_near, part_far_near), sums)
        grad_wq, grad_wo = sums

        dkv, dkvt = kv_finish(core, dkvs, dkv_far, tab_own, tab_oth)
        dkv_oth = near(dkv)
        kv_part = kvgrad(core, dkvt, hidden, x_oth)
        kv_part_far = far(kv_part)
        kv_part_near = near(kv_part)
        kv_part_far_near = near(kv_part_far)
        grad_wk, grad_wv = kv_combine(core, (kv_part, kv_part_far, kv_part_near, kv_part_far_near))
        out = attn_out(core, acts, acts_oth, w_o)
        g_hidden = grad_hidden(core, acts, acts_oth, dkv, dkv_oth, w_q, w_k, w_v)
        return out, g_hidden, grad_wq, grad_wk, grad_wv, grad_wo

    tok_spec = P(("dp", "sp"), None)
    vec_spec = P(("dp", "sp"))
    rep_spec = P(None, None)
    part_spec = P("dp", None)


    return jax.shard_map(
        device_step,
        mesh=mesh,
        in_specs=(tok_spec, tok_spec, vec_spec, vec_spec, rep_spec, rep_spec, rep_spec, rep_spec),
        out_specs=(tok_spec, tok_spec, part_spec, part_spec, part_spec, part_spec),
        check_vma=False,
    )
```

```python
import functools

import jax
import jax.numpy as jnp
from jax import lax
from jax.experimental import pallas as pl
from jax.experimental.pallas import tpu as pltpu
from jax.sharding import PartitionSpec as P

HEAD = 128
ROPE_THETA = 500000.0
ROPE_FACTOR = 8.0
ROPE_LOW = 1.0
ROPE_HIGH = 4.0
ROPE_OLD_CTX = 8192.0
NEG_BIG = float("-inf")
SCALE = HEAD ** -0.5
LOG2E = 1.4426950408889634

PAIR = 2
WIDE = PAIR * HEAD
BQ = 512
BK = 512
MIX = 16
ALIGN = 128
BF = jnp.bfloat16
F32 = jnp.float32


def rope_freqs():
    half_idx = jnp.arange(HEAD // 2, dtype=F32)
    inv_freq = jnp.power(ROPE_THETA, -2.0 * half_idx / HEAD)
    wavelen = 2.0 * jnp.pi / inv_freq
    smooth = (ROPE_OLD_CTX / wavelen - ROPE_LOW) / (ROPE_HIGH - ROPE_LOW)
    mixed_freq = (1.0 - smooth) * inv_freq / ROPE_FACTOR + smooth * inv_freq
    scaled = jnp.where(wavelen > ROPE_OLD_CTX / ROPE_LOW, inv_freq / ROPE_FACTOR, mixed_freq)
    return jnp.where(wavelen < ROPE_OLD_CTX / ROPE_HIGH, inv_freq, scaled)


def rope_table(pos_vec):
    angles = pos_vec.astype(F32)[:, None] * rope_freqs()[None, :]
    return jnp.concatenate([jnp.cos(angles), jnp.sin(angles)], axis=-1)


def dot_nn(a, b):
    return lax.dot_general(a, b, (((1,), (0,)), ((), ())), preferred_element_type=F32)


def dot_nt(a, b):
    return lax.dot_general(a, b, (((1,), (1,)), ((), ())), preferred_element_type=F32)


def swap_halves(v):
    return pltpu.roll(v, HEAD // 2, 1)


def spread_table(tab):
    low = lax.broadcasted_iota(jnp.int32, tab.shape, 1) < HEAD // 2
    other = swap_halves(tab)
    return jnp.where(low, tab, other), jnp.where(low, -other, tab)


def cost(flops, nbytes, trans=0):
    return pl.CostEstimate(flops=int(flops), bytes_accessed=int(nbytes), transcendentals=int(trans))


def params(**kw):
    return pltpu.CompilerParams(vmem_limit_bytes=67_000_000, **kw)


def by_rows(rows, body, size=16):
    def step(r, carry):
        body(span(r, size))
        return carry

    lax.fori_loop(0, rows // size, step, 0)


def span(index, size):
    return pl.ds(pl.multiple_of(index * size, size), size)


def qkv_kernel(s_ref, x_ref, wq_ref, wk_ref, wv_ref, tab_ref, *rest):
    kv_ref, q_ref, w_s = rest[-3:]

    @pl.when(pl.program_id(0) == 0)
    def _():
        w_s[:, :HEAD] = wk_ref[...]
        w_s[:, HEAD:] = wv_ref[...]

    x = x_ref[...]
    cos_t, sin_t = spread_table(tab_ref[...])
    kv = dot_nn(x, w_s[...])
    k = kv[:, :HEAD]
    kv_ref[:, :HEAD] = (k * cos_t + swap_halves(k) * sin_t).astype(BF)
    kv_ref[:, HEAD:] = kv[:, HEAD:].astype(BF)
    step = 4 * HEAD
    for n in range(wq_ref.shape[1] // step):
        q = dot_nn(x, wq_ref[:, n * step:(n + 1) * step])
        for h in range(step // HEAD):
            part = q[:, h * HEAD:(h + 1) * HEAD]
            at = n * step + h * HEAD
            q_ref[:, at:at + HEAD] = (part * cos_t + swap_halves(part) * sin_t).astype(BF)


def qkv_proj(sel, x, w_q, w_k, w_v, tab, prev):
    tokens, width = x.shape
    cols = w_q.shape[1] // 2
    rows = tokens // 2
    extra = [] if prev is None else [prev]
    return pl.pallas_call(
        qkv_kernel,
        grid_spec=pltpu.PrefetchScalarGridSpec(
            num_scalar_prefetch=1,
            grid=(2,),
            in_specs=[
                pl.BlockSpec((rows, width), lambda m, s: (m, 0)),
                pl.BlockSpec((width, cols), lambda m, s: (0, s[0])),
                pl.BlockSpec((width, HEAD), lambda m, s: (0, s[0])),
                pl.BlockSpec((width, HEAD), lambda m, s: (0, s[0])),
                pl.BlockSpec((rows, HEAD), lambda m, s: (m, 0)),
            ] + [pl.BlockSpec(memory_space=pl.ANY)] * len(extra),
            out_specs=[
                pl.BlockSpec((rows, 2 * HEAD), lambda m, s: (m, 0)),
                pl.BlockSpec((rows, cols), lambda m, s: (s[1] * 2 + m, 0)),
            ],
            scratch_shapes=[pltpu.VMEM((width, 2 * HEAD), BF)],
        ),
        out_shape=[
            jax.ShapeDtypeStruct((tokens, 2 * HEAD), BF),
            jax.ShapeDtypeStruct((2 * tokens, cols), BF),
        ],
        input_output_aliases={} if prev is None else {6: 1},
        compiler_params=params(),
        cost_estimate=cost(2 * tokens * width * (cols + 2 * HEAD), tokens * width * 2 + cols * width * 2),
        name="qkv_proj",
    )(sel, x, w_q, w_k, w_v, tab, *extra)


def dctx_kernel(s_ref, own_ref, oth_ref, wo_ref, out_ref):
    def put(ref):
        step = 4 * HEAD
        for n in range(wo_ref.shape[0] // step):
            out_ref[:, n * step:(n + 1) * step] = dot_nt(ref[...], wo_ref[n * step:(n + 1) * step, :]).astype(BF)

    @pl.when(pl.program_id(0) < 2)
    def _():
        put(own_ref)

    @pl.when(pl.program_id(0) >= 2)
    def _():
        put(oth_ref)


def dctx_proj(core, own, oth, w_o):
    tokens, width = own.shape
    cols = w_o.shape[0] // 2
    rows = tokens // 2

    def place(m, s):
        far = m // 2
        return (s[0] + far - 2 * s[0] * far) * 2 + m % 2

    return pl.pallas_call(
        dctx_kernel,
        grid_spec=pltpu.PrefetchScalarGridSpec(
            num_scalar_prefetch=1,
            grid=(4,),
            in_specs=[
                pl.BlockSpec((rows, width), lambda m, s: (jnp.minimum(m, 1), 0)),
                pl.BlockSpec((rows, width), lambda m, s: (jnp.maximum(m - 2, 0), 0)),
                pl.BlockSpec((cols, width), lambda m, s: (s[0], 0)),
            ],
            out_specs=pl.BlockSpec((rows, cols), lambda m, s: (place(m, s), 0)),
        ),
        out_shape=jax.ShapeDtypeStruct((2 * tokens, cols), BF),
        compiler_params=params(),
        cost_estimate=cost(4 * tokens * width * cols, tokens * width * 4 + cols * width * 2),
        name="dctx_proj",
    )(core, own, oth, w_o)


def attn_kernel(
    core_ref, lo_ref, nb_ref, q_ref, do_ref, kdoc_ref, tab_own, tab_oth, kvp_own, kvp_oth, kvc_own, kvc_oth,
    x_own, x_oth, g_own, g_oth, act_ref, part_ref, dkv_ref,
    k_s, v_s, s_s, dp_s, m_s, l_s, d_s, qd_s, ahead_s, ctx_s, dq_s, q_s, do_s, qt_s, dot_s, tab_s, dk_s, dv_s,
    x_s, g_s, at_s, w_s, init_sem, row_sem, out_sem,
):
    i = pl.program_id(0)
    tokens = kvc_own.shape[0]
    chip_len = 2 * tokens
    core = core_ref[0]
    per_half = tokens // BQ
    rows_here = span(i % per_half, BQ)

    def row_copies(x, g):
        return (
            pltpu.make_async_copy(x.at[rows_here, :], x_s, row_sem.at[0]),
            pltpu.make_async_copy(g.at[rows_here, :], g_s, row_sem.at[1]),
        )

    def init_copies():
        moves = []
        for base, place, ref in ((0, core, kvp_own), (0, 1 - core, kvp_oth), (2, core, kvc_own), (2, 1 - core, kvc_oth)):
            moves.append((ref.at[:, pl.ds(0, HEAD)], k_s.at[span(base + place, tokens), :]))
        for base, place, ref in ((0, core, kvp_own), (0, 1 - core, kvp_oth), (2, core, kvc_own), (2, 1 - core, kvc_oth)):
            moves.append((ref.at[:, pl.ds(HEAD, HEAD)], v_s.at[span(base + place, tokens), :]))
        moves.append((tab_own, tab_s.at[span(core, tokens), :]))
        moves.append((tab_oth, tab_s.at[span(1 - core, tokens), :]))
        return [pltpu.make_async_copy(src, dst, init_sem.at[n]) for n, (src, dst) in enumerate(moves)]

    def arrive(first, last):
        @pl.when(i == 0)
        def _():
            for copy in init_copies()[first:last]:
                copy.wait()

    @pl.when(i == 0)
    def _():
        for copy in init_copies():
            copy.start()
        k_s[2 * chip_len:, :] = jnp.zeros((BK, HEAD), BF)
        v_s[2 * chip_len:, :] = jnp.zeros((BK, HEAD), BF)

        def clear(r):
            w_s[r, :] = jnp.zeros((16, w_s.shape[1]), F32)

        def clear_kv(r):
            dk_s[r, :] = jnp.zeros((16, dk_s.shape[1]), F32)
            dv_s[r, :] = jnp.zeros((16, dv_s.shape[1]), F32)

        def order(r):
            row = lax.broadcasted_iota(jnp.int32, (16, BK), 0)
            ahead_s[r, :] = lax.broadcasted_iota(jnp.int32, (16, BK), 1) - row - r.start

        by_rows(BQ, order)
        by_rows(w_s.shape[0], clear)
        by_rows(HEAD, clear_kv)

    @pl.when(i // per_half == core)
    def _():
        for copy in row_copies(x_own, g_own):
            copy.start()

    @pl.when(i // per_half != core)
    def _():
        for copy in row_copies(x_oth, g_oth):
            copy.start()

    def mixed(ref):
        parts = [ref[:, h * HEAD:(h + 1) * HEAD].reshape(BQ // MIX, 1, MIX, HEAD) for h in range(PAIR)]
        return jnp.concatenate(parts, axis=1).reshape(PAIR * BQ, HEAD)

    def apart(v, h):
        return v.reshape(BQ // MIX, PAIR, MIX, HEAD)[:, h].reshape(BQ, HEAD)

    q_mix, do_mix = mixed(q_ref), mixed(do_ref)
    q_s[...] = q_mix
    do_s[...] = do_mix
    qt_s[...] = q_mix.T
    dot_s[...] = do_mix.T
    qdoc = kdoc_ref[:, pl.ds(pl.multiple_of(chip_len + i * BQ, BQ), BQ)]
    qd_s[...] = jnp.broadcast_to(qdoc, (HEAD, BQ)).T
    m_s[...] = jnp.full(m_s.shape, NEG_BIG, F32)
    l_s[...] = jnp.zeros(l_s.shape, F32)
    d_s[...] = jnp.zeros(d_s.shape, F32)
    ctx_s[...] = jnp.zeros(ctx_s.shape, F32)
    dq_s[...] = jnp.zeros(dq_s.shape, F32)
    lo = lo_ref[i]
    n_blocks = nb_ref[i]
    lanes = BK // HEAD

    def fold(v, op):
        out = v[:, :HEAD]
        for n in range(1, lanes):
            out = op(out, v[:, n * HEAD:(n + 1) * HEAD])
        return out

    def spread(v):
        return jnp.concatenate([v] * lanes, axis=1)

    def offset(b):
        return pl.multiple_of(lo + b * BK, ALIGN)

    def scores(b, carry):
        off = offset(b)
        s = dot_nt(q_s[...], k_s[pl.ds(off, BK), :])
        limit = chip_len + i * BQ - off
        key_doc = kdoc_ref[:, pl.ds(off, BK)]
        for c in range(BQ // MIX):
            here = slice(c * MIX, (c + 1) * MIX)
            keep = (ahead_s[here, :] <= limit) & (key_doc == spread(qd_s[here, :]))
            shift = jnp.where(keep, 0.0, NEG_BIG)
            for h in range(PAIR):
                rows = slice((c * PAIR + h) * MIX, (c * PAIR + h + 1) * MIX)
                sh = s[rows, :] * (SCALE * LOG2E) + shift
                s_s[b, rows, :] = sh
                m_s[rows, :] = jnp.maximum(m_s[rows, :], fold(sh, jnp.maximum))
        return carry

    arrive(0, 4)
    lax.fori_loop(0, n_blocks, scores, 0)
    m_s[...] = jnp.broadcast_to(jnp.max(m_s[...], axis=1, keepdims=True), m_s.shape)

    def weights(b, carry):
        dp = dot_nt(do_s[...], v_s[pl.ds(offset(b), BK), :])
        e = jnp.exp2(s_s[b] - spread(m_s[...]))
        s_s[b] = e
        dp_s[b] = dp
        l_s[...] += fold(e, jnp.add)
        d_s[...] += fold(e * dp, jnp.add)
        return carry

    arrive(4, 10)
    lax.fori_loop(0, n_blocks, weights, 0)
    inv = 1.0 / jnp.sum(l_s[...], axis=1, keepdims=True)
    delta = jnp.sum(d_s[...], axis=1, keepdims=True) * inv
    l_s[...] = jnp.broadcast_to(inv, l_s.shape)
    d_s[...] = jnp.broadcast_to(delta, d_s.shape)

    def grads(b, carry):
        off = offset(b)
        p = s_s[b] * spread(l_s[...])
        pb = p.astype(BF)
        ds = (p * (dp_s[b] - spread(d_s[...])) * SCALE).astype(BF)
        ctx_s[...] += dot_nn(pb, v_s[pl.ds(off, BK), :])
        dq_s[...] += dot_nn(ds, k_s[pl.ds(off, BK), :])
        dv_s[:, pl.ds(off, BK)] += dot_nn(dot_s[...], pb)
        dk_s[:, pl.ds(off, BK)] += dot_nn(qt_s[...], ds)
        return carry

    lax.fori_loop(0, n_blocks, grads, 0)
    cos_t, sin_t = spread_table(tab_s[span(i, BQ), :])
    ctx_all, dq_all = ctx_s[...].astype(BF), dq_s[...].astype(BF).astype(F32)
    for h in range(PAIR):
        cols = slice(h * HEAD, (h + 1) * HEAD)
        ctx = apart(ctx_all, h)
        act_ref[0, :, cols] = ctx
        at_s[WIDE + h * HEAD:WIDE + (h + 1) * HEAD, :] = ctx.T
        dq = apart(dq_all, h)
        dq = (dq * cos_t - swap_halves(dq) * sin_t).astype(BF)
        act_ref[1, :, cols] = dq
        at_s[h * HEAD:(h + 1) * HEAD, :] = dq.T
    step = 4 * HEAD
    for copy in row_copies(x_own, g_own):
        copy.wait()

    def products(c, carry):
        cols = span(c, step)
        w_s[:WIDE, cols] += dot_nn(at_s[:WIDE, :], x_s[:, cols])
        w_s[WIDE:, cols] += dot_nn(at_s[WIDE:, :], g_s[:, cols])
        return carry

    lax.fori_loop(0, x_s.shape[1] // step, products, 0)

    @pl.when(i == pl.num_programs(0) - 1)
    def _():
        def narrow(r):
            x_s[r, :] = w_s[r, :].astype(BF)

        by_rows(w_s.shape[0], narrow)
        part_copy = pltpu.make_async_copy(x_s, part_ref, out_sem.at[0])
        part_copy.start()

        def narrow_kv(r, carry):
            rows = span(r, 16)
            for n, acc in enumerate((dk_s, dv_s)):
                for side in range(2):
                    at = pl.ds(pl.multiple_of((2 * n + side) * HEAD + r * 16, 16), 16)
                    g_s[at, :] = acc[rows, side * chip_len:(side + 1) * chip_len].astype(BF)
            return carry

        lax.fori_loop(0, HEAD // 16, narrow_kv, 0)
        dkv_copy = pltpu.make_async_copy(g_s, dkv_ref, out_sem.at[1])
        dkv_copy.start()
        part_copy.wait()
        dkv_copy.wait()


def attention(chunk, core, lo, n_blocks, q, dctx, kdoc, tabs, kv_prev, kv_chip, xs, gs):
    chip_len = q.shape[0]
    width = xs[0].shape[1]
    assert 2 * WIDE == BQ == 4 * HEAD and width == chip_len
    padded = 2 * chip_len + BK
    max_blocks = 2 * chip_len // BK
    rows = PAIR * BQ
    full = lambda shape: pl.BlockSpec(shape, lambda i, *s: (0,) * len(shape))
    pairs = chip_len * chip_len * PAIR
    return pl.pallas_call(
        attn_kernel,
        grid_spec=pltpu.PrefetchScalarGridSpec(
            num_scalar_prefetch=3,
            grid=(chip_len // BQ,),
            in_specs=[
                pl.BlockSpec((BQ, WIDE), lambda i, *s: (i, chunk)),
                pl.BlockSpec((BQ, WIDE), lambda i, *s: (i, chunk)),
                full((1, padded)),
            ] + [pl.BlockSpec(memory_space=pl.ANY)] * 10,
            out_specs=[
                pl.BlockSpec((2, BQ, WIDE), lambda i, *s: (0, i, 0)),
                pl.BlockSpec(memory_space=pl.ANY),
                pl.BlockSpec(memory_space=pl.ANY),
            ],
            scratch_shapes=[
                pltpu.VMEM((padded, HEAD), BF),
                pltpu.VMEM((padded, HEAD), BF),
                pltpu.VMEM((max_blocks, rows, BK), F32),
                pltpu.VMEM((max_blocks, rows, BK), F32),
                pltpu.VMEM((rows, HEAD), F32),
                pltpu.VMEM((rows, HEAD), F32),
                pltpu.VMEM((rows, HEAD), F32),
                pltpu.VMEM((BQ, HEAD), jnp.int32),
                pltpu.VMEM((BQ, BK), jnp.int32),
                pltpu.VMEM((rows, HEAD), F32),
                pltpu.VMEM((rows, HEAD), F32),
                pltpu.VMEM((rows, HEAD), BF),
                pltpu.VMEM((rows, HEAD), BF),
                pltpu.VMEM((HEAD, rows), BF),
                pltpu.VMEM((HEAD, rows), BF),
                pltpu.VMEM((chip_len, HEAD), F32),
                pltpu.VMEM((HEAD, padded), F32),
                pltpu.VMEM((HEAD, padded), F32),
                pltpu.VMEM((BQ, width), BF),
                pltpu.VMEM((BQ, width), BF),
                pltpu.VMEM((2 * WIDE, BQ), BF),
                pltpu.VMEM((2 * WIDE, width), F32),
                pltpu.SemaphoreType.DMA((10,)),
                pltpu.SemaphoreType.DMA((2,)),
                pltpu.SemaphoreType.DMA((2,)),
            ],
        ),
        out_shape=[
            jax.ShapeDtypeStruct((2, chip_len, WIDE), BF),
            jax.ShapeDtypeStruct((2 * WIDE, width), BF),
            jax.ShapeDtypeStruct((4 * HEAD, chip_len), BF),
        ],
        compiler_params=params(),
        cost_estimate=cost(pairs * HEAD * 2 * 8, 12 * 1024 * 1024, pairs),
        name="attention",
    )(core, lo, n_blocks, q, dctx, kdoc, *tabs, *kv_prev, *kv_chip, *xs, *gs)


def kv_finish_kernel(n, s_ref, *refs):
    far_ref, tab_own, tab_oth, out_ref, outt_ref, tab_s = refs[n:]
    tokens = tab_own.shape[0]
    step = out_ref.shape[0]

    @pl.when(pl.program_id(0) == 0)
    def _():
        tab_s[span(s_ref[0], tokens), :] = tab_own[...]
        tab_s[span(1 - s_ref[0], tokens), :] = tab_oth[...]

    total = far_ref[...].astype(F32)
    for ref in refs[:n]:
        total = total + ref[:, 0].astype(F32)
    cos_t, sin_t = spread_table(tab_s[span(pl.program_id(0), step), :])
    dk = total[0].astype(BF).astype(F32).T
    dk = (dk * cos_t - swap_halves(dk) * sin_t).astype(BF)
    dvt = total[1].astype(BF)
    out_ref[:, :HEAD] = dk
    out_ref[:, HEAD:] = dvt.T
    outt_ref[:HEAD, :] = dk.T
    outt_ref[HEAD:, :] = dvt


def kv_finish(core, parts, far, tab_own, tab_oth):
    tokens = tab_own.shape[0]
    chip_len = 2 * tokens
    step = 512
    return pl.pallas_call(
        functools.partial(kv_finish_kernel, len(parts)),
        grid_spec=pltpu.PrefetchScalarGridSpec(
            num_scalar_prefetch=1,
            grid=(chip_len // step,),
            in_specs=[pl.BlockSpec((2, 1, HEAD, step), lambda t, s: (0, 1, 0, t))] * len(parts)
            + [
                pl.BlockSpec((2, HEAD, step), lambda t, s: (0, 0, t)),
                pl.BlockSpec((tokens, HEAD), lambda t, s: (0, 0)),
                pl.BlockSpec((tokens, HEAD), lambda t, s: (0, 0)),
            ],
            out_specs=[
                pl.BlockSpec((step, 2 * HEAD), lambda t, s: (t, 0)),
                pl.BlockSpec((2 * HEAD, step), lambda t, s: (0, t)),
            ],
            scratch_shapes=[pltpu.VMEM((chip_len, HEAD), F32)],
        ),
        out_shape=[
            jax.ShapeDtypeStruct((chip_len, 2 * HEAD), BF),
            jax.ShapeDtypeStruct((2 * HEAD, chip_len), BF),
        ],
        compiler_params=params(),
        cost_estimate=cost(chip_len * HEAD * 64, chip_len * HEAD * 16),
        name="kv_finish",
    )(core, *parts, far, tab_own, tab_oth)


def kvgrad_kernel(s_ref, dkvt_ref, x_own, x_oth, out_ref):
    tokens = x_own.shape[0]
    own, oth = span(s_ref[0], tokens), span(1 - s_ref[0], tokens)
    out_ref[...] = (dot_nn(dkvt_ref[:, own], x_own[...]) + dot_nn(dkvt_ref[:, oth], x_oth[...])).astype(BF)


def kvgrad(core, dkvt, x_own, x_oth):
    tokens, width = x_own.shape
    step = 512
    piece = pl.BlockSpec((tokens, step), lambda n, s: (0, n))
    return pl.pallas_call(
        kvgrad_kernel,
        grid_spec=pltpu.PrefetchScalarGridSpec(
            num_scalar_prefetch=1,
            grid=(width // step,),
            in_specs=[pl.BlockSpec((2 * HEAD, 2 * tokens), lambda n, s: (0, 0)), piece, piece],
            out_specs=pl.BlockSpec((2 * HEAD, step), lambda n, s: (0, n)),
        ),
        out_shape=jax.ShapeDtypeStruct((2 * HEAD, width), BF),
        compiler_params=params(),
        cost_estimate=cost(4 * tokens * width * 2 * HEAD, 4 * tokens * width),
        name="kvgrad",
    )(core, dkvt, x_own, x_oth)


def kv_combine_kernel(s_ref, a_ref, b_ref, c_ref, d_ref, gk_ref, gv_ref):
    for place, u_ref, v_ref in ((s_ref[0], a_ref, b_ref), (1 - s_ref[0], c_ref, d_ref)):
        total = u_ref[...].astype(F32) + v_ref[...].astype(F32)
        where = span(place, HEAD)
        gk_ref[:, where] = total[:HEAD, :].T
        gv_ref[:, where] = total[HEAD:, :].T


def kv_combine(core, parts):
    rows, width = parts[0].shape
    step = 1024
    out = jax.ShapeDtypeStruct((width, rows), F32)
    return pl.pallas_call(
        kv_combine_kernel,
        grid_spec=pltpu.PrefetchScalarGridSpec(
            num_scalar_prefetch=1,
            grid=(width // step,),
            in_specs=[pl.BlockSpec((rows, step), lambda n, s: (0, n))] * 4,
            out_specs=[pl.BlockSpec((step, rows), lambda n, s: (n, 0))] * 2,
        ),
        out_shape=[out, out],
        compiler_params=params(),
        cost_estimate=cost(16 * width * rows * 16, 16 * width * rows),
        name="kv_combine",
    )(core, *parts)


def combine_kernel(s_ref, a_ref, b_ref, c_ref, d_ref, *rest):
    gq_ref, go_ref = rest[-2:]

    def put(u_ref, v_ref):
        def part(c, carry):
            cols = span(c, 256)
            gq_ref[cols, :] = (u_ref[0, :, cols].astype(F32) + v_ref[0, :, cols].astype(F32)).T
            go_ref[:, cols] = u_ref[1, :, cols].astype(F32) + v_ref[1, :, cols].astype(F32)
            return carry

        lax.fori_loop(0, u_ref.shape[2] // 256, part, 0)

    @pl.when(pl.program_id(0) == 0)
    def _():
        put(a_ref, b_ref)

    @pl.when(pl.program_id(0) == 1)
    def _():
        put(c_ref, d_ref)


def combine(core, chunk, n_chunks, parts, prev):
    width = parts[0].shape[2]
    step = 1024
    last = width // step - 1
    near = pl.BlockSpec((2, WIDE, step), lambda w, r, s: (0, 0, r + w * (last - r)))
    far = pl.BlockSpec((2, WIDE, step), lambda w, r, s: (0, 0, r * w))

    def place(w, s):
        return (s[0] + w - 2 * s[0] * w) * n_chunks + chunk

    shape = jax.ShapeDtypeStruct((width, 2 * n_chunks * WIDE), F32)
    shape_o = jax.ShapeDtypeStruct((2 * n_chunks * WIDE, width), F32)
    extra = [] if prev is None else list(prev)
    return pl.pallas_call(
        combine_kernel,
        grid_spec=pltpu.PrefetchScalarGridSpec(
            num_scalar_prefetch=1,
            grid=(2, width // step),
            in_specs=[near, near, far, far] + [pl.BlockSpec(memory_space=pl.ANY)] * len(extra),
            out_specs=[
                pl.BlockSpec((step, WIDE), lambda w, r, s: (r, place(w, s))),
                pl.BlockSpec((WIDE, step), lambda w, r, s: (place(w, s), r)),
            ],
        ),
        out_shape=[shape, shape_o],
        input_output_aliases={} if prev is None else {5: 0, 6: 1},
        compiler_params=params(),
        cost_estimate=cost(16 * width * WIDE * 64, 32 * width * WIDE),
        name="combine",
    )(core, *parts, *extra)


def fill_heads(core, own_refs, oth_refs, lhs):
    n = len(own_refs)
    for j in range(n):
        lhs[:, pl.ds(pl.multiple_of((core * n + j) * WIDE, WIDE), WIDE)] = own_refs[j][0]
        lhs[:, pl.ds(pl.multiple_of(((1 - core) * n + j) * WIDE, WIDE), WIDE)] = oth_refs[j][0]


def attn_out_kernel(n, s_ref, *refs):
    own_refs, oth_refs = refs[:n], refs[n:2 * n]
    wo_ref, out_ref, lhs = refs[2 * n:]

    @pl.when(pl.program_id(0) == 0)
    def _():
        fill_heads(s_ref[0], own_refs, oth_refs, lhs)

    out_ref[...] = dot_nn(lhs[...], wo_ref[...]).astype(BF)


def attn_out(core, own, oth, w_o):
    n = len(own)
    tokens = own[0].shape[1] // 2
    heads, width = w_o.shape
    step = 512
    return pl.pallas_call(
        functools.partial(attn_out_kernel, n),
        grid_spec=pltpu.PrefetchScalarGridSpec(
            num_scalar_prefetch=1,
            grid=(width // step,),
            in_specs=[pl.BlockSpec((1, tokens, WIDE), lambda k, s: (0, s[0], 0))] * (2 * n)
            + [pl.BlockSpec((heads, step), lambda k, s: (0, k))],
            out_specs=pl.BlockSpec((tokens, step), lambda k, s: (0, k)),
            scratch_shapes=[pltpu.VMEM((tokens, heads), BF)],
        ),
        out_shape=jax.ShapeDtypeStruct((tokens, width), BF),
        compiler_params=params(),
        cost_estimate=cost(2 * tokens * heads * width, 2 * heads * width + 4 * tokens * width),
        name="attn_out",
    )(core, *own, *oth, w_o)


def hidden_kernel(n, s_ref, *refs):
    own_refs, oth_refs = refs[:n], refs[n:2 * n]
    kv_own, kv_oth, wq_ref, wk_ref, wv_ref, out_ref, lhs, klhs, vlhs = refs[2 * n:]
    core = s_ref[0]

    @pl.when(pl.program_id(0) == 0)
    def _():
        fill_heads(core, own_refs, oth_refs, lhs)
        for place, ref in ((core, kv_own), (1 - core, kv_oth)):
            where = pl.ds(pl.multiple_of(place * HEAD, HEAD), HEAD)
            klhs[:, where] = ref[:, :HEAD]
            vlhs[:, where] = ref[:, HEAD:]

    out_ref[...] = (
        dot_nt(lhs[...], wq_ref[...]) + dot_nt(klhs[...], wk_ref[...]) + dot_nt(vlhs[...], wv_ref[...])
    ).astype(BF)


def grad_hidden(core, own, oth, kv_own, kv_oth, w_q, w_k, w_v):
    n = len(own)
    tokens = own[0].shape[1] // 2
    width, heads = w_q.shape
    kv_cols = w_k.shape[1]
    step = 512
    return pl.pallas_call(
        functools.partial(hidden_kernel, n),
        grid_spec=pltpu.PrefetchScalarGridSpec(
            num_scalar_prefetch=1,
            grid=(width // step,),
            in_specs=[pl.BlockSpec((1, tokens, WIDE), lambda k, s: (1, s[0], 0))] * (2 * n)
            + [pl.BlockSpec((tokens, 2 * HEAD), lambda k, s: (s[0], 0))] * 2
            + [
                pl.BlockSpec((step, heads), lambda k, s: (k, 0)),
                pl.BlockSpec((step, kv_cols), lambda k, s: (k, 0)),
                pl.BlockSpec((step, kv_cols), lambda k, s: (k, 0)),
            ],
            out_specs=pl.BlockSpec((tokens, step), lambda k, s: (0, k)),
            scratch_shapes=[
                pltpu.VMEM((tokens, heads), BF),
                pltpu.VMEM((tokens, kv_cols), BF),
                pltpu.VMEM((tokens, kv_cols), BF),
            ],
        ),
        out_shape=jax.ShapeDtypeStruct((tokens, width), BF),
        compiler_params=params(),
        cost_estimate=cost(2 * tokens * (heads + 2 * kv_cols) * width, 2 * heads * width + 4 * tokens * width),
        name="grad_hidden",
    )(core, *own, *oth, kv_own, kv_oth, w_q, w_k, w_v)


def solution(mesh):
    n_dev = mesh.shape["sp"]
    n_chunks = 4
    near_perm = [(d, d ^ 1) for d in range(n_dev)]
    far_perm = [(d, d ^ 2) for d in range(n_dev)]
    down_perm = [(0, 2), (1, 3)]
    up_perm = [(2, 0), (3, 1)]

    def near(v):
        return lax.ppermute(v, "sp", near_perm)

    def far(v):
        return lax.ppermute(v, "sp", far_perm)

    def device_step(hidden, grad_out, positions, doc_ids, w_q, w_k, w_v, w_o):
        tokens = hidden.shape[0]
        chip_len = 2 * tokens
        assert n_chunks == w_q.shape[1] // (2 * WIDE)
        place = lax.axis_index("sp")
        core_id, chip_id = place & 1, place >> 1
        core = core_id.astype(jnp.int32)[None]
        sel_own = jnp.stack([core_id, core_id]).astype(jnp.int32)
        sel_oth = jnp.stack([core_id, 1 - core_id]).astype(jnp.int32)

        doc_oth = near(doc_ids)
        doc_far = far(doc_ids)
        doc_far_oth = lax.ppermute(doc_ids, "sp", [(d, d ^ 3) for d in range(n_dev)])
        x_oth = near(hidden)
        g_oth = near(grad_out)
        tab_own = rope_table(positions)
        tab_oth = near(tab_own)
        kv_own, q = qkv_proj(sel_own, hidden, w_q, w_k, w_v, tab_own, None)
        kvp_own = lax.ppermute(kv_own, "sp", down_perm)

        def in_order(own, oth):
            return jnp.where(core_id == 0, jnp.concatenate([own, oth]), jnp.concatenate([oth, own]))

        doc_chip, doc_far = in_order(doc_ids, doc_oth), in_order(doc_far, doc_far_oth)
        kv_oth, q = qkv_proj(sel_oth, x_oth, w_q, w_k, w_v, tab_oth, q)
        kvp_oth = lax.ppermute(kv_oth, "sp", down_perm)
        dctx = dctx_proj(core, grad_out, g_oth, w_o)

        heads_doc = doc_chip[::BQ]
        lo = jnp.sum(doc_chip[None, :] < heads_doc[:, None], axis=1, dtype=jnp.int32)
        lo_far = jnp.sum(doc_far[None, :] < heads_doc[:, None], axis=1, dtype=jnp.int32)
        lo = lo + jnp.where(chip_id == 0, chip_len, lo_far)
        lo = (lo >> (ALIGN.bit_length() - 1)) << (ALIGN.bit_length() - 1)
        end = chip_len + BQ * (1 + jnp.arange(chip_len // BQ, dtype=jnp.int32))
        n_blocks = (end - lo + BK - 1) >> (BK.bit_length() - 1)
        kdoc = jnp.concatenate([doc_far, doc_chip, jnp.zeros((BK,), jnp.int32)])[None, :]

        acts, acts_oth, dkvs, sums = [], [], [], None
        for j in range(n_chunks):
            act, part, dkv = attention(
                j, core, lo, n_blocks, q, dctx, kdoc, (tab_own, tab_oth), (kvp_own, kvp_oth), (kv_own, kv_oth),
                (hidden, x_oth), (grad_out, g_oth),
            )
            part = part.reshape(2, WIDE, -1)
            acts.append(act)
            dkvs.append(dkv.reshape(2, 2, HEAD, chip_len))
            if j == n_chunks - 1:
                dkv_up = (dkv_early + dkvs[j][:, 0].astype(F32)).astype(BF)
                dkv_far = lax.ppermute(dkv_up, "sp", up_perm)
            if j == n_chunks - 2:
                dkv_early = lax.optimization_barrier(sum(d[:, 0].astype(F32) for d in dkvs))
            acts_oth.append(near(act))
            part_far = far(part)
            part_near = near(part)
            part_far_near = near(part_far)
            sums = combine(core, j, n_chunks, (part, part_far, part_near, part_far_near), sums)
        grad_wq, grad_wo = sums

        dkv, dkvt = kv_finish(core, dkvs, dkv_far, tab_own, tab_oth)
        dkv_oth = near(dkv)
        kv_part = kvgrad(core, dkvt, hidden, x_oth)
        kv_part_far = far(kv_part)
        kv_part_near = near(kv_part)
        kv_part_far_near = near(kv_part_far)
        grad_wk, grad_wv = kv_combine(core, (kv_part, kv_part_far, kv_part_near, kv_part_far_near))
        out = attn_out(core, acts, acts_oth, w_o)
        g_hidden = grad_hidden(core, acts, acts_oth, dkv, dkv_oth, w_q, w_k, w_v)
        return out, g_hidden, grad_wq, grad_wk, grad_wv, grad_wo

    tok_spec = P(("dp", "sp"), None)
    vec_spec = P(("dp", "sp"))
    rep_spec = P(None, None)
    part_spec = P("dp", None)


    return jax.shard_map(
        device_step,
        mesh=mesh,
        in_specs=(tok_spec, tok_spec, vec_spec, vec_spec, rep_spec, rep_spec, rep_spec, rep_spec),
        out_specs=(tok_spec, tok_spec, part_spec, part_spec, part_spec, part_spec),
        check_vma=False,
    )
```

```python
import functools

import jax
import jax.numpy as jnp
from jax import lax
from jax.experimental import pallas as pl
from jax.experimental.pallas import tpu as pltpu
from jax.sharding import PartitionSpec as P

HEAD = 128
ROPE_THETA = 500000.0
ROPE_FACTOR = 8.0
ROPE_LOW = 1.0
ROPE_HIGH = 4.0
ROPE_OLD_CTX = 8192.0
NEG_BIG = float("-inf")
SCALE = HEAD ** -0.5
LOG2E = 1.4426950408889634

PAIR = 2
WIDE = PAIR * HEAD
BQ = 512
BK = 512
MIX = 16
ALIGN = 128
BF = jnp.bfloat16
F32 = jnp.float32


def rope_freqs():
    half_idx = jnp.arange(HEAD // 2, dtype=F32)
    inv_freq = jnp.power(ROPE_THETA, -2.0 * half_idx / HEAD)
    wavelen = 2.0 * jnp.pi / inv_freq
    smooth = (ROPE_OLD_CTX / wavelen - ROPE_LOW) / (ROPE_HIGH - ROPE_LOW)
    mixed_freq = (1.0 - smooth) * inv_freq / ROPE_FACTOR + smooth * inv_freq
    scaled = jnp.where(wavelen > ROPE_OLD_CTX / ROPE_LOW, inv_freq / ROPE_FACTOR, mixed_freq)
    return jnp.where(wavelen < ROPE_OLD_CTX / ROPE_HIGH, inv_freq, scaled)


def rope_table(pos_vec):
    angles = pos_vec.astype(F32)[:, None] * rope_freqs()[None, :]
    return jnp.concatenate([jnp.cos(angles), jnp.sin(angles)], axis=-1)


def dot_nn(a, b):
    return lax.dot_general(a, b, (((1,), (0,)), ((), ())), preferred_element_type=F32)


def dot_nt(a, b):
    return lax.dot_general(a, b, (((1,), (1,)), ((), ())), preferred_element_type=F32)


def swap_halves(v):
    return pltpu.roll(v, HEAD // 2, 1)


def spread_table(tab):
    low = lax.broadcasted_iota(jnp.int32, tab.shape, 1) < HEAD // 2
    other = swap_halves(tab)
    return jnp.where(low, tab, other), jnp.where(low, -other, tab)


def cost(flops, nbytes, trans=0):
    return pl.CostEstimate(flops=int(flops), bytes_accessed=int(nbytes), transcendentals=int(trans))


def params(**kw):
    return pltpu.CompilerParams(vmem_limit_bytes=67_000_000, **kw)


def by_rows(rows, body, size=16):
    def step(r, carry):
        body(span(r, size))
        return carry

    lax.fori_loop(0, rows // size, step, 0)


def span(index, size):
    return pl.ds(pl.multiple_of(index * size, size), size)


def qkv_kernel(s_ref, x_ref, wq_ref, wk_ref, wv_ref, tab_ref, *rest):
    kv_ref, q_ref, w_s = rest[-3:]
    part = pl.program_id(0)

    @pl.when((part == 0) & (pl.program_id(1) == 0))
    def _():
        w_s[:, :HEAD] = wk_ref[...]
        w_s[:, HEAD:] = wv_ref[...]

    @pl.when(part == 0)
    def _():
        kv = dot_nn(x_ref[...], w_s[...])
        cos_t, sin_t = spread_table(tab_ref[...])
        k = kv[:, :HEAD]
        kv_ref[:, :HEAD] = (k * cos_t + swap_halves(k) * sin_t).astype(BF)
        kv_ref[:, HEAD:] = kv[:, HEAD:].astype(BF)

    @pl.when(part > 0)
    def _():
        q = dot_nn(x_ref[...], wq_ref[...])
        cos_t, sin_t = spread_table(tab_ref[...])
        for h in range(wq_ref.shape[1] // HEAD):
            head = q[:, h * HEAD:(h + 1) * HEAD]
            q_ref[:, h * HEAD:(h + 1) * HEAD] = (head * cos_t + swap_halves(head) * sin_t).astype(BF)


def qkv_proj(own, core, x, w_q, w_k, w_v, tab, prev):
    tokens, width = x.shape
    cols = w_q.shape[1] // 2
    step, rows = 512, 256
    n, m_all = cols // step, tokens // rows
    extra = [] if prev is None else [prev]

    def q_place(p, m, s):
        half = s[0] if own else 1 - s[0]
        return half * m_all + jnp.where(p == 0, 0, m), jnp.maximum(p - 1, 0)

    return pl.pallas_call(
        qkv_kernel,
        grid_spec=pltpu.PrefetchScalarGridSpec(
            num_scalar_prefetch=1,
            grid=(n + 1, m_all),
            in_specs=[
                pl.BlockSpec((rows, width), lambda p, m, s: (m, 0)),
                pl.BlockSpec((width, step), lambda p, m, s: (0, s[0] * n + jnp.maximum(p - 1, 0))),
                pl.BlockSpec((width, HEAD), lambda p, m, s: (0, s[0])),
                pl.BlockSpec((width, HEAD), lambda p, m, s: (0, s[0])),
                pl.BlockSpec((rows, HEAD), lambda p, m, s: (m, 0)),
            ] + [pl.BlockSpec(memory_space=pl.ANY)] * len(extra),
            out_specs=[
                pl.BlockSpec((rows, 2 * HEAD), lambda p, m, s: (jnp.where(p == 0, m, m_all - 1), 0)),
                pl.BlockSpec((rows, step), q_place),
            ],
            scratch_shapes=[pltpu.VMEM((width, 2 * HEAD), BF)],
        ),
        out_shape=[
            jax.ShapeDtypeStruct((tokens, 2 * HEAD), BF),
            jax.ShapeDtypeStruct((2 * tokens, cols), BF),
        ],
        input_output_aliases={} if prev is None else {6: 1},
        compiler_params=params(),
        cost_estimate=cost(2 * tokens * width * (cols + 2 * HEAD), tokens * width * 2 + cols * width * 2),
        name="qkv_proj",
    )(core, x, w_q, w_k, w_v, tab, *extra)


def dctx_kernel(steps, s_ref, own_ref, oth_ref, wo_ref, out_ref):
    @pl.when(pl.program_id(1) < steps)
    def _():
        out_ref[...] = dot_nt(own_ref[...], wo_ref[...]).astype(BF)

    @pl.when(pl.program_id(1) >= steps)
    def _():
        out_ref[...] = dot_nt(oth_ref[...], wo_ref[...]).astype(BF)


def dctx_proj(core, own, oth, w_o):
    tokens, width = own.shape
    cols = w_o.shape[0] // 2
    step, rows = 512, 256
    n, m_all = cols // step, tokens // rows

    def place(m, s):
        far = m // m_all
        return (s[0] + far - 2 * s[0] * far) * m_all + m % m_all

    return pl.pallas_call(
        functools.partial(dctx_kernel, m_all),
        grid_spec=pltpu.PrefetchScalarGridSpec(
            num_scalar_prefetch=1,
            grid=(n, 2 * m_all),
            in_specs=[
                pl.BlockSpec((rows, width), lambda p, m, s: (jnp.minimum(m, m_all - 1), 0)),
                pl.BlockSpec((rows, width), lambda p, m, s: (jnp.maximum(m - m_all, 0), 0)),
                pl.BlockSpec((step, width), lambda p, m, s: (s[0] * n + p, 0)),
            ],
            out_specs=pl.BlockSpec((rows, step), lambda p, m, s: (place(m, s), p)),
        ),
        out_shape=jax.ShapeDtypeStruct((2 * tokens, cols), BF),
        compiler_params=params(),
        cost_estimate=cost(4 * tokens * width * cols, tokens * width * 4 + cols * width * 2),
        name="dctx_proj",
    )(core, own, oth, w_o)


def attn_kernel(
    first, core_ref, lo_ref, nb_ref, q_ref, do_ref, kdoc_ref, tab_own, tab_oth, kvp_own, kvp_oth, kvc_own, kvc_oth,
    x_own, x_oth, g_own, g_oth, before_ref, act_ref, part_ref, dkv_ref,
    k_s, v_s, s_s, dp_s, m_s, l_s, d_s, qd_s, ahead_s, ctx_s, dq_s, q_s, do_s, qt_s, dot_s, tab_s, dk_s, dv_s,
    x_s, g_s, at_s, w_s, before_s, init_sem, row_sem, out_sem,
):
    before_copy = pltpu.make_async_copy(before_ref, before_s, out_sem.at[2])
    i = pl.program_id(0)
    tokens = kvc_own.shape[0]
    chip_len = 2 * tokens
    core = core_ref[0]
    per_half = tokens // BQ
    rows_here = span(i % per_half, BQ)

    def row_copies(x, g):
        return (
            pltpu.make_async_copy(x.at[rows_here, :], x_s, row_sem.at[0]),
            pltpu.make_async_copy(g.at[rows_here, :], g_s, row_sem.at[1]),
        )

    def init_copies():
        moves = []
        for base, place, ref in ((0, core, kvp_own), (0, 1 - core, kvp_oth), (2, core, kvc_own), (2, 1 - core, kvc_oth)):
            moves.append((ref.at[:, pl.ds(0, HEAD)], k_s.at[span(base + place, tokens), :]))
        for base, place, ref in ((0, core, kvp_own), (0, 1 - core, kvp_oth), (2, core, kvc_own), (2, 1 - core, kvc_oth)):
            moves.append((ref.at[:, pl.ds(HEAD, HEAD)], v_s.at[span(base + place, tokens), :]))
        moves.append((tab_own, tab_s.at[span(core, tokens), :]))
        moves.append((tab_oth, tab_s.at[span(1 - core, tokens), :]))
        return [pltpu.make_async_copy(src, dst, init_sem.at[n]) for n, (src, dst) in enumerate(moves)]

    def arrive(first, last):
        @pl.when(i == 0)
        def _():
            for copy in init_copies()[first:last]:
                copy.wait()

    @pl.when(i == 0)
    def _():
        for copy in init_copies():
            copy.start()
        if not first:
            before_copy.start()
        k_s[2 * chip_len:, :] = jnp.zeros((BK, HEAD), BF)
        v_s[2 * chip_len:, :] = jnp.zeros((BK, HEAD), BF)

        def clear(r):
            w_s[r, :] = jnp.zeros((16, w_s.shape[1]), F32)

        def clear_kv(r):
            dk_s[r, :] = jnp.zeros((16, dk_s.shape[1]), F32)
            dv_s[r, :] = jnp.zeros((16, dv_s.shape[1]), F32)

        def order(r):
            row = lax.broadcasted_iota(jnp.int32, (16, BK), 0)
            ahead_s[r, :] = lax.broadcasted_iota(jnp.int32, (16, BK), 1) - row - r.start

        by_rows(BQ, order)
        by_rows(w_s.shape[0], clear)
        by_rows(HEAD, clear_kv)

    @pl.when(i // per_half == core)
    def _():
        for copy in row_copies(x_own, g_own):
            copy.start()

    @pl.when(i // per_half != core)
    def _():
        for copy in row_copies(x_oth, g_oth):
            copy.start()

    def mixed(ref):
        parts = [ref[:, h * HEAD:(h + 1) * HEAD].reshape(BQ // MIX, 1, MIX, HEAD) for h in range(PAIR)]
        return jnp.concatenate(parts, axis=1).reshape(PAIR * BQ, HEAD)

    def apart(v, h):
        return v.reshape(BQ // MIX, PAIR, MIX, HEAD)[:, h].reshape(BQ, HEAD)

    q_mix, do_mix = mixed(q_ref), mixed(do_ref)
    q_s[...] = q_mix
    do_s[...] = do_mix
    qt_s[...] = q_mix.T
    dot_s[...] = do_mix.T
    qdoc = kdoc_ref[:, pl.ds(pl.multiple_of(chip_len + i * BQ, BQ), BQ)]
    qd_s[...] = jnp.broadcast_to(qdoc, (HEAD, BQ)).T
    m_s[...] = jnp.full(m_s.shape, NEG_BIG, F32)
    l_s[...] = jnp.zeros(l_s.shape, F32)
    d_s[...] = jnp.zeros(d_s.shape, F32)
    ctx_s[...] = jnp.zeros(ctx_s.shape, F32)
    dq_s[...] = jnp.zeros(dq_s.shape, F32)
    lo = lo_ref[i]
    n_blocks = nb_ref[i]
    lanes = BK // HEAD

    def fold(v, op):
        out = v[:, :HEAD]
        for n in range(1, lanes):
            out = op(out, v[:, n * HEAD:(n + 1) * HEAD])
        return out

    def spread(v):
        return jnp.concatenate([v] * lanes, axis=1)

    def offset(b):
        return pl.multiple_of(lo + b * BK, ALIGN)

    def scores(b, carry):
        off = offset(b)
        s = dot_nt(q_s[...], k_s[pl.ds(off, BK), :])
        limit = chip_len + i * BQ - off
        key_doc = kdoc_ref[:, pl.ds(off, BK)]
        for c in range(BQ // MIX):
            here = slice(c * MIX, (c + 1) * MIX)
            keep = (ahead_s[here, :] <= limit) & (key_doc == spread(qd_s[here, :]))
            shift = jnp.where(keep, 0.0, NEG_BIG)
            for h in range(PAIR):
                rows = slice((c * PAIR + h) * MIX, (c * PAIR + h + 1) * MIX)
                sh = s[rows, :] * (SCALE * LOG2E) + shift
                s_s[b, rows, :] = sh
                m_s[rows, :] = jnp.maximum(m_s[rows, :], fold(sh, jnp.maximum))
        return carry

    arrive(0, 4)
    lax.fori_loop(0, n_blocks, scores, 0)
    m_s[...] = jnp.broadcast_to(jnp.max(m_s[...], axis=1, keepdims=True), m_s.shape)

    def weights(b, carry):
        dp = dot_nt(do_s[...], v_s[pl.ds(offset(b), BK), :])
        e = jnp.exp2(s_s[b] - spread(m_s[...]))
        s_s[b] = e
        dp_s[b] = dp
        l_s[...] += fold(e, jnp.add)
        d_s[...] += fold(e * dp, jnp.add)
        return carry

    arrive(4, 10)
    lax.fori_loop(0, n_blocks, weights, 0)
    inv = 1.0 / jnp.sum(l_s[...], axis=1, keepdims=True)
    delta = jnp.sum(d_s[...], axis=1, keepdims=True) * inv
    l_s[...] = jnp.broadcast_to(inv, l_s.shape)
    d_s[...] = jnp.broadcast_to(delta, d_s.shape)

    def grads(b, carry):
        off = offset(b)
        p = s_s[b] * spread(l_s[...])
        pb = p.astype(BF)
        ds = (p * (dp_s[b] - spread(d_s[...])) * SCALE).astype(BF)
        ctx_s[...] += dot_nn(pb, v_s[pl.ds(off, BK), :])
        dq_s[...] += dot_nn(ds, k_s[pl.ds(off, BK), :])
        dv_s[:, pl.ds(off, BK)] += dot_nn(dot_s[...], pb)
        dk_s[:, pl.ds(off, BK)] += dot_nn(qt_s[...], ds)
        return carry

    lax.fori_loop(0, n_blocks, grads, 0)
    cos_t, sin_t = spread_table(tab_s[span(i, BQ), :])
    ctx_all, dq_all = ctx_s[...].astype(BF), dq_s[...].astype(BF).astype(F32)
    for h in range(PAIR):
        cols = slice(h * HEAD, (h + 1) * HEAD)
        ctx = apart(ctx_all, h)
        act_ref[0, :, cols] = ctx
        at_s[WIDE + h * HEAD:WIDE + (h + 1) * HEAD, :] = ctx.T
        dq = apart(dq_all, h)
        dq = (dq * cos_t - swap_halves(dq) * sin_t).astype(BF)
        act_ref[1, :, cols] = dq
        at_s[h * HEAD:(h + 1) * HEAD, :] = dq.T
    step = 4 * HEAD
    for copy in row_copies(x_own, g_own):
        copy.wait()

    def products(c, carry):
        cols = span(c, step)
        w_s[:WIDE, cols] += dot_nn(at_s[:WIDE, :], x_s[:, cols])
        w_s[WIDE:, cols] += dot_nn(at_s[WIDE:, :], g_s[:, cols])
        return carry

    lax.fori_loop(0, x_s.shape[1] // step, products, 0)

    @pl.when(i == pl.num_programs(0) - 1)
    def _():
        def narrow(r):
            x_s[r, :] = w_s[r, :].astype(BF)

        by_rows(w_s.shape[0], narrow)
        part_copy = pltpu.make_async_copy(x_s, part_ref, out_sem.at[0])
        part_copy.start()
        if not first:
            before_copy.wait()

        def narrow_kv(r, carry):
            rows = span(r, 16)
            for n, acc in enumerate((dk_s, dv_s)):
                for side in range(2):
                    at = pl.ds(pl.multiple_of((n + 2 * side) * HEAD + r * 16, 16), 16)
                    total = acc[rows, side * chip_len:(side + 1) * chip_len]
                    if not first:
                        total = total + before_s[at, :].astype(F32)
                    g_s[at, :] = total.astype(BF)
            return carry

        lax.fori_loop(0, HEAD // 16, narrow_kv, 0)
        dkv_copy = pltpu.make_async_copy(g_s, dkv_ref, out_sem.at[1])
        dkv_copy.start()
        part_copy.wait()
        dkv_copy.wait()


def attention(chunk, core, lo, n_blocks, q, dctx, kdoc, tabs, kv_prev, kv_chip, xs, gs, before):
    first = before is None
    chip_len = q.shape[0]
    width = xs[0].shape[1]
    assert 2 * WIDE == BQ == 4 * HEAD and width == chip_len
    padded = 2 * chip_len + BK
    max_blocks = 2 * chip_len // BK
    rows = PAIR * BQ
    full = lambda shape: pl.BlockSpec(shape, lambda i, *s: (0,) * len(shape))
    pairs = chip_len * chip_len * PAIR
    return pl.pallas_call(
        functools.partial(attn_kernel, first),
        grid_spec=pltpu.PrefetchScalarGridSpec(
            num_scalar_prefetch=3,
            grid=(chip_len // BQ,),
            in_specs=[
                pl.BlockSpec((BQ, WIDE), lambda i, *s: (i, chunk)),
                pl.BlockSpec((BQ, WIDE), lambda i, *s: (i, chunk)),
                full((1, padded)),
            ] + [pl.BlockSpec(memory_space=pl.ANY)] * 11,
            out_specs=[
                pl.BlockSpec((2, BQ, WIDE), lambda i, *s: (0, i, 0)),
                pl.BlockSpec(memory_space=pl.ANY),
                pl.BlockSpec(memory_space=pl.ANY),
            ],
            scratch_shapes=[
                pltpu.VMEM((padded, HEAD), BF),
                pltpu.VMEM((padded, HEAD), BF),
                pltpu.VMEM((max_blocks, rows, BK), F32),
                pltpu.VMEM((max_blocks, rows, BK), F32),
                pltpu.VMEM((rows, HEAD), F32),
                pltpu.VMEM((rows, HEAD), F32),
                pltpu.VMEM((rows, HEAD), F32),
                pltpu.VMEM((BQ, HEAD), jnp.int32),
                pltpu.VMEM((BQ, BK), jnp.int32),
                pltpu.VMEM((rows, HEAD), F32),
                pltpu.VMEM((rows, HEAD), F32),
                pltpu.VMEM((rows, HEAD), BF),
                pltpu.VMEM((rows, HEAD), BF),
                pltpu.VMEM((HEAD, rows), BF),
                pltpu.VMEM((HEAD, rows), BF),
                pltpu.VMEM((chip_len, HEAD), F32),
                pltpu.VMEM((HEAD, padded), F32),
                pltpu.VMEM((HEAD, padded), F32),
                pltpu.VMEM((BQ, width), BF),
                pltpu.VMEM((BQ, width), BF),
                pltpu.VMEM((2 * WIDE, BQ), BF),
                pltpu.VMEM((2 * WIDE, width), F32),
                pltpu.VMEM((4 * HEAD, chip_len), BF),
                pltpu.SemaphoreType.DMA((10,)),
                pltpu.SemaphoreType.DMA((2,)),
                pltpu.SemaphoreType.DMA((3,)),
            ],
        ),
        out_shape=[
            jax.ShapeDtypeStruct((2, chip_len, WIDE), BF),
            jax.ShapeDtypeStruct((2 * WIDE, width), BF),
            jax.ShapeDtypeStruct((4 * HEAD, chip_len), BF),
        ],
        compiler_params=params(),
        cost_estimate=cost(pairs * HEAD * 2 * 8, 12 * 1024 * 1024, pairs),
        name="attention",
    )(core, lo, n_blocks, q, dctx, kdoc, *tabs, *kv_prev, *kv_chip, *xs, *gs, gs[0] if first else before)


def kv_finish_kernel(s_ref, near_ref, far_ref, tab_own, tab_oth, out_ref, outt_ref, tab_s):
    tokens = tab_own.shape[0]
    step = out_ref.shape[0]

    @pl.when(pl.program_id(0) == 0)
    def _():
        tab_s[span(s_ref[0], tokens), :] = tab_own[...]
        tab_s[span(1 - s_ref[0], tokens), :] = tab_oth[...]

    total = near_ref[...].astype(F32) + far_ref[...].astype(F32)
    cos_t, sin_t = spread_table(tab_s[span(pl.program_id(0), step), :])
    dk = total[:HEAD].astype(BF).astype(F32).T
    dk = (dk * cos_t - swap_halves(dk) * sin_t).astype(BF)
    dvt = total[HEAD:].astype(BF)
    out_ref[:, :HEAD] = dk
    out_ref[:, HEAD:] = dvt.T
    outt_ref[:HEAD, :] = dk.T
    outt_ref[HEAD:, :] = dvt


def kv_finish(core, near, far, tab_own, tab_oth):
    tokens = tab_own.shape[0]
    chip_len = 2 * tokens
    step = 512
    return pl.pallas_call(
        kv_finish_kernel,
        grid_spec=pltpu.PrefetchScalarGridSpec(
            num_scalar_prefetch=1,
            grid=(chip_len // step,),
            in_specs=[
                pl.BlockSpec((2 * HEAD, step), lambda t, s: (1, t)),
                pl.BlockSpec((2 * HEAD, step), lambda t, s: (0, t)),
                pl.BlockSpec((tokens, HEAD), lambda t, s: (0, 0)),
                pl.BlockSpec((tokens, HEAD), lambda t, s: (0, 0)),
            ],
            out_specs=[
                pl.BlockSpec((step, 2 * HEAD), lambda t, s: (t, 0)),
                pl.BlockSpec((2 * HEAD, step), lambda t, s: (0, t)),
            ],
            scratch_shapes=[pltpu.VMEM((chip_len, HEAD), F32)],
        ),
        out_shape=[
            jax.ShapeDtypeStruct((chip_len, 2 * HEAD), BF),
            jax.ShapeDtypeStruct((2 * HEAD, chip_len), BF),
        ],
        compiler_params=params(),
        cost_estimate=cost(chip_len * HEAD * 64, chip_len * HEAD * 16),
        name="kv_finish",
    )(core, near, far, tab_own, tab_oth)


def kvgrad_kernel(s_ref, dkvt_ref, x_own, x_oth, out_ref):
    tokens = x_own.shape[0]
    own, oth = span(s_ref[0], tokens), span(1 - s_ref[0], tokens)
    out_ref[...] = (dot_nn(dkvt_ref[:, own], x_own[...]) + dot_nn(dkvt_ref[:, oth], x_oth[...])).astype(BF)


def kvgrad(core, dkvt, x_own, x_oth):
    tokens, width = x_own.shape
    step = 512
    piece = pl.BlockSpec((tokens, step), lambda n, s: (0, n))
    return pl.pallas_call(
        kvgrad_kernel,
        grid_spec=pltpu.PrefetchScalarGridSpec(
            num_scalar_prefetch=1,
            grid=(width // step,),
            in_specs=[pl.BlockSpec((2 * HEAD, 2 * tokens), lambda n, s: (0, 0)), piece, piece],
            out_specs=pl.BlockSpec((2 * HEAD, step), lambda n, s: (0, n)),
        ),
        out_shape=jax.ShapeDtypeStruct((2 * HEAD, width), BF),
        compiler_params=params(),
        cost_estimate=cost(4 * tokens * width * 2 * HEAD, 4 * tokens * width),
        name="kvgrad",
    )(core, dkvt, x_own, x_oth)


def kv_combine_kernel(s_ref, a_ref, b_ref, c_ref, d_ref, gk_ref, gv_ref):
    for place, u_ref, v_ref in ((s_ref[0], a_ref, b_ref), (1 - s_ref[0], c_ref, d_ref)):
        total = u_ref[...].astype(F32) + v_ref[...].astype(F32)
        where = span(place, HEAD)
        gk_ref[:, where] = total[:HEAD, :].T
        gv_ref[:, where] = total[HEAD:, :].T


def kv_combine(core, parts):
    rows, width = parts[0].shape
    step = 1024
    out = jax.ShapeDtypeStruct((width, rows), F32)
    return pl.pallas_call(
        kv_combine_kernel,
        grid_spec=pltpu.PrefetchScalarGridSpec(
            num_scalar_prefetch=1,
            grid=(width // step,),
            in_specs=[pl.BlockSpec((rows, step), lambda n, s: (0, n))] * 4,
            out_specs=[pl.BlockSpec((step, rows), lambda n, s: (n, 0))] * 2,
        ),
        out_shape=[out, out],
        compiler_params=params(),
        cost_estimate=cost(16 * width * rows * 16, 16 * width * rows),
        name="kv_combine",
    )(core, *parts)


def combine_kernel(s_ref, a_ref, b_ref, c_ref, d_ref, *rest):
    gq_ref, go_ref = rest[-2:]

    def put(u_ref, v_ref):
        def part(c, carry):
            cols = span(c, 256)
            gq_ref[cols, :] = (u_ref[0, :, cols].astype(F32) + v_ref[0, :, cols].astype(F32)).T
            go_ref[:, cols] = u_ref[1, :, cols].astype(F32) + v_ref[1, :, cols].astype(F32)
            return carry

        lax.fori_loop(0, u_ref.shape[2] // 256, part, 0)

    @pl.when(pl.program_id(0) == 0)
    def _():
        put(a_ref, b_ref)

    @pl.when(pl.program_id(0) == 1)
    def _():
        put(c_ref, d_ref)


def combine(core, chunk, n_chunks, parts, prev):
    width = parts[0].shape[2]
    step = 1024
    last = width // step - 1
    near = pl.BlockSpec((2, WIDE, step), lambda w, r, s: (0, 0, r + w * (last - r)))
    far = pl.BlockSpec((2, WIDE, step), lambda w, r, s: (0, 0, r * w))

    def place(w, s):
        return (s[0] + w - 2 * s[0] * w) * n_chunks + chunk

    shape = jax.ShapeDtypeStruct((width, 2 * n_chunks * WIDE), F32)
    shape_o = jax.ShapeDtypeStruct((2 * n_chunks * WIDE, width), F32)
    extra = [] if prev is None else list(prev)
    return pl.pallas_call(
        combine_kernel,
        grid_spec=pltpu.PrefetchScalarGridSpec(
            num_scalar_prefetch=1,
            grid=(2, width // step),
            in_specs=[near, near, far, far] + [pl.BlockSpec(memory_space=pl.ANY)] * len(extra),
            out_specs=[
                pl.BlockSpec((step, WIDE), lambda w, r, s: (r, place(w, s))),
                pl.BlockSpec((WIDE, step), lambda w, r, s: (place(w, s), r)),
            ],
        ),
        out_shape=[shape, shape_o],
        input_output_aliases={} if prev is None else {5: 0, 6: 1},
        compiler_params=params(),
        cost_estimate=cost(16 * width * WIDE * 64, 32 * width * WIDE),
        name="combine",
    )(core, *parts, *extra)


def fill_heads(core, own_refs, oth_refs, lhs):
    n = len(own_refs)
    for j in range(n):
        lhs[:, pl.ds(pl.multiple_of((core * n + j) * WIDE, WIDE), WIDE)] = own_refs[j][0]
        lhs[:, pl.ds(pl.multiple_of(((1 - core) * n + j) * WIDE, WIDE), WIDE)] = oth_refs[j][0]


def attn_out_kernel(n, s_ref, *refs):
    own_refs, oth_refs = refs[:n], refs[n:2 * n]
    wo_ref, out_ref, lhs = refs[2 * n:]

    @pl.when(pl.program_id(0) == 0)
    def _():
        fill_heads(s_ref[0], own_refs, oth_refs, lhs)

    out_ref[...] = dot_nn(lhs[...], wo_ref[...]).astype(BF)


def attn_out(core, own, oth, w_o):
    n = len(own)
    tokens = own[0].shape[1] // 2
    heads, width = w_o.shape
    step = 512
    return pl.pallas_call(
        functools.partial(attn_out_kernel, n),
        grid_spec=pltpu.PrefetchScalarGridSpec(
            num_scalar_prefetch=1,
            grid=(width // step,),
            in_specs=[pl.BlockSpec((1, tokens, WIDE), lambda k, s: (0, s[0], 0))] * (2 * n)
            + [pl.BlockSpec((heads, step), lambda k, s: (0, k))],
            out_specs=pl.BlockSpec((tokens, step), lambda k, s: (0, k)),
            scratch_shapes=[pltpu.VMEM((tokens, heads), BF)],
        ),
        out_shape=jax.ShapeDtypeStruct((tokens, width), BF),
        compiler_params=params(),
        cost_estimate=cost(2 * tokens * heads * width, 2 * heads * width + 4 * tokens * width),
        name="attn_out",
    )(core, *own, *oth, w_o)


def hidden_kernel(n, s_ref, *refs):
    own_refs, oth_refs = refs[:n], refs[n:2 * n]
    kv_own, kv_oth, wq_ref, wk_ref, wv_ref, out_ref, lhs, klhs, vlhs = refs[2 * n:]
    core = s_ref[0]

    @pl.when(pl.program_id(0) == 0)
    def _():
        fill_heads(core, own_refs, oth_refs, lhs)
        for place, ref in ((core, kv_own), (1 - core, kv_oth)):
            where = pl.ds(pl.multiple_of(place * HEAD, HEAD), HEAD)
            klhs[:, where] = ref[:, :HEAD]
            vlhs[:, where] = ref[:, HEAD:]

    out_ref[...] = (
        dot_nt(lhs[...], wq_ref[...]) + dot_nt(klhs[...], wk_ref[...]) + dot_nt(vlhs[...], wv_ref[...])
    ).astype(BF)


def grad_hidden(core, own, oth, kv_own, kv_oth, w_q, w_k, w_v):
    n = len(own)
    tokens = own[0].shape[1] // 2
    width, heads = w_q.shape
    kv_cols = w_k.shape[1]
    step = 512
    return pl.pallas_call(
        functools.partial(hidden_kernel, n),
        grid_spec=pltpu.PrefetchScalarGridSpec(
            num_scalar_prefetch=1,
            grid=(width // step,),
            in_specs=[pl.BlockSpec((1, tokens, WIDE), lambda k, s: (1, s[0], 0))] * (2 * n)
            + [pl.BlockSpec((tokens, 2 * HEAD), lambda k, s: (s[0], 0))] * 2
            + [
                pl.BlockSpec((step, heads), lambda k, s: (k, 0)),
                pl.BlockSpec((step, kv_cols), lambda k, s: (k, 0)),
                pl.BlockSpec((step, kv_cols), lambda k, s: (k, 0)),
            ],
            out_specs=pl.BlockSpec((tokens, step), lambda k, s: (0, k)),
            scratch_shapes=[
                pltpu.VMEM((tokens, heads), BF),
                pltpu.VMEM((tokens, kv_cols), BF),
                pltpu.VMEM((tokens, kv_cols), BF),
            ],
        ),
        out_shape=jax.ShapeDtypeStruct((tokens, width), BF),
        compiler_params=params(),
        cost_estimate=cost(2 * tokens * (heads + 2 * kv_cols) * width, 2 * heads * width + 4 * tokens * width),
        name="grad_hidden",
    )(core, *own, *oth, kv_own, kv_oth, w_q, w_k, w_v)


def solution(mesh):
    n_dev = mesh.shape["sp"]
    n_chunks = 4
    near_perm = [(d, d ^ 1) for d in range(n_dev)]
    far_perm = [(d, d ^ 2) for d in range(n_dev)]
    down_perm = [(0, 2), (1, 3)]
    up_perm = [(2, 0), (3, 1)]

    def near(v):
        return lax.ppermute(v, "sp", near_perm)

    def far(v):
        return lax.ppermute(v, "sp", far_perm)

    def device_step(hidden, grad_out, positions, doc_ids, w_q, w_k, w_v, w_o):
        tokens = hidden.shape[0]
        chip_len = 2 * tokens
        assert n_chunks == w_q.shape[1] // (2 * WIDE)
        place = lax.axis_index("sp")
        core_id, chip_id = place & 1, place >> 1
        core = core_id.astype(jnp.int32)[None]

        doc_oth = near(doc_ids)
        doc_far = far(doc_ids)
        doc_far_oth = lax.ppermute(doc_ids, "sp", [(d, d ^ 3) for d in range(n_dev)])
        x_oth = near(hidden)
        g_oth = near(grad_out)
        tab_own = rope_table(positions)
        tab_oth = near(tab_own)
        kv_own, q = qkv_proj(True, core, hidden, w_q, w_k, w_v, tab_own, None)
        kvp_own = lax.ppermute(kv_own, "sp", down_perm)

        def in_order(own, oth):
            return jnp.where(core_id == 0, jnp.concatenate([own, oth]), jnp.concatenate([oth, own]))

        doc_chip, doc_far = in_order(doc_ids, doc_oth), in_order(doc_far, doc_far_oth)
        kv_oth, q = qkv_proj(False, core, x_oth, w_q, w_k, w_v, tab_oth, q)
        kvp_oth = lax.ppermute(kv_oth, "sp", down_perm)
        dctx = dctx_proj(core, grad_out, g_oth, w_o)

        heads_doc = doc_chip[::BQ]
        lo = jnp.sum(doc_chip[None, :] < heads_doc[:, None], axis=1, dtype=jnp.int32)
        lo_far = jnp.sum(doc_far[None, :] < heads_doc[:, None], axis=1, dtype=jnp.int32)
        lo = lo + jnp.where(chip_id == 0, chip_len, lo_far)
        lo = (lo >> (ALIGN.bit_length() - 1)) << (ALIGN.bit_length() - 1)
        end = chip_len + BQ * (1 + jnp.arange(chip_len // BQ, dtype=jnp.int32))
        n_blocks = (end - lo + BK - 1) >> (BK.bit_length() - 1)
        kdoc = jnp.concatenate([doc_far, doc_chip, jnp.zeros((BK,), jnp.int32)])[None, :]

        acts, acts_oth, dkv_sum, sums = [], [], None, None
        for j in range(n_chunks):
            act, part, dkv = attention(
                j, core, lo, n_blocks, q, dctx, kdoc, (tab_own, tab_oth), (kvp_own, kvp_oth), (kv_own, kv_oth),
                (hidden, x_oth), (grad_out, g_oth), dkv_sum,
            )
            part = part.reshape(2, WIDE, -1)
            acts.append(act)
            dkv_sum = dkv
            if j == n_chunks - 1:
                dkv_up = dkv[:2 * HEAD]
                dkv_far = lax.ppermute(dkv_up, "sp", up_perm)
            acts_oth.append(near(act))
            part_far = far(part)
            part_near = near(part)
            part_far_near = near(part_far)
            sums = combine(core, j, n_chunks, (part, part_far, part_near, part_far_near), sums)
        grad_wq, grad_wo = sums

        dkv, dkvt = kv_finish(core, dkv_sum, dkv_far, tab_own, tab_oth)
        dkv_oth = near(dkv)
        kv_part = kvgrad(core, dkvt, hidden, x_oth)
        kv_part_far = far(kv_part)
        kv_part_near = near(kv_part)
        kv_part_far_near = near(kv_part_far)
        grad_wk, grad_wv = kv_combine(core, (kv_part, kv_part_far, kv_part_near, kv_part_far_near))
        out = attn_out(core, acts, acts_oth, w_o)
        g_hidden = grad_hidden(core, acts, acts_oth, dkv, dkv_oth, w_q, w_k, w_v)
        return out, g_hidden, grad_wq, grad_wk, grad_wv, grad_wo

    tok_spec = P(("dp", "sp"), None)
    vec_spec = P(("dp", "sp"))
    rep_spec = P(None, None)
    part_spec = P("dp", None)


    return jax.shard_map(
        device_step,
        mesh=mesh,
        in_specs=(tok_spec, tok_spec, vec_spec, vec_spec, rep_spec, rep_spec, rep_spec, rep_spec),
        out_specs=(tok_spec, tok_spec, part_spec, part_spec, part_spec, part_spec),
        check_vma=False,
    )
```

```python
import functools

import jax
import jax.numpy as jnp
from jax import lax
from jax.experimental import pallas as pl
from jax.experimental.pallas import tpu as pltpu
from jax.sharding import PartitionSpec as P

HEAD = 128
ROPE_THETA = 500000.0
ROPE_FACTOR = 8.0
ROPE_LOW = 1.0
ROPE_HIGH = 4.0
ROPE_OLD_CTX = 8192.0
NEG_BIG = float("-inf")
SCALE = HEAD ** -0.5
LOG2E = 1.4426950408889634

PAIR = 2
WIDE = PAIR * HEAD
BQ = 512
BK = 512
MIX = 16
ALIGN = 128
BF = jnp.bfloat16
F32 = jnp.float32


def rope_freqs():
    half_idx = jnp.arange(HEAD // 2, dtype=F32)
    inv_freq = jnp.power(ROPE_THETA, -2.0 * half_idx / HEAD)
    wavelen = 2.0 * jnp.pi / inv_freq
    smooth = (ROPE_OLD_CTX / wavelen - ROPE_LOW) / (ROPE_HIGH - ROPE_LOW)
    mixed_freq = (1.0 - smooth) * inv_freq / ROPE_FACTOR + smooth * inv_freq
    scaled = jnp.where(wavelen > ROPE_OLD_CTX / ROPE_LOW, inv_freq / ROPE_FACTOR, mixed_freq)
    return jnp.where(wavelen < ROPE_OLD_CTX / ROPE_HIGH, inv_freq, scaled)


def rope_table(pos_vec):
    angles = pos_vec.astype(F32)[:, None] * rope_freqs()[None, :]
    return jnp.concatenate([jnp.cos(angles), jnp.sin(angles)], axis=-1)


def dot_nn(a, b):
    return lax.dot_general(a, b, (((1,), (0,)), ((), ())), preferred_element_type=F32)


def dot_nt(a, b):
    return lax.dot_general(a, b, (((1,), (1,)), ((), ())), preferred_element_type=F32)


def swap_halves(v):
    return pltpu.roll(v, HEAD // 2, 1)


def spread_table(tab):
    low = lax.broadcasted_iota(jnp.int32, tab.shape, 1) < HEAD // 2
    other = swap_halves(tab)
    return jnp.where(low, tab, other), jnp.where(low, -other, tab)


def cost(flops, nbytes, trans=0):
    return pl.CostEstimate(flops=int(flops), bytes_accessed=int(nbytes), transcendentals=int(trans))


def params(**kw):
    return pltpu.CompilerParams(vmem_limit_bytes=67_000_000, **kw)


def by_rows(rows, body, size=16):
    def step(r, carry):
        body(span(r, size))
        return carry

    lax.fori_loop(0, rows // size, step, 0)


def span(index, size):
    return pl.ds(pl.multiple_of(index * size, size), size)


def qkv_kernel(s_ref, x_ref, wq_ref, wk_ref, wv_ref, tab_ref, *rest):
    kv_ref, q_ref, w_s = rest[-3:]

    @pl.when(pl.program_id(0) == 0)
    def _():
        w_s[:, :HEAD] = wk_ref[...]
        w_s[:, HEAD:] = wv_ref[...]

    x = x_ref[...]
    cos_t, sin_t = spread_table(tab_ref[...])
    kv = dot_nn(x, w_s[...])
    k = kv[:, :HEAD]
    kv_ref[:, :HEAD] = (k * cos_t + swap_halves(k) * sin_t).astype(BF)
    kv_ref[:, HEAD:] = kv[:, HEAD:].astype(BF)
    step = 4 * HEAD
    for n in range(wq_ref.shape[1] // step):
        q = dot_nn(x, wq_ref[:, n * step:(n + 1) * step])
        for h in range(step // HEAD):
            part = q[:, h * HEAD:(h + 1) * HEAD]
            at = n * step + h * HEAD
            q_ref[:, at:at + HEAD] = (part * cos_t + swap_halves(part) * sin_t).astype(BF)


def qkv_proj(own, core, x, w_q, w_k, w_v, tab, prev):
    tokens, width = x.shape
    cols = w_q.shape[1] // 2
    rows = tokens // 2
    extra = [] if prev is None else [prev]
    return pl.pallas_call(
        qkv_kernel,
        grid_spec=pltpu.PrefetchScalarGridSpec(
            num_scalar_prefetch=1,
            grid=(2,),
            in_specs=[
                pl.BlockSpec((rows, width), lambda m, s: (m, 0)),
                pl.BlockSpec((width, cols), lambda m, s: (0, s[0])),
                pl.BlockSpec((width, HEAD), lambda m, s: (0, s[0])),
                pl.BlockSpec((width, HEAD), lambda m, s: (0, s[0])),
                pl.BlockSpec((rows, HEAD), lambda m, s: (m, 0)),
            ] + [pl.BlockSpec(memory_space=pl.ANY)] * len(extra),
            out_specs=[
                pl.BlockSpec((rows, 2 * HEAD), lambda m, s: (m, 0)),
                pl.BlockSpec((rows, cols), lambda m, s: ((s[0] if own else 1 - s[0]) * 2 + m, 0)),
            ],
            scratch_shapes=[pltpu.VMEM((width, 2 * HEAD), BF)],
        ),
        out_shape=[
            jax.ShapeDtypeStruct((tokens, 2 * HEAD), BF),
            jax.ShapeDtypeStruct((2 * tokens, cols), BF),
        ],
        input_output_aliases={} if prev is None else {6: 1},
        compiler_params=params(),
        cost_estimate=cost(2 * tokens * width * (cols + 2 * HEAD), tokens * width * 2 + cols * width * 2),
        name="qkv_proj",
    )(core, x, w_q, w_k, w_v, tab, *extra)


def dctx_kernel(s_ref, own_ref, oth_ref, wo_ref, out_ref):
    def put(ref):
        step = 4 * HEAD
        for n in range(wo_ref.shape[0] // step):
            out_ref[:, n * step:(n + 1) * step] = dot_nt(ref[...], wo_ref[n * step:(n + 1) * step, :]).astype(BF)

    @pl.when(pl.program_id(0) < 2)
    def _():
        put(own_ref)

    @pl.when(pl.program_id(0) >= 2)
    def _():
        put(oth_ref)


def dctx_proj(core, own, oth, w_o):
    tokens, width = own.shape
    cols = w_o.shape[0] // 2
    rows = tokens // 2

    def place(m, s):
        far = m // 2
        return (s[0] + far - 2 * s[0] * far) * 2 + m % 2

    return pl.pallas_call(
        dctx_kernel,
        grid_spec=pltpu.PrefetchScalarGridSpec(
            num_scalar_prefetch=1,
            grid=(4,),
            in_specs=[
                pl.BlockSpec((rows, width), lambda m, s: (jnp.minimum(m, 1), 0)),
                pl.BlockSpec((rows, width), lambda m, s: (jnp.maximum(m - 2, 0), 0)),
                pl.BlockSpec((cols, width), lambda m, s: (s[0], 0)),
            ],
            out_specs=pl.BlockSpec((rows, cols), lambda m, s: (place(m, s), 0)),
        ),
        out_shape=jax.ShapeDtypeStruct((2 * tokens, cols), BF),
        compiler_params=params(),
        cost_estimate=cost(4 * tokens * width * cols, tokens * width * 4 + cols * width * 2),
        name="dctx_proj",
    )(core, own, oth, w_o)


def attn_kernel(
    first, core_ref, lo_ref, nb_ref, q_ref, do_ref, kdoc_ref, tab_own, tab_oth, kvp_own, kvp_oth, kvc_own, kvc_oth,
    x_own, x_oth, g_own, g_oth, before_up, before_here, act_ref, part_ref, up_ref, here_ref,
    kv_s, s_s, dp_s, m_s, l_s, d_s, qd_s, ahead_s, ctx_s, dq_s, q_s, do_s, qt_s, dot_s, tab_s, dk_s, dv_s,
    x_s, g_s, at_s, w_s, before_s, init_sem, row_sem, out_sem,
):

    def before_copies():
        return (
            pltpu.make_async_copy(before_up, before_s.at[pl.ds(0, 2 * HEAD), :], out_sem.at[3]),
            pltpu.make_async_copy(before_here, before_s.at[pl.ds(2 * HEAD, 2 * HEAD), :], out_sem.at[4]),
        )

    i = pl.program_id(0)
    tokens = kvc_own.shape[0]
    chip_len = 2 * tokens
    core = core_ref[0]
    per_half = tokens // BQ
    rows_here = span(i % per_half, BQ)

    def row_copies(x, g):
        return (
            pltpu.make_async_copy(x.at[rows_here, :], x_s, row_sem.at[0]),
            pltpu.make_async_copy(g.at[rows_here, :], g_s, row_sem.at[1]),
        )

    def init_copies():
        moves = []
        for base, place, ref in ((0, core, kvp_own), (0, 1 - core, kvp_oth), (2, core, kvc_own), (2, 1 - core, kvc_oth)):
            moves.append((ref, kv_s.at[span(base + place, tokens), :]))
        moves.append((tab_own, tab_s.at[span(core, tokens), :]))
        moves.append((tab_oth, tab_s.at[span(1 - core, tokens), :]))
        return [pltpu.make_async_copy(src, dst, init_sem.at[n]) for n, (src, dst) in enumerate(moves)]

    def arrive(first, last):
        @pl.when(i == 0)
        def _():
            for copy in init_copies()[first:last]:
                copy.wait()

    @pl.when(i == 0)
    def _():
        for copy in init_copies():
            copy.start()
        if not first:
            for copy in before_copies():
                copy.start()
        kv_s[2 * chip_len:, :] = jnp.zeros((BK, 2 * HEAD), BF)

        def clear(r):
            w_s[r, :] = jnp.zeros((16, w_s.shape[1]), F32)

        def clear_kv(r):
            dk_s[r, :] = jnp.zeros((16, dk_s.shape[1]), F32)
            dv_s[r, :] = jnp.zeros((16, dv_s.shape[1]), F32)

        def order(r):
            row = lax.broadcasted_iota(jnp.int32, (16, BK), 0)
            ahead_s[r, :] = lax.broadcasted_iota(jnp.int32, (16, BK), 1) - row - r.start

        by_rows(BQ, order)
        by_rows(w_s.shape[0], clear)
        by_rows(HEAD, clear_kv)

    @pl.when(i // per_half == core)
    def _():
        for copy in row_copies(x_own, g_own):
            copy.start()

    @pl.when(i // per_half != core)
    def _():
        for copy in row_copies(x_oth, g_oth):
            copy.start()

    def mixed(ref):
        parts = [ref[:, h * HEAD:(h + 1) * HEAD].reshape(BQ // MIX, 1, MIX, HEAD) for h in range(PAIR)]
        return jnp.concatenate(parts, axis=1).reshape(PAIR * BQ, HEAD)

    def apart(v, h):
        return v.reshape(BQ // MIX, PAIR, MIX, HEAD)[:, h].reshape(BQ, HEAD)

    q_mix, do_mix = mixed(q_ref), mixed(do_ref)
    q_s[...] = q_mix
    do_s[...] = do_mix
    qt_s[...] = q_mix.T
    dot_s[...] = do_mix.T
    qdoc = kdoc_ref[:, pl.ds(pl.multiple_of(chip_len + i * BQ, BQ), BQ)]
    qd_s[...] = jnp.broadcast_to(qdoc, (HEAD, BQ)).T
    m_s[...] = jnp.full(m_s.shape, NEG_BIG, F32)
    l_s[...] = jnp.zeros(l_s.shape, F32)
    d_s[...] = jnp.zeros(d_s.shape, F32)
    ctx_s[...] = jnp.zeros(ctx_s.shape, F32)
    dq_s[...] = jnp.zeros(dq_s.shape, F32)
    lo = lo_ref[i]
    n_blocks = nb_ref[i]
    lanes = BK // HEAD

    def fold(v, op):
        out = v[:, :HEAD]
        for n in range(1, lanes):
            out = op(out, v[:, n * HEAD:(n + 1) * HEAD])
        return out

    def spread(v):
        return jnp.concatenate([v] * lanes, axis=1)

    def offset(b):
        return pl.multiple_of(lo + b * BK, ALIGN)

    def scores(b, carry):
        off = offset(b)
        s = dot_nt(q_s[...], kv_s[pl.ds(off, BK), :HEAD])
        limit = chip_len + i * BQ - off
        key_doc = kdoc_ref[:, pl.ds(off, BK)]
        for c in range(BQ // MIX):
            here = slice(c * MIX, (c + 1) * MIX)
            keep = (ahead_s[here, :] <= limit) & (key_doc == spread(qd_s[here, :]))
            shift = jnp.where(keep, 0.0, NEG_BIG)
            for h in range(PAIR):
                rows = slice((c * PAIR + h) * MIX, (c * PAIR + h + 1) * MIX)
                sh = s[rows, :] * (SCALE * LOG2E) + shift
                s_s[b, rows, :] = sh
                m_s[rows, :] = jnp.maximum(m_s[rows, :], fold(sh, jnp.maximum))
        return carry

    arrive(0, 4)
    lax.fori_loop(0, n_blocks, scores, 0)
    m_s[...] = jnp.broadcast_to(jnp.max(m_s[...], axis=1, keepdims=True), m_s.shape)

    def weights(b, carry):
        dp = dot_nt(do_s[...], kv_s[pl.ds(offset(b), BK), HEAD:])
        e = jnp.exp2(s_s[b] - spread(m_s[...]))
        s_s[b] = e
        dp_s[b] = dp
        l_s[...] += fold(e, jnp.add)
        d_s[...] += fold(e * dp, jnp.add)
        return carry

    arrive(4, 6)
    lax.fori_loop(0, n_blocks, weights, 0)
    inv = 1.0 / jnp.sum(l_s[...], axis=1, keepdims=True)
    delta = jnp.sum(d_s[...], axis=1, keepdims=True) * inv
    l_s[...] = jnp.broadcast_to(inv, l_s.shape)
    d_s[...] = jnp.broadcast_to(delta, d_s.shape)

    def grads(b, carry):
        off = offset(b)
        p = s_s[b] * spread(l_s[...])
        pb = p.astype(BF)
        ds = (p * (dp_s[b] - spread(d_s[...])) * SCALE).astype(BF)
        ctx_s[...] += dot_nn(pb, kv_s[pl.ds(off, BK), HEAD:])
        dq_s[...] += dot_nn(ds, kv_s[pl.ds(off, BK), :HEAD])
        dv_s[:, pl.ds(off, BK)] += dot_nn(dot_s[...], pb)
        dk_s[:, pl.ds(off, BK)] += dot_nn(qt_s[...], ds)
        return carry

    lax.fori_loop(0, n_blocks, grads, 0)
    cos_t, sin_t = spread_table(tab_s[span(i, BQ), :])
    ctx_all, dq_all = ctx_s[...].astype(BF), dq_s[...].astype(BF).astype(F32)
    for h in range(PAIR):
        cols = slice(h * HEAD, (h + 1) * HEAD)
        ctx = apart(ctx_all, h)
        act_ref[0, :, cols] = ctx
        at_s[WIDE + h * HEAD:WIDE + (h + 1) * HEAD, :] = ctx.T
        dq = apart(dq_all, h)
        dq = (dq * cos_t - swap_halves(dq) * sin_t).astype(BF)
        act_ref[1, :, cols] = dq
        at_s[h * HEAD:(h + 1) * HEAD, :] = dq.T
    step = 4 * HEAD
    for copy in row_copies(x_own, g_own):
        copy.wait()

    def products(c, carry):
        cols = span(c, step)
        w_s[:WIDE, cols] += dot_nn(at_s[:WIDE, :], x_s[:, cols])
        w_s[WIDE:, cols] += dot_nn(at_s[WIDE:, :], g_s[:, cols])
        return carry

    lax.fori_loop(0, x_s.shape[1] // step, products, 0)

    @pl.when(i == pl.num_programs(0) - 1)
    def _():
        def narrow(r):
            x_s[r, :] = w_s[r, :].astype(BF)

        by_rows(w_s.shape[0], narrow)
        part_copy = pltpu.make_async_copy(x_s, part_ref, out_sem.at[0])
        part_copy.start()
        if not first:
            for copy in before_copies():
                copy.wait()

        def narrow_kv(r, carry):
            rows = span(r, 16)
            for n, acc in enumerate((dk_s, dv_s)):
                for side in range(2):
                    at = pl.ds(pl.multiple_of((n + 2 * side) * HEAD + r * 16, 16), 16)
                    total = acc[rows, side * chip_len:(side + 1) * chip_len]
                    if not first:
                        total = total + before_s[at, :].astype(F32)
                    g_s[at, :] = total.astype(BF)
            return carry

        lax.fori_loop(0, HEAD // 16, narrow_kv, 0)
        up_copy = pltpu.make_async_copy(g_s.at[pl.ds(0, 2 * HEAD), :], up_ref, out_sem.at[1])
        here_copy = pltpu.make_async_copy(g_s.at[pl.ds(2 * HEAD, 2 * HEAD), :], here_ref, out_sem.at[2])
        up_copy.start()
        here_copy.start()
        part_copy.wait()
        up_copy.wait()
        here_copy.wait()


def attention(chunk, core, lo, n_blocks, q, dctx, kdoc, tabs, kv_prev, kv_chip, xs, gs, before):
    first = before is None
    chip_len = q.shape[0]
    width = xs[0].shape[1]
    assert 2 * WIDE == BQ == 4 * HEAD and width == chip_len
    padded = 2 * chip_len + BK
    max_blocks = 2 * chip_len // BK
    rows = PAIR * BQ
    full = lambda shape: pl.BlockSpec(shape, lambda i, *s: (0,) * len(shape))
    pairs = chip_len * chip_len * PAIR
    return pl.pallas_call(
        functools.partial(attn_kernel, first),
        grid_spec=pltpu.PrefetchScalarGridSpec(
            num_scalar_prefetch=3,
            grid=(chip_len // BQ,),
            in_specs=[
                pl.BlockSpec((BQ, WIDE), lambda i, *s: (i, chunk)),
                pl.BlockSpec((BQ, WIDE), lambda i, *s: (i, chunk)),
                full((1, padded)),
            ] + [pl.BlockSpec(memory_space=pl.ANY)] * 12,
            out_specs=[
                pl.BlockSpec((2, BQ, WIDE), lambda i, *s: (0, i, 0)),
                pl.BlockSpec(memory_space=pl.ANY),
                pl.BlockSpec(memory_space=pl.ANY),
                pl.BlockSpec(memory_space=pl.ANY),
            ],
            scratch_shapes=[
                pltpu.VMEM((padded, 2 * HEAD), BF),
                pltpu.VMEM((max_blocks, rows, BK), F32),
                pltpu.VMEM((max_blocks, rows, BK), F32),
                pltpu.VMEM((rows, HEAD), F32),
                pltpu.VMEM((rows, HEAD), F32),
                pltpu.VMEM((rows, HEAD), F32),
                pltpu.VMEM((BQ, HEAD), jnp.int32),
                pltpu.VMEM((BQ, BK), jnp.int32),
                pltpu.VMEM((rows, HEAD), F32),
                pltpu.VMEM((rows, HEAD), F32),
                pltpu.VMEM((rows, HEAD), BF),
                pltpu.VMEM((rows, HEAD), BF),
                pltpu.VMEM((HEAD, rows), BF),
                pltpu.VMEM((HEAD, rows), BF),
                pltpu.VMEM((chip_len, HEAD), F32),
                pltpu.VMEM((HEAD, padded), F32),
                pltpu.VMEM((HEAD, padded), F32),
                pltpu.VMEM((BQ, width), BF),
                pltpu.VMEM((BQ, width), BF),
                pltpu.VMEM((2 * WIDE, BQ), BF),
                pltpu.VMEM((2 * WIDE, width), F32),
                pltpu.VMEM((4 * HEAD, chip_len), BF),
                pltpu.SemaphoreType.DMA((6,)),
                pltpu.SemaphoreType.DMA((2,)),
                pltpu.SemaphoreType.DMA((5,)),
            ],
        ),
        out_shape=[
            jax.ShapeDtypeStruct((2, chip_len, WIDE), BF),
            jax.ShapeDtypeStruct((2 * WIDE, width), BF),
            jax.ShapeDtypeStruct((2 * HEAD, chip_len), BF),
            jax.ShapeDtypeStruct((2 * HEAD, chip_len), BF),
        ],
        compiler_params=params(),
        cost_estimate=cost(pairs * HEAD * 2 * 8, 12 * 1024 * 1024, pairs),
        name="attention",
    )(core, lo, n_blocks, q, dctx, kdoc, *tabs, *kv_prev, *kv_chip, *xs, *gs, *(gs if first else before))


def kv_finish_kernel(s_ref, near_ref, far_ref, tab_own, tab_oth, out_ref, outt_ref, tab_s):
    tokens = tab_own.shape[0]
    step = out_ref.shape[0]

    @pl.when(pl.program_id(0) == 0)
    def _():
        tab_s[span(s_ref[0], tokens), :] = tab_own[...]
        tab_s[span(1 - s_ref[0], tokens), :] = tab_oth[...]

    total = near_ref[...].astype(F32) + far_ref[...].astype(F32)
    cos_t, sin_t = spread_table(tab_s[span(pl.program_id(0), step), :])
    dk = total[:HEAD].astype(BF).astype(F32).T
    dk = (dk * cos_t - swap_halves(dk) * sin_t).astype(BF)
    dvt = total[HEAD:].astype(BF)
    out_ref[:, :HEAD] = dk
    out_ref[:, HEAD:] = dvt.T
    outt_ref[:HEAD, :] = dk.T
    outt_ref[HEAD:, :] = dvt


def kv_finish(core, near, far, tab_own, tab_oth):
    tokens = tab_own.shape[0]
    chip_len = 2 * tokens
    step = 512
    return pl.pallas_call(
        kv_finish_kernel,
        grid_spec=pltpu.PrefetchScalarGridSpec(
            num_scalar_prefetch=1,
            grid=(chip_len // step,),
            in_specs=[
                pl.BlockSpec((2 * HEAD, step), lambda t, s: (0, t)),
                pl.BlockSpec((2 * HEAD, step), lambda t, s: (0, t)),
                pl.BlockSpec((tokens, HEAD), lambda t, s: (0, 0)),
                pl.BlockSpec((tokens, HEAD), lambda t, s: (0, 0)),
            ],
            out_specs=[
                pl.BlockSpec((step, 2 * HEAD), lambda t, s: (t, 0)),
                pl.BlockSpec((2 * HEAD, step), lambda t, s: (0, t)),
            ],
            scratch_shapes=[pltpu.VMEM((chip_len, HEAD), F32)],
        ),
        out_shape=[
            jax.ShapeDtypeStruct((chip_len, 2 * HEAD), BF),
            jax.ShapeDtypeStruct((2 * HEAD, chip_len), BF),
        ],
        compiler_params=params(),
        cost_estimate=cost(chip_len * HEAD * 64, chip_len * HEAD * 16),
        name="kv_finish",
    )(core, near, far, tab_own, tab_oth)


def kvgrad_kernel(s_ref, dkvt_ref, x_own, x_oth, out_ref):
    tokens = x_own.shape[0]
    own, oth = span(s_ref[0], tokens), span(1 - s_ref[0], tokens)
    out_ref[...] = (dot_nn(dkvt_ref[:, own], x_own[...]) + dot_nn(dkvt_ref[:, oth], x_oth[...])).astype(BF)


def kvgrad(core, dkvt, x_own, x_oth):
    tokens, width = x_own.shape
    step = 512
    piece = pl.BlockSpec((tokens, step), lambda n, s: (0, n))
    return pl.pallas_call(
        kvgrad_kernel,
        grid_spec=pltpu.PrefetchScalarGridSpec(
            num_scalar_prefetch=1,
            grid=(width // step,),
            in_specs=[pl.BlockSpec((2 * HEAD, 2 * tokens), lambda n, s: (0, 0)), piece, piece],
            out_specs=pl.BlockSpec((2 * HEAD, step), lambda n, s: (0, n)),
        ),
        out_shape=jax.ShapeDtypeStruct((2 * HEAD, width), BF),
        compiler_params=params(),
        cost_estimate=cost(4 * tokens * width * 2 * HEAD, 4 * tokens * width),
        name="kvgrad",
    )(core, dkvt, x_own, x_oth)


def kv_combine_kernel(s_ref, a_ref, b_ref, c_ref, d_ref, gk_ref, gv_ref):
    for place, u_ref, v_ref in ((s_ref[0], a_ref, b_ref), (1 - s_ref[0], c_ref, d_ref)):
        total = u_ref[...].astype(F32) + v_ref[...].astype(F32)
        where = span(place, HEAD)
        gk_ref[:, where] = total[:HEAD, :].T
        gv_ref[:, where] = total[HEAD:, :].T


def kv_combine(core, parts):
    rows, width = parts[0].shape
    step = 1024
    out = jax.ShapeDtypeStruct((width, rows), F32)
    return pl.pallas_call(
        kv_combine_kernel,
        grid_spec=pltpu.PrefetchScalarGridSpec(
            num_scalar_prefetch=1,
            grid=(width // step,),
            in_specs=[pl.BlockSpec((rows, step), lambda n, s: (0, n))] * 4,
            out_specs=[pl.BlockSpec((step, rows), lambda n, s: (n, 0))] * 2,
        ),
        out_shape=[out, out],
        compiler_params=params(),
        cost_estimate=cost(16 * width * rows * 16, 16 * width * rows),
        name="kv_combine",
    )(core, *parts)


def combine_kernel(s_ref, a_ref, b_ref, c_ref, d_ref, *rest):
    gq_ref, go_ref = rest[-2:]

    def put(u_ref, v_ref):
        def part(c, carry):
            cols = span(c, 256)
            gq_ref[cols, :] = (u_ref[0, :, cols].astype(F32) + v_ref[0, :, cols].astype(F32)).T
            go_ref[:, cols] = u_ref[1, :, cols].astype(F32) + v_ref[1, :, cols].astype(F32)
            return carry

        lax.fori_loop(0, u_ref.shape[2] // 256, part, 0)

    @pl.when(pl.program_id(0) == 0)
    def _():
        put(a_ref, b_ref)

    @pl.when(pl.program_id(0) == 1)
    def _():
        put(c_ref, d_ref)


def combine(core, chunk, n_chunks, parts, prev):
    width = parts[0].shape[2]
    step = 1024
    last = width // step - 1
    near = pl.BlockSpec((2, WIDE, step), lambda w, r, s: (0, 0, r + w * (last - r)))
    far = pl.BlockSpec((2, WIDE, step), lambda w, r, s: (0, 0, r * w))

    def place(w, s):
        return (s[0] + w - 2 * s[0] * w) * n_chunks + chunk

    shape = jax.ShapeDtypeStruct((width, 2 * n_chunks * WIDE), F32)
    shape_o = jax.ShapeDtypeStruct((2 * n_chunks * WIDE, width), F32)
    extra = [] if prev is None else list(prev)
    return pl.pallas_call(
        combine_kernel,
        grid_spec=pltpu.PrefetchScalarGridSpec(
            num_scalar_prefetch=1,
            grid=(2, width // step),
            in_specs=[near, near, far, far] + [pl.BlockSpec(memory_space=pl.ANY)] * len(extra),
            out_specs=[
                pl.BlockSpec((step, WIDE), lambda w, r, s: (r, place(w, s))),
                pl.BlockSpec((WIDE, step), lambda w, r, s: (place(w, s), r)),
            ],
        ),
        out_shape=[shape, shape_o],
        input_output_aliases={} if prev is None else {5: 0, 6: 1},
        compiler_params=params(),
        cost_estimate=cost(16 * width * WIDE * 64, 32 * width * WIDE),
        name="combine",
    )(core, *parts, *extra)


def fill_heads(core, own_refs, oth_refs, lhs):
    n = len(own_refs)
    for j in range(n):
        lhs[:, pl.ds(pl.multiple_of((core * n + j) * WIDE, WIDE), WIDE)] = own_refs[j][0]
        lhs[:, pl.ds(pl.multiple_of(((1 - core) * n + j) * WIDE, WIDE), WIDE)] = oth_refs[j][0]


def attn_out_kernel(n, s_ref, *refs):
    own_refs, oth_refs = refs[:n], refs[n:2 * n]
    wo_ref, out_ref, lhs = refs[2 * n:]

    @pl.when(pl.program_id(0) == 0)
    def _():
        fill_heads(s_ref[0], own_refs, oth_refs, lhs)

    out_ref[...] = dot_nn(lhs[...], wo_ref[...]).astype(BF)


def attn_out(core, own, oth, w_o):
    n = len(own)
    tokens = own[0].shape[1] // 2
    heads, width = w_o.shape
    step = 512
    return pl.pallas_call(
        functools.partial(attn_out_kernel, n),
        grid_spec=pltpu.PrefetchScalarGridSpec(
            num_scalar_prefetch=1,
            grid=(width // step,),
            in_specs=[pl.BlockSpec((1, tokens, WIDE), lambda k, s: (0, s[0], 0))] * (2 * n)
            + [pl.BlockSpec((heads, step), lambda k, s: (0, k))],
            out_specs=pl.BlockSpec((tokens, step), lambda k, s: (0, k)),
            scratch_shapes=[pltpu.VMEM((tokens, heads), BF)],
        ),
        out_shape=jax.ShapeDtypeStruct((tokens, width), BF),
        compiler_params=params(),
        cost_estimate=cost(2 * tokens * heads * width, 2 * heads * width + 4 * tokens * width),
        name="attn_out",
    )(core, *own, *oth, w_o)


def hidden_kernel(n, s_ref, *refs):
    own_refs, oth_refs = refs[:n], refs[n:2 * n]
    kv_own, kv_oth, wq_ref, wk_ref, wv_ref, out_ref, lhs, klhs, vlhs = refs[2 * n:]
    core = s_ref[0]

    @pl.when(pl.program_id(0) == 0)
    def _():
        fill_heads(core, own_refs, oth_refs, lhs)
        for place, ref in ((core, kv_own), (1 - core, kv_oth)):
            where = pl.ds(pl.multiple_of(place * HEAD, HEAD), HEAD)
            klhs[:, where] = ref[:, :HEAD]
            vlhs[:, where] = ref[:, HEAD:]

    out_ref[...] = (
        dot_nt(lhs[...], wq_ref[...]) + dot_nt(klhs[...], wk_ref[...]) + dot_nt(vlhs[...], wv_ref[...])
    ).astype(BF)


def grad_hidden(core, own, oth, kv_own, kv_oth, w_q, w_k, w_v):
    n = len(own)
    tokens = own[0].shape[1] // 2
    width, heads = w_q.shape
    kv_cols = w_k.shape[1]
    step = 512
    return pl.pallas_call(
        functools.partial(hidden_kernel, n),
        grid_spec=pltpu.PrefetchScalarGridSpec(
            num_scalar_prefetch=1,
            grid=(width // step,),
            in_specs=[pl.BlockSpec((1, tokens, WIDE), lambda k, s: (1, s[0], 0))] * (2 * n)
            + [pl.BlockSpec((tokens, 2 * HEAD), lambda k, s: (s[0], 0))] * 2
            + [
                pl.BlockSpec((step, heads), lambda k, s: (k, 0)),
                pl.BlockSpec((step, kv_cols), lambda k, s: (k, 0)),
                pl.BlockSpec((step, kv_cols), lambda k, s: (k, 0)),
            ],
            out_specs=pl.BlockSpec((tokens, step), lambda k, s: (0, k)),
            scratch_shapes=[
                pltpu.VMEM((tokens, heads), BF),
                pltpu.VMEM((tokens, kv_cols), BF),
                pltpu.VMEM((tokens, kv_cols), BF),
            ],
        ),
        out_shape=jax.ShapeDtypeStruct((tokens, width), BF),
        compiler_params=params(),
        cost_estimate=cost(2 * tokens * (heads + 2 * kv_cols) * width, 2 * heads * width + 4 * tokens * width),
        name="grad_hidden",
    )(core, *own, *oth, kv_own, kv_oth, w_q, w_k, w_v)


def solution(mesh):
    n_dev = mesh.shape["sp"]
    n_chunks = 4
    near_perm = [(d, d ^ 1) for d in range(n_dev)]
    far_perm = [(d, d ^ 2) for d in range(n_dev)]
    down_perm = [(0, 2), (1, 3)]
    up_perm = [(2, 0), (3, 1)]

    def near(v):
        return lax.ppermute(v, "sp", near_perm)

    def far(v):
        return lax.ppermute(v, "sp", far_perm)

    def device_step(hidden, grad_out, positions, doc_ids, w_q, w_k, w_v, w_o):
        tokens = hidden.shape[0]
        chip_len = 2 * tokens
        assert n_chunks == w_q.shape[1] // (2 * WIDE)
        place = lax.axis_index("sp")
        core_id, chip_id = place & 1, place >> 1
        core = core_id.astype(jnp.int32)[None]

        doc_oth = near(doc_ids)
        doc_far = far(doc_ids)
        doc_far_oth = lax.ppermute(doc_ids, "sp", [(d, d ^ 3) for d in range(n_dev)])
        x_oth = near(hidden)
        g_oth = near(grad_out)
        tab_own = rope_table(positions)
        tab_oth = near(tab_own)
        kv_own, q = qkv_proj(True, core, hidden, w_q, w_k, w_v, tab_own, None)
        kvp_own = lax.ppermute(kv_own, "sp", down_perm)

        def in_order(own, oth):
            return jnp.where(core_id == 0, jnp.concatenate([own, oth]), jnp.concatenate([oth, own]))

        doc_chip, doc_far = in_order(doc_ids, doc_oth), in_order(doc_far, doc_far_oth)
        kv_oth, q = qkv_proj(False, core, x_oth, w_q, w_k, w_v, tab_oth, q)
        kvp_oth = lax.ppermute(kv_oth, "sp", down_perm)
        dctx = dctx_proj(core, grad_out, g_oth, w_o)

        heads_doc = doc_chip[::BQ]
        lo = jnp.sum(doc_chip[None, :] < heads_doc[:, None], axis=1, dtype=jnp.int32)
        lo_far = jnp.sum(doc_far[None, :] < heads_doc[:, None], axis=1, dtype=jnp.int32)
        lo = lo + jnp.where(chip_id == 0, chip_len, lo_far)
        lo = (lo >> (ALIGN.bit_length() - 1)) << (ALIGN.bit_length() - 1)
        end = chip_len + BQ * (1 + jnp.arange(chip_len // BQ, dtype=jnp.int32))
        n_blocks = (end - lo + BK - 1) >> (BK.bit_length() - 1)
        kdoc = jnp.concatenate([doc_far, doc_chip, jnp.zeros((BK,), jnp.int32)])[None, :]

        acts, acts_oth, dkv_sum, sums = [], [], None, None
        for j in range(n_chunks):
            act, part, dkv_up, dkv_here = attention(
                j, core, lo, n_blocks, q, dctx, kdoc, (tab_own, tab_oth), (kvp_own, kvp_oth), (kv_own, kv_oth),
                (hidden, x_oth), (grad_out, g_oth), dkv_sum,
            )
            part = part.reshape(2, WIDE, -1)
            acts.append(act)
            dkv_sum = (dkv_up, dkv_here)
            if j == n_chunks - 1:
                dkv_far = lax.ppermute(dkv_up, "sp", up_perm)
            acts_oth.append(near(act))
            part_far = far(part)
            part_near = near(part)
            part_far_near = near(part_far)
            sums = combine(core, j, n_chunks, (part, part_far, part_near, part_far_near), sums)
        grad_wq, grad_wo = sums

        dkv, dkvt = kv_finish(core, dkv_here, dkv_far, tab_own, tab_oth)
        dkv_oth = near(dkv)
        kv_part = kvgrad(core, dkvt, hidden, x_oth)
        kv_part_far = far(kv_part)
        kv_part_near = near(kv_part)
        kv_part_far_near = near(kv_part_far)
        grad_wk, grad_wv = kv_combine(core, (kv_part, kv_part_far, kv_part_near, kv_part_far_near))
        out = attn_out(core, acts, acts_oth, w_o)
        g_hidden = grad_hidden(core, acts, acts_oth, dkv, dkv_oth, w_q, w_k, w_v)
        return out, g_hidden, grad_wq, grad_wk, grad_wv, grad_wo

    tok_spec = P(("dp", "sp"), None)
    vec_spec = P(("dp", "sp"))
    rep_spec = P(None, None)
    part_spec = P("dp", None)


    return jax.shard_map(
        device_step,
        mesh=mesh,
        in_specs=(tok_spec, tok_spec, vec_spec, vec_spec, rep_spec, rep_spec, rep_spec, rep_spec),
        out_specs=(tok_spec, tok_spec, part_spec, part_spec, part_spec, part_spec),
        check_vma=False,
    )
```

```python
import functools

import jax
import jax.numpy as jnp
from jax import lax
from jax.experimental import pallas as pl
from jax.experimental.pallas import tpu as pltpu
from jax.sharding import PartitionSpec as P

HEAD = 128
ROPE_THETA = 500000.0
ROPE_FACTOR = 8.0
ROPE_LOW = 1.0
ROPE_HIGH = 4.0
ROPE_OLD_CTX = 8192.0
NEG_BIG = float("-inf")
SCALE = HEAD ** -0.5
LOG2E = 1.4426950408889634

PAIR = 2
WIDE = PAIR * HEAD
BQ = 512
BK = 512
MIX = 16
ALIGN = 128
BF = jnp.bfloat16
F32 = jnp.float32


def rope_freqs():
    half_idx = jnp.arange(HEAD // 2, dtype=F32)
    inv_freq = jnp.power(ROPE_THETA, -2.0 * half_idx / HEAD)
    wavelen = 2.0 * jnp.pi / inv_freq
    smooth = (ROPE_OLD_CTX / wavelen - ROPE_LOW) / (ROPE_HIGH - ROPE_LOW)
    mixed_freq = (1.0 - smooth) * inv_freq / ROPE_FACTOR + smooth * inv_freq
    scaled = jnp.where(wavelen > ROPE_OLD_CTX / ROPE_LOW, inv_freq / ROPE_FACTOR, mixed_freq)
    return jnp.where(wavelen < ROPE_OLD_CTX / ROPE_HIGH, inv_freq, scaled)


def rope_table(pos_vec):
    angles = pos_vec.astype(F32)[:, None] * rope_freqs()[None, :]
    return jnp.concatenate([jnp.cos(angles), jnp.sin(angles)], axis=-1)


def dot_nn(a, b):
    return lax.dot_general(a, b, (((1,), (0,)), ((), ())), preferred_element_type=F32)


def dot_nt(a, b):
    return lax.dot_general(a, b, (((1,), (1,)), ((), ())), preferred_element_type=F32)


def swap_halves(v):
    return pltpu.roll(v, HEAD // 2, 1)


def spread_table(tab):
    low = lax.broadcasted_iota(jnp.int32, tab.shape, 1) < HEAD // 2
    other = swap_halves(tab)
    return jnp.where(low, tab, other), jnp.where(low, -other, tab)


def cost(flops, nbytes, trans=0):
    return pl.CostEstimate(flops=int(flops), bytes_accessed=int(nbytes), transcendentals=int(trans))


def params(**kw):
    return pltpu.CompilerParams(vmem_limit_bytes=67_000_000, **kw)


def by_rows(rows, body, size=16):
    def step(r, carry):
        body(span(r, size))
        return carry

    lax.fori_loop(0, rows // size, step, 0)


def span(index, size):
    return pl.ds(pl.multiple_of(index * size, size), size)


def qkv_kernel(s_ref, x_ref, wq_ref, wk_ref, wv_ref, tab_ref, *rest):
    kv_ref, q_ref, w_s = rest[-3:]

    @pl.when(pl.program_id(0) == 0)
    def _():
        w_s[:, :HEAD] = wk_ref[...]
        w_s[:, HEAD:] = wv_ref[...]

    x = x_ref[...]
    cos_t, sin_t = spread_table(tab_ref[...])
    kv = dot_nn(x, w_s[...])
    k = kv[:, :HEAD]
    kv_ref[:, :HEAD] = (k * cos_t + swap_halves(k) * sin_t).astype(BF)
    kv_ref[:, HEAD:] = kv[:, HEAD:].astype(BF)
    step = 4 * HEAD
    for n in range(wq_ref.shape[1] // step):
        q = dot_nn(x, wq_ref[:, n * step:(n + 1) * step])
        for h in range(step // HEAD):
            part = q[:, h * HEAD:(h + 1) * HEAD]
            j, at = divmod(n * step + h * HEAD, WIDE)
            q_ref[j, :, at:at + HEAD] = (part * cos_t + swap_halves(part) * sin_t).astype(BF)


def qkv_proj(own, core, x, w_q, w_k, w_v, tab, prev):
    tokens, width = x.shape
    cols = w_q.shape[1] // 2
    rows = tokens // 2
    extra = [] if prev is None else [prev]
    return pl.pallas_call(
        qkv_kernel,
        grid_spec=pltpu.PrefetchScalarGridSpec(
            num_scalar_prefetch=1,
            grid=(2,),
            in_specs=[
                pl.BlockSpec((rows, width), lambda m, s: (m, 0)),
                pl.BlockSpec((width, cols), lambda m, s: (0, s[0])),
                pl.BlockSpec((width, HEAD), lambda m, s: (0, s[0])),
                pl.BlockSpec((width, HEAD), lambda m, s: (0, s[0])),
                pl.BlockSpec((rows, HEAD), lambda m, s: (m, 0)),
            ] + [pl.BlockSpec(memory_space=pl.ANY)] * len(extra),
            out_specs=[
                pl.BlockSpec((rows, 2 * HEAD), lambda m, s: (m, 0)),
                pl.BlockSpec((cols // WIDE, rows, WIDE), lambda m, s: (0, (s[0] if own else 1 - s[0]) * 2 + m, 0)),
            ],
            scratch_shapes=[pltpu.VMEM((width, 2 * HEAD), BF)],
        ),
        out_shape=[
            jax.ShapeDtypeStruct((tokens, 2 * HEAD), BF),
            jax.ShapeDtypeStruct((cols // WIDE, 2 * tokens, WIDE), BF),
        ],
        input_output_aliases={} if prev is None else {6: 1},
        compiler_params=params(),
        cost_estimate=cost(2 * tokens * width * (cols + 2 * HEAD), tokens * width * 2 + cols * width * 2),
        name="qkv_proj",
    )(core, x, w_q, w_k, w_v, tab, *extra)


def dctx_kernel(s_ref, own_ref, oth_ref, wo_ref, out_ref):
    def put(ref):
        step = 4 * HEAD
        for n in range(wo_ref.shape[0] // step):
            part = dot_nt(ref[...], wo_ref[n * step:(n + 1) * step, :]).astype(BF)
            for j in range(step // WIDE):
                out_ref[n * (step // WIDE) + j] = part[:, j * WIDE:(j + 1) * WIDE]

    @pl.when(pl.program_id(0) < 2)
    def _():
        put(own_ref)

    @pl.when(pl.program_id(0) >= 2)
    def _():
        put(oth_ref)


def dctx_proj(core, own, oth, w_o):
    tokens, width = own.shape
    cols = w_o.shape[0] // 2
    rows = tokens // 2

    def place(m, s):
        far = m // 2
        return (s[0] + far - 2 * s[0] * far) * 2 + m % 2

    return pl.pallas_call(
        dctx_kernel,
        grid_spec=pltpu.PrefetchScalarGridSpec(
            num_scalar_prefetch=1,
            grid=(4,),
            in_specs=[
                pl.BlockSpec((rows, width), lambda m, s: (jnp.minimum(m, 1), 0)),
                pl.BlockSpec((rows, width), lambda m, s: (jnp.maximum(m - 2, 0), 0)),
                pl.BlockSpec((cols, width), lambda m, s: (s[0], 0)),
            ],
            out_specs=pl.BlockSpec((cols // WIDE, rows, WIDE), lambda m, s: (0, place(m, s), 0)),
        ),
        out_shape=jax.ShapeDtypeStruct((cols // WIDE, 2 * tokens, WIDE), BF),
        compiler_params=params(),
        cost_estimate=cost(4 * tokens * width * cols, tokens * width * 4 + cols * width * 2),
        name="dctx_proj",
    )(core, own, oth, w_o)


def attn_kernel(
    first, core_ref, lo_ref, nb_ref, q_ref, do_ref, kdoc_ref, tab_own, tab_oth, kvp_own, kvp_oth, kvc_own, kvc_oth,
    x_own, x_oth, g_own, g_oth, before_up, before_here, act_ref, part_ref, up_ref, here_ref,
    kv_s, s_s, dp_s, m_s, l_s, d_s, qd_s, ahead_s, ctx_s, dq_s, q_s, do_s, qt_s, dot_s, tab_s, dk_s, dv_s,
    x_s, g_s, at_s, w_s, before_s, init_sem, row_sem, out_sem, part_sem,
):

    def before_copies():
        return (
            pltpu.make_async_copy(before_up, before_s.at[pl.ds(0, 2 * HEAD), :], out_sem.at[2]),
            pltpu.make_async_copy(before_here, before_s.at[pl.ds(2 * HEAD, 2 * HEAD), :], out_sem.at[3]),
        )

    i = pl.program_id(0)
    tokens = kvc_own.shape[0]
    chip_len = 2 * tokens
    core = core_ref[0]
    per_half = tokens // BQ
    rows_here = span(i % per_half, BQ)

    def row_copies(x, g):
        return (
            pltpu.make_async_copy(x.at[rows_here, :], x_s, row_sem.at[0]),
            pltpu.make_async_copy(g.at[rows_here, :], g_s, row_sem.at[1]),
        )

    def init_copies():
        moves = []
        for base, place, ref in ((0, core, kvp_own), (0, 1 - core, kvp_oth), (2, core, kvc_own), (2, 1 - core, kvc_oth)):
            moves.append((ref, kv_s.at[span(base + place, tokens), :]))
        moves.append((tab_own, tab_s.at[span(core, tokens), :]))
        moves.append((tab_oth, tab_s.at[span(1 - core, tokens), :]))
        return [pltpu.make_async_copy(src, dst, init_sem.at[n]) for n, (src, dst) in enumerate(moves)]

    def arrive(first, last):
        @pl.when(i == 0)
        def _():
            for copy in init_copies()[first:last]:
                copy.wait()

    @pl.when(i == 0)
    def _():
        for copy in init_copies():
            copy.start()
        if not first:
            for copy in before_copies():
                copy.start()
        kv_s[2 * chip_len:, :] = jnp.zeros((BK, 2 * HEAD), BF)

        def clear(r):
            w_s[r, :] = jnp.zeros((16, w_s.shape[1]), F32)

        def clear_kv(r):
            dk_s[r, :] = jnp.zeros((16, dk_s.shape[1]), F32)
            dv_s[r, :] = jnp.zeros((16, dv_s.shape[1]), F32)

        def order(r):
            row = lax.broadcasted_iota(jnp.int32, (16, BK), 0)
            ahead_s[r, :] = lax.broadcasted_iota(jnp.int32, (16, BK), 1) - row - r.start

        by_rows(BQ, order)
        by_rows(w_s.shape[0], clear)
        by_rows(HEAD, clear_kv)

    @pl.when(i // per_half == core)
    def _():
        for copy in row_copies(x_own, g_own):
            copy.start()

    @pl.when(i // per_half != core)
    def _():
        for copy in row_copies(x_oth, g_oth):
            copy.start()

    def mixed(ref):
        parts = [ref[0, :, h * HEAD:(h + 1) * HEAD].reshape(BQ // MIX, 1, MIX, HEAD) for h in range(PAIR)]
        return jnp.concatenate(parts, axis=1).reshape(PAIR * BQ, HEAD)

    def apart(v, h):
        return v.reshape(BQ // MIX, PAIR, MIX, HEAD)[:, h].reshape(BQ, HEAD)

    q_mix, do_mix = mixed(q_ref), mixed(do_ref)
    q_s[...] = q_mix
    do_s[...] = do_mix
    qt_s[...] = q_mix.T
    dot_s[...] = do_mix.T
    qdoc = kdoc_ref[:, pl.ds(pl.multiple_of(chip_len + i * BQ, BQ), BQ)]
    qd_s[...] = jnp.broadcast_to(qdoc, (HEAD, BQ)).T
    m_s[...] = jnp.full(m_s.shape, NEG_BIG, F32)
    l_s[...] = jnp.zeros(l_s.shape, F32)
    d_s[...] = jnp.zeros(d_s.shape, F32)
    ctx_s[...] = jnp.zeros(ctx_s.shape, F32)
    dq_s[...] = jnp.zeros(dq_s.shape, F32)
    lo = lo_ref[i]
    n_blocks = nb_ref[i]
    lanes = BK // HEAD

    def fold(v, op):
        out = v[:, :HEAD]
        for n in range(1, lanes):
            out = op(out, v[:, n * HEAD:(n + 1) * HEAD])
        return out

    def spread(v):
        return jnp.concatenate([v] * lanes, axis=1)

    def offset(b):
        return pl.multiple_of(lo + b * BK, ALIGN)

    def scores(b, carry):
        off = offset(b)
        s = dot_nt(q_s[...], kv_s[pl.ds(off, BK), :HEAD])
        limit = chip_len + i * BQ - off
        key_doc = kdoc_ref[:, pl.ds(off, BK)]
        for c in range(BQ // MIX):
            here = slice(c * MIX, (c + 1) * MIX)
            keep = (ahead_s[here, :] <= limit) & (key_doc == spread(qd_s[here, :]))
            shift = jnp.where(keep, 0.0, NEG_BIG)
            for h in range(PAIR):
                rows = slice((c * PAIR + h) * MIX, (c * PAIR + h + 1) * MIX)
                sh = s[rows, :] * (SCALE * LOG2E) + shift
                s_s[b, rows, :] = sh
                m_s[rows, :] = jnp.maximum(m_s[rows, :], fold(sh, jnp.maximum))
        return carry

    arrive(0, 4)
    lax.fori_loop(0, n_blocks, scores, 0)
    m_s[...] = jnp.broadcast_to(jnp.max(m_s[...], axis=1, keepdims=True), m_s.shape)

    def weights(b, carry):
        dp = dot_nt(do_s[...], kv_s[pl.ds(offset(b), BK), HEAD:])
        e = jnp.exp2(s_s[b] - spread(m_s[...]))
        s_s[b] = e
        dp_s[b] = dp
        l_s[...] += fold(e, jnp.add)
        d_s[...] += fold(e * dp, jnp.add)
        return carry

    arrive(4, 6)
    lax.fori_loop(0, n_blocks, weights, 0)
    inv = 1.0 / jnp.sum(l_s[...], axis=1, keepdims=True)
    delta = jnp.sum(d_s[...], axis=1, keepdims=True) * inv
    l_s[...] = jnp.broadcast_to(inv, l_s.shape)
    d_s[...] = jnp.broadcast_to(delta, d_s.shape)

    def grads(b, carry):
        off = offset(b)
        p = s_s[b] * spread(l_s[...])
        pb = p.astype(BF)
        ds = (p * (dp_s[b] - spread(d_s[...])) * SCALE).astype(BF)
        ctx_s[...] += dot_nn(pb, kv_s[pl.ds(off, BK), HEAD:])
        dq_s[...] += dot_nn(ds, kv_s[pl.ds(off, BK), :HEAD])
        dv_s[:, pl.ds(off, BK)] += dot_nn(dot_s[...], pb)
        dk_s[:, pl.ds(off, BK)] += dot_nn(qt_s[...], ds)
        return carry

    lax.fori_loop(0, n_blocks, grads, 0)
    last = pl.num_programs(0) - 1

    def out_copies():
        return (
            pltpu.make_async_copy(before_s.at[pl.ds(0, 2 * HEAD), :], up_ref, out_sem.at[0]),
            pltpu.make_async_copy(before_s.at[pl.ds(2 * HEAD, 2 * HEAD), :], here_ref, out_sem.at[1]),
        )

    @pl.when(i == last)
    def _():
        if not first:
            for copy in before_copies():
                copy.wait()

        def narrow_kv(r, carry):
            rows = span(r, 16)
            for n, acc in enumerate((dk_s, dv_s)):
                for side in range(2):
                    at = pl.ds(pl.multiple_of((n + 2 * side) * HEAD + r * 16, 16), 16)
                    total = acc[rows, side * chip_len:(side + 1) * chip_len]
                    if not first:
                        total = total + before_s[at, :].astype(F32)
                    before_s[at, :] = total.astype(BF)
            return carry

        lax.fori_loop(0, HEAD // 16, narrow_kv, 0)
        for copy in out_copies():
            copy.start()

    cos_t, sin_t = spread_table(tab_s[span(i, BQ), :])
    ctx_all, dq_all = ctx_s[...].astype(BF), dq_s[...].astype(BF).astype(F32)
    for h in range(PAIR):
        cols = slice(h * HEAD, (h + 1) * HEAD)
        ctx = apart(ctx_all, h)
        act_ref[0, :, cols] = ctx
        at_s[WIDE + h * HEAD:WIDE + (h + 1) * HEAD, :] = ctx.T
        dq = apart(dq_all, h)
        dq = (dq * cos_t - swap_halves(dq) * sin_t).astype(BF)
        act_ref[1, :, cols] = dq
        at_s[h * HEAD:(h + 1) * HEAD, :] = dq.T
    step = 4 * HEAD
    for copy in row_copies(x_own, g_own):
        copy.wait()

    def product(c):
        cols = span(c, step)
        for lhs, rows_ref in ((slice(0, WIDE), x_s), (slice(WIDE, 2 * WIDE), g_s)):
            w_s[lhs, cols] += dot_nn(at_s[lhs, :], rows_ref[:, cols])
        return cols

    def products(c, carry):
        product(c)
        return carry

    def part_copy(c):
        cols = span(c, step)
        return pltpu.make_async_copy(x_s.at[:, cols], part_ref.at[:, cols], part_sem.at[c])

    def last_products(c, carry):
        cols = product(c)
        x_s[:, cols] = w_s[:, cols].astype(BF)
        part_copy(c).start()
        return carry

    n_products = x_s.shape[1] // step

    @pl.when(i < last)
    def _():
        lax.fori_loop(0, n_products, products, 0)

    @pl.when(i == last)
    def _():
        lax.fori_loop(0, n_products, last_products, 0)
        for c in range(n_products):
            part_copy(c).wait()
        for copy in out_copies():
            copy.wait()


def attention(chunk, core, lo, n_blocks, q, dctx, kdoc, tabs, kv_prev, kv_chip, xs, gs, before):
    first = before is None
    chip_len = q.shape[1]
    width = xs[0].shape[1]
    assert 2 * WIDE == BQ == 4 * HEAD and width == chip_len
    padded = 2 * chip_len + BK
    max_blocks = 2 * chip_len // BK
    rows = PAIR * BQ
    full = lambda shape: pl.BlockSpec(shape, lambda i, *s: (0,) * len(shape))
    pairs = chip_len * chip_len * PAIR
    return pl.pallas_call(
        functools.partial(attn_kernel, first),
        grid_spec=pltpu.PrefetchScalarGridSpec(
            num_scalar_prefetch=3,
            grid=(chip_len // BQ,),
            in_specs=[
                pl.BlockSpec((1, BQ, WIDE), lambda i, *s: (chunk, i, 0)),
                pl.BlockSpec((1, BQ, WIDE), lambda i, *s: (chunk, i, 0)),
                full((1, padded)),
            ] + [pl.BlockSpec(memory_space=pl.ANY)] * 12,
            out_specs=[
                pl.BlockSpec((2, BQ, WIDE), lambda i, *s: (0, i, 0)),
                pl.BlockSpec(memory_space=pl.ANY),
                pl.BlockSpec(memory_space=pl.ANY),
                pl.BlockSpec(memory_space=pl.ANY),
            ],
            scratch_shapes=[
                pltpu.VMEM((padded, 2 * HEAD), BF),
                pltpu.VMEM((max_blocks, rows, BK), F32),
                pltpu.VMEM((max_blocks, rows, BK), F32),
                pltpu.VMEM((rows, HEAD), F32),
                pltpu.VMEM((rows, HEAD), F32),
                pltpu.VMEM((rows, HEAD), F32),
                pltpu.VMEM((BQ, HEAD), jnp.int32),
                pltpu.VMEM((BQ, BK), jnp.int32),
                pltpu.VMEM((rows, HEAD), F32),
                pltpu.VMEM((rows, HEAD), F32),
                pltpu.VMEM((rows, HEAD), BF),
                pltpu.VMEM((rows, HEAD), BF),
                pltpu.VMEM((HEAD, rows), BF),
                pltpu.VMEM((HEAD, rows), BF),
                pltpu.VMEM((chip_len, HEAD), F32),
                pltpu.VMEM((HEAD, padded), F32),
                pltpu.VMEM((HEAD, padded), F32),
                pltpu.VMEM((BQ, width), BF),
                pltpu.VMEM((BQ, width), BF),
                pltpu.VMEM((2 * WIDE, BQ), BF),
                pltpu.VMEM((2 * WIDE, width), F32),
                pltpu.VMEM((4 * HEAD, chip_len), BF),
                pltpu.SemaphoreType.DMA((6,)),
                pltpu.SemaphoreType.DMA((2,)),
                pltpu.SemaphoreType.DMA((4,)),
                pltpu.SemaphoreType.DMA((width // (4 * HEAD),)),
            ],
        ),
        out_shape=[
            jax.ShapeDtypeStruct((2, chip_len, WIDE), BF),
            jax.ShapeDtypeStruct((2 * WIDE, width), BF),
            jax.ShapeDtypeStruct((2 * HEAD, chip_len), BF),
            jax.ShapeDtypeStruct((2 * HEAD, chip_len), BF),
        ],
        compiler_params=params(),
        cost_estimate=cost(pairs * HEAD * 2 * 8, 12 * 1024 * 1024, pairs),
        name="attention",
    )(core, lo, n_blocks, q, dctx, kdoc, *tabs, *kv_prev, *kv_chip, *xs, *gs, *(gs if first else before))


def kv_finish_kernel(s_ref, near_ref, far_ref, tab_own, tab_oth, out_ref, outt_ref, tab_s):
    tokens = tab_own.shape[0]
    step = out_ref.shape[0]

    @pl.when(pl.program_id(0) == 0)
    def _():
        tab_s[span(s_ref[0], tokens), :] = tab_own[...]
        tab_s[span(1 - s_ref[0], tokens), :] = tab_oth[...]

    total = near_ref[...].astype(F32) + far_ref[...].astype(F32)
    cos_t, sin_t = spread_table(tab_s[span(pl.program_id(0), step), :])
    dk = total[:HEAD].astype(BF).astype(F32).T
    dk = (dk * cos_t - swap_halves(dk) * sin_t).astype(BF)
    dvt = total[HEAD:].astype(BF)
    out_ref[:, :HEAD] = dk
    out_ref[:, HEAD:] = dvt.T
    outt_ref[:HEAD, :] = dk.T
    outt_ref[HEAD:, :] = dvt


def kv_finish(core, near, far, tab_own, tab_oth):
    tokens = tab_own.shape[0]
    chip_len = 2 * tokens
    step = 512
    return pl.pallas_call(
        kv_finish_kernel,
        grid_spec=pltpu.PrefetchScalarGridSpec(
            num_scalar_prefetch=1,
            grid=(chip_len // step,),
            in_specs=[
                pl.BlockSpec((2 * HEAD, step), lambda t, s: (0, t)),
                pl.BlockSpec((2 * HEAD, step), lambda t, s: (0, t)),
                pl.BlockSpec((tokens, HEAD), lambda t, s: (0, 0)),
                pl.BlockSpec((tokens, HEAD), lambda t, s: (0, 0)),
            ],
            out_specs=[
                pl.BlockSpec((step, 2 * HEAD), lambda t, s: (t, 0)),
                pl.BlockSpec((2 * HEAD, step), lambda t, s: (0, t)),
            ],
            scratch_shapes=[pltpu.VMEM((chip_len, HEAD), F32)],
        ),
        out_shape=[
            jax.ShapeDtypeStruct((chip_len, 2 * HEAD), BF),
            jax.ShapeDtypeStruct((2 * HEAD, chip_len), BF),
        ],
        compiler_params=params(),
        cost_estimate=cost(chip_len * HEAD * 64, chip_len * HEAD * 16),
        name="kv_finish",
    )(core, near, far, tab_own, tab_oth)


def kvgrad_kernel(s_ref, dkvt_ref, x_own, x_oth, out_ref):
    tokens = x_own.shape[0]
    own, oth = span(s_ref[0], tokens), span(1 - s_ref[0], tokens)
    out_ref[...] = (dot_nn(dkvt_ref[:, own], x_own[...]) + dot_nn(dkvt_ref[:, oth], x_oth[...])).astype(BF)


def kvgrad(core, dkvt, x_own, x_oth):
    tokens, width = x_own.shape
    step = 512
    piece = pl.BlockSpec((tokens, step), lambda n, s: (0, n))
    return pl.pallas_call(
        kvgrad_kernel,
        grid_spec=pltpu.PrefetchScalarGridSpec(
            num_scalar_prefetch=1,
            grid=(width // step,),
            in_specs=[pl.BlockSpec((2 * HEAD, 2 * tokens), lambda n, s: (0, 0)), piece, piece],
            out_specs=pl.BlockSpec((2 * HEAD, step), lambda n, s: (0, n)),
        ),
        out_shape=jax.ShapeDtypeStruct((2 * HEAD, width), BF),
        compiler_params=params(),
        cost_estimate=cost(4 * tokens * width * 2 * HEAD, 4 * tokens * width),
        name="kvgrad",
    )(core, dkvt, x_own, x_oth)


def kv_combine_kernel(s_ref, a_ref, b_ref, c_ref, d_ref, gk_ref, gv_ref):
    for place, u_ref, v_ref in ((s_ref[0], a_ref, b_ref), (1 - s_ref[0], c_ref, d_ref)):
        total = u_ref[...].astype(F32) + v_ref[...].astype(F32)
        where = span(place, HEAD)
        gk_ref[:, where] = total[:HEAD, :].T
        gv_ref[:, where] = total[HEAD:, :].T


def kv_combine(core, parts):
    rows, width = parts[0].shape
    step = 1024
    out = jax.ShapeDtypeStruct((width, rows), F32)
    return pl.pallas_call(
        kv_combine_kernel,
        grid_spec=pltpu.PrefetchScalarGridSpec(
            num_scalar_prefetch=1,
            grid=(width // step,),
            in_specs=[pl.BlockSpec((rows, step), lambda n, s: (0, n))] * 4,
            out_specs=[pl.BlockSpec((step, rows), lambda n, s: (n, 0))] * 2,
        ),
        out_shape=[out, out],
        compiler_params=params(),
        cost_estimate=cost(16 * width * rows * 16, 16 * width * rows),
        name="kv_combine",
    )(core, *parts)


def combine_kernel(s_ref, a_ref, b_ref, c_ref, d_ref, *rest):
    gq_ref, go_ref = rest[-2:]

    def put(u_ref, v_ref):
        def part(c, carry):
            cols = span(c, 256)
            gq_ref[cols, :] = (u_ref[0, :, cols].astype(F32) + v_ref[0, :, cols].astype(F32)).T
            go_ref[:, cols] = u_ref[1, :, cols].astype(F32) + v_ref[1, :, cols].astype(F32)
            return carry

        lax.fori_loop(0, u_ref.shape[2] // 256, part, 0)

    @pl.when(pl.program_id(0) == 0)
    def _():
        put(a_ref, b_ref)

    @pl.when(pl.program_id(0) == 1)
    def _():
        put(c_ref, d_ref)


def combine(core, chunk, n_chunks, parts, prev):
    width = parts[0].shape[2]
    step = 1024
    last = width // step - 1
    near = pl.BlockSpec((2, WIDE, step), lambda w, r, s: (0, 0, r + w * (last - r)))
    far = pl.BlockSpec((2, WIDE, step), lambda w, r, s: (0, 0, r * w))

    def place(w, s):
        return (s[0] + w - 2 * s[0] * w) * n_chunks + chunk

    shape = jax.ShapeDtypeStruct((width, 2 * n_chunks * WIDE), F32)
    shape_o = jax.ShapeDtypeStruct((2 * n_chunks * WIDE, width), F32)
    extra = [] if prev is None else list(prev)
    return pl.pallas_call(
        combine_kernel,
        grid_spec=pltpu.PrefetchScalarGridSpec(
            num_scalar_prefetch=1,
            grid=(2, width // step),
            in_specs=[near, near, far, far] + [pl.BlockSpec(memory_space=pl.ANY)] * len(extra),
            out_specs=[
                pl.BlockSpec((step, WIDE), lambda w, r, s: (r, place(w, s))),
                pl.BlockSpec((WIDE, step), lambda w, r, s: (place(w, s), r)),
            ],
        ),
        out_shape=[shape, shape_o],
        input_output_aliases={} if prev is None else {5: 0, 6: 1},
        compiler_params=params(),
        cost_estimate=cost(16 * width * WIDE * 64, 32 * width * WIDE),
        name="combine",
    )(core, *parts, *extra)


def fill_heads(core, own_refs, oth_refs, lhs):
    n = len(own_refs)
    for j in range(n):
        lhs[:, pl.ds(pl.multiple_of((core * n + j) * WIDE, WIDE), WIDE)] = own_refs[j][0]
        lhs[:, pl.ds(pl.multiple_of(((1 - core) * n + j) * WIDE, WIDE), WIDE)] = oth_refs[j][0]


def attn_out_kernel(n, s_ref, *refs):
    own_refs, oth_refs = refs[:n], refs[n:2 * n]
    wo_ref, out_ref, lhs = refs[2 * n:]

    @pl.when(pl.program_id(0) == 0)
    def _():
        fill_heads(s_ref[0], own_refs, oth_refs, lhs)

    out_ref[...] = dot_nn(lhs[...], wo_ref[...]).astype(BF)


def attn_out(core, own, oth, w_o):
    n = len(own)
    tokens = own[0].shape[1] // 2
    heads, width = w_o.shape
    step = 512
    return pl.pallas_call(
        functools.partial(attn_out_kernel, n),
        grid_spec=pltpu.PrefetchScalarGridSpec(
            num_scalar_prefetch=1,
            grid=(width // step,),
            in_specs=[pl.BlockSpec((1, tokens, WIDE), lambda k, s: (0, s[0], 0))] * (2 * n)
            + [pl.BlockSpec((heads, step), lambda k, s: (0, k))],
            out_specs=pl.BlockSpec((tokens, step), lambda k, s: (0, k)),
            scratch_shapes=[pltpu.VMEM((tokens, heads), BF)],
        ),
        out_shape=jax.ShapeDtypeStruct((tokens, width), BF),
        compiler_params=params(),
        cost_estimate=cost(2 * tokens * heads * width, 2 * heads * width + 4 * tokens * width),
        name="attn_out",
    )(core, *own, *oth, w_o)


def hidden_kernel(n, s_ref, *refs):
    own_refs, oth_refs = refs[:n], refs[n:2 * n]
    kv_own, kv_oth, wq_ref, wk_ref, wv_ref, out_ref, lhs, klhs, vlhs = refs[2 * n:]
    core = s_ref[0]

    @pl.when(pl.program_id(0) == 0)
    def _():
        fill_heads(core, own_refs, oth_refs, lhs)
        for place, ref in ((core, kv_own), (1 - core, kv_oth)):
            where = pl.ds(pl.multiple_of(place * HEAD, HEAD), HEAD)
            klhs[:, where] = ref[:, :HEAD]
            vlhs[:, where] = ref[:, HEAD:]

    out_ref[...] = (
        dot_nt(lhs[...], wq_ref[...]) + dot_nt(klhs[...], wk_ref[...]) + dot_nt(vlhs[...], wv_ref[...])
    ).astype(BF)


def grad_hidden(core, own, oth, kv_own, kv_oth, w_q, w_k, w_v):
    n = len(own)
    tokens = own[0].shape[1] // 2
    width, heads = w_q.shape
    kv_cols = w_k.shape[1]
    step = 512
    return pl.pallas_call(
        functools.partial(hidden_kernel, n),
        grid_spec=pltpu.PrefetchScalarGridSpec(
            num_scalar_prefetch=1,
            grid=(width // step,),
            in_specs=[pl.BlockSpec((1, tokens, WIDE), lambda k, s: (1, s[0], 0))] * (2 * n)
            + [pl.BlockSpec((tokens, 2 * HEAD), lambda k, s: (s[0], 0))] * 2
            + [
                pl.BlockSpec((step, heads), lambda k, s: (k, 0)),
                pl.BlockSpec((step, kv_cols), lambda k, s: (k, 0)),
                pl.BlockSpec((step, kv_cols), lambda k, s: (k, 0)),
            ],
            out_specs=pl.BlockSpec((tokens, step), lambda k, s: (0, k)),
            scratch_shapes=[
                pltpu.VMEM((tokens, heads), BF),
                pltpu.VMEM((tokens, kv_cols), BF),
                pltpu.VMEM((tokens, kv_cols), BF),
            ],
        ),
        out_shape=jax.ShapeDtypeStruct((tokens, width), BF),
        compiler_params=params(),
        cost_estimate=cost(2 * tokens * (heads + 2 * kv_cols) * width, 2 * heads * width + 4 * tokens * width),
        name="grad_hidden",
    )(core, *own, *oth, kv_own, kv_oth, w_q, w_k, w_v)


def solution(mesh):
    n_dev = mesh.shape["sp"]
    n_chunks = 4
    near_perm = [(d, d ^ 1) for d in range(n_dev)]
    far_perm = [(d, d ^ 2) for d in range(n_dev)]
    down_perm = [(0, 2), (1, 3)]
    up_perm = [(2, 0), (3, 1)]

    def near(v):
        return lax.ppermute(v, "sp", near_perm)

    def far(v):
        return lax.ppermute(v, "sp", far_perm)

    def device_step(hidden, grad_out, positions, doc_ids, w_q, w_k, w_v, w_o):
        tokens = hidden.shape[0]
        chip_len = 2 * tokens
        assert n_chunks == w_q.shape[1] // (2 * WIDE)
        place = lax.axis_index("sp")
        core_id, chip_id = place & 1, place >> 1
        core = core_id.astype(jnp.int32)[None]

        doc_oth = near(doc_ids)
        doc_far = far(doc_ids)
        doc_far_oth = lax.ppermute(doc_ids, "sp", [(d, d ^ 3) for d in range(n_dev)])
        x_oth = near(hidden)
        g_oth = near(grad_out)
        tab_own = rope_table(positions)
        tab_oth = near(tab_own)
        kv_own, q = qkv_proj(True, core, hidden, w_q, w_k, w_v, tab_own, None)
        kvp_own = lax.ppermute(kv_own, "sp", down_perm)

        def in_order(own, oth):
            return jnp.where(core_id == 0, jnp.concatenate([own, oth]), jnp.concatenate([oth, own]))

        doc_chip, doc_far = in_order(doc_ids, doc_oth), in_order(doc_far, doc_far_oth)
        kv_oth, q = qkv_proj(False, core, x_oth, w_q, w_k, w_v, tab_oth, q)
        kvp_oth = lax.ppermute(kv_oth, "sp", down_perm)
        dctx = dctx_proj(core, grad_out, g_oth, w_o)

        heads_doc = doc_chip[::BQ]
        lo = jnp.sum(doc_chip[None, :] < heads_doc[:, None], axis=1, dtype=jnp.int32)
        lo_far = jnp.sum(doc_far[None, :] < heads_doc[:, None], axis=1, dtype=jnp.int32)
        lo = lo + jnp.where(chip_id == 0, chip_len, lo_far)
        lo = (lo >> (ALIGN.bit_length() - 1)) << (ALIGN.bit_length() - 1)
        end = chip_len + BQ * (1 + jnp.arange(chip_len // BQ, dtype=jnp.int32))
        n_blocks = (end - lo + BK - 1) >> (BK.bit_length() - 1)
        kdoc = jnp.concatenate([doc_far, doc_chip, jnp.zeros((BK,), jnp.int32)])[None, :]

        acts, acts_oth, dkv_sum, sums = [], [], None, None
        for j in range(n_chunks):
            act, part, dkv_up, dkv_here = attention(
                j, core, lo, n_blocks, q, dctx, kdoc, (tab_own, tab_oth), (kvp_own, kvp_oth), (kv_own, kv_oth),
                (hidden, x_oth), (grad_out, g_oth), dkv_sum,
            )
            part = part.reshape(2, WIDE, -1)
            acts.append(act)
            dkv_sum = (dkv_up, dkv_here)
            if j == n_chunks - 1:
                dkv_far = lax.ppermute(dkv_up, "sp", up_perm)
            acts_oth.append(near(act))
            part_far = far(part)
            part_near = near(part)
            part_far_near = near(part_far)
            sums = combine(core, j, n_chunks, (part, part_far, part_near, part_far_near), sums)
        grad_wq, grad_wo = sums

        dkv, dkvt = kv_finish(core, dkv_here, dkv_far, tab_own, tab_oth)
        dkv_oth = near(dkv)
        kv_part = kvgrad(core, dkvt, hidden, x_oth)
        kv_part_far = far(kv_part)
        kv_part_near = near(kv_part)
        kv_part_far_near = near(kv_part_far)
        grad_wk, grad_wv = kv_combine(core, (kv_part, kv_part_far, kv_part_near, kv_part_far_near))
        out = attn_out(core, acts, acts_oth, w_o)
        g_hidden = grad_hidden(core, acts, acts_oth, dkv, dkv_oth, w_q, w_k, w_v)
        return out, g_hidden, grad_wq, grad_wk, grad_wv, grad_wo

    tok_spec = P(("dp", "sp"), None)
    vec_spec = P(("dp", "sp"))
    rep_spec = P(None, None)
    part_spec = P("dp", None)


    return jax.shard_map(
        device_step,
        mesh=mesh,
        in_specs=(tok_spec, tok_spec, vec_spec, vec_spec, rep_spec, rep_spec, rep_spec, rep_spec),
        out_specs=(tok_spec, tok_spec, part_spec, part_spec, part_spec, part_spec),
        check_vma=False,
    )
```

```python
import functools

import jax
import jax.numpy as jnp
from jax import lax
from jax.experimental import pallas as pl
from jax.experimental.pallas import tpu as pltpu
from jax.sharding import PartitionSpec as P

HEAD = 128
ROPE_THETA = 500000.0
ROPE_FACTOR = 8.0
ROPE_LOW = 1.0
ROPE_HIGH = 4.0
ROPE_OLD_CTX = 8192.0
NEG_BIG = float("-inf")
SCALE = HEAD ** -0.5
LOG2E = 1.4426950408889634

PAIR = 2
WIDE = PAIR * HEAD
BQ = 512
BK = 512
MIX = 16
ALIGN = 128
BF = jnp.bfloat16
F32 = jnp.float32


def rope_freqs():
    half_idx = jnp.arange(HEAD // 2, dtype=F32)
    inv_freq = jnp.power(ROPE_THETA, -2.0 * half_idx / HEAD)
    wavelen = 2.0 * jnp.pi / inv_freq
    smooth = (ROPE_OLD_CTX / wavelen - ROPE_LOW) / (ROPE_HIGH - ROPE_LOW)
    mixed_freq = (1.0 - smooth) * inv_freq / ROPE_FACTOR + smooth * inv_freq
    scaled = jnp.where(wavelen > ROPE_OLD_CTX / ROPE_LOW, inv_freq / ROPE_FACTOR, mixed_freq)
    return jnp.where(wavelen < ROPE_OLD_CTX / ROPE_HIGH, inv_freq, scaled)


def rope_table(pos_vec):
    angles = pos_vec.astype(F32)[:, None] * rope_freqs()[None, :]
    return jnp.concatenate([jnp.cos(angles), jnp.sin(angles)], axis=-1)


def dot_nn(a, b):
    return lax.dot_general(a, b, (((1,), (0,)), ((), ())), preferred_element_type=F32)


def dot_nt(a, b):
    return lax.dot_general(a, b, (((1,), (1,)), ((), ())), preferred_element_type=F32)


def swap_halves(v):
    return pltpu.roll(v, HEAD // 2, 1)


def spread_table(tab):
    low = lax.broadcasted_iota(jnp.int32, tab.shape, 1) < HEAD // 2
    other = swap_halves(tab)
    return jnp.where(low, tab, other), jnp.where(low, -other, tab)


def cost(flops, nbytes, trans=0):
    return pl.CostEstimate(flops=int(flops), bytes_accessed=int(nbytes), transcendentals=int(trans))


def params(**kw):
    return pltpu.CompilerParams(vmem_limit_bytes=67_000_000, **kw)


def by_rows(rows, body, size=16):
    def step(r, carry):
        body(span(r, size))
        return carry

    lax.fori_loop(0, rows // size, step, 0)


def span(index, size):
    return pl.ds(pl.multiple_of(index * size, size), size)


def qkv_kernel(s_ref, x_ref, wq_ref, wk_ref, wv_ref, tab_ref, *rest):
    kv_ref, q_ref, w_s = rest[-3:]

    @pl.when(pl.program_id(0) == 0)
    def _():
        w_s[:, :HEAD] = wk_ref[...]
        w_s[:, HEAD:] = wv_ref[...]

    x = x_ref[...]
    cos_t, sin_t = spread_table(tab_ref[...])
    kv = dot_nn(x, w_s[...])
    k = kv[:, :HEAD]
    kv_ref[:, :HEAD] = (k * cos_t + swap_halves(k) * sin_t).astype(BF)
    kv_ref[:, HEAD:] = kv[:, HEAD:].astype(BF)
    step = 4 * HEAD
    for n in range(wq_ref.shape[1] // step):
        q = dot_nn(x, wq_ref[:, n * step:(n + 1) * step])
        for h in range(step // HEAD):
            part = q[:, h * HEAD:(h + 1) * HEAD]
            j, at = divmod(n * step + h * HEAD, WIDE)
            q_ref[j, :, at:at + HEAD] = (part * cos_t + swap_halves(part) * sin_t).astype(BF)


def qkv_proj(own, core, x, w_q, w_k, w_v, tab, prev):
    tokens, width = x.shape
    cols = w_q.shape[1] // 2
    rows = tokens // 2
    extra = [] if prev is None else [prev]
    return pl.pallas_call(
        qkv_kernel,
        grid_spec=pltpu.PrefetchScalarGridSpec(
            num_scalar_prefetch=1,
            grid=(2,),
            in_specs=[
                pl.BlockSpec((rows, width), lambda m, s: (m, 0)),
                pl.BlockSpec((width, cols), lambda m, s: (0, s[0])),
                pl.BlockSpec((width, HEAD), lambda m, s: (0, s[0])),
                pl.BlockSpec((width, HEAD), lambda m, s: (0, s[0])),
                pl.BlockSpec((rows, HEAD), lambda m, s: (m, 0)),
            ] + [pl.BlockSpec(memory_space=pl.ANY)] * len(extra),
            out_specs=[
                pl.BlockSpec((rows, 2 * HEAD), lambda m, s: (m, 0)),
                pl.BlockSpec((cols // WIDE, rows, WIDE), lambda m, s: (0, (s[0] if own else 1 - s[0]) * 2 + m, 0)),
            ],
            scratch_shapes=[pltpu.VMEM((width, 2 * HEAD), BF)],
        ),
        out_shape=[
            jax.ShapeDtypeStruct((tokens, 2 * HEAD), BF),
            jax.ShapeDtypeStruct((cols // WIDE, 2 * tokens, WIDE), BF),
        ],
        input_output_aliases={} if prev is None else {6: 1},
        compiler_params=params(),
        cost_estimate=cost(2 * tokens * width * (cols + 2 * HEAD), tokens * width * 2 + cols * width * 2),
        name="qkv_proj",
    )(core, x, w_q, w_k, w_v, tab, *extra)


def dctx_kernel(s_ref, own_ref, oth_ref, wo_ref, out_ref):
    def put(ref):
        step = 4 * HEAD
        for n in range(wo_ref.shape[0] // step):
            part = dot_nt(ref[...], wo_ref[n * step:(n + 1) * step, :]).astype(BF)
            for j in range(step // WIDE):
                out_ref[n * (step // WIDE) + j] = part[:, j * WIDE:(j + 1) * WIDE]

    @pl.when(pl.program_id(0) < 2)
    def _():
        put(own_ref)

    @pl.when(pl.program_id(0) >= 2)
    def _():
        put(oth_ref)


def dctx_proj(core, own, oth, w_o):
    tokens, width = own.shape
    cols = w_o.shape[0] // 2
    rows = tokens // 2

    def place(m, s):
        far = m // 2
        return (s[0] + far - 2 * s[0] * far) * 2 + m % 2

    return pl.pallas_call(
        dctx_kernel,
        grid_spec=pltpu.PrefetchScalarGridSpec(
            num_scalar_prefetch=1,
            grid=(4,),
            in_specs=[
                pl.BlockSpec((rows, width), lambda m, s: (jnp.minimum(m, 1), 0)),
                pl.BlockSpec((rows, width), lambda m, s: (jnp.maximum(m - 2, 0), 0)),
                pl.BlockSpec((cols, width), lambda m, s: (s[0], 0)),
            ],
            out_specs=pl.BlockSpec((cols // WIDE, rows, WIDE), lambda m, s: (0, place(m, s), 0)),
        ),
        out_shape=jax.ShapeDtypeStruct((cols // WIDE, 2 * tokens, WIDE), BF),
        compiler_params=params(),
        cost_estimate=cost(4 * tokens * width * cols, tokens * width * 4 + cols * width * 2),
        name="dctx_proj",
    )(core, own, oth, w_o)


def attn_kernel(
    first, core_ref, lo_ref, nb_ref, q_ref, do_ref, kdoc_ref, tab_own, tab_oth, kvp_own, kvp_oth, kvc_own, kvc_oth,
    x_own, x_oth, g_own, g_oth, before_up, before_here, act_ref, part_ref, up_ref, here_ref,
    kv_s, s_s, dp_s, m_s, l_s, d_s, qd_s, ahead_s, ctx_s, dq_s, q_s, do_s, qt_s, dot_s, tab_s, dk_s, dv_s,
    x_s, g_s, at_s, w_s, before_s, init_sem, row_sem, out_sem, part_sem,
):

    def before_copies():
        return (
            pltpu.make_async_copy(before_up, before_s.at[pl.ds(0, 2 * HEAD), :], out_sem.at[2]),
            pltpu.make_async_copy(before_here, before_s.at[pl.ds(2 * HEAD, 2 * HEAD), :], out_sem.at[3]),
        )

    i = pl.program_id(0)
    tokens = kvc_own.shape[0]
    chip_len = 2 * tokens
    core = core_ref[0]
    per_half = tokens // BQ
    rows_here = span(i % per_half, BQ)

    def row_copies(x, g):
        return (
            pltpu.make_async_copy(x.at[rows_here, :], x_s, row_sem.at[0]),
            pltpu.make_async_copy(g.at[rows_here, :], g_s, row_sem.at[1]),
        )

    def init_copies():
        moves = []
        for base, place, ref in ((0, core, kvp_own), (0, 1 - core, kvp_oth), (2, core, kvc_own), (2, 1 - core, kvc_oth)):
            moves.append((ref, kv_s.at[span(base + place, tokens), :]))
        moves.append((tab_own, tab_s.at[span(core, tokens), :]))
        moves.append((tab_oth, tab_s.at[span(1 - core, tokens), :]))
        return [pltpu.make_async_copy(src, dst, init_sem.at[n]) for n, (src, dst) in enumerate(moves)]

    def arrive(first, last):
        @pl.when(i == 0)
        def _():
            for copy in init_copies()[first:last]:
                copy.wait()

    @pl.when(i == 0)
    def _():
        for copy in init_copies():
            copy.start()
        if not first:
            for copy in before_copies():
                copy.start()
        kv_s[2 * chip_len:, :] = jnp.zeros((BK, 2 * HEAD), BF)

        def clear(r):
            w_s[r, :] = jnp.zeros((16, w_s.shape[1]), F32)

        def clear_kv(r):
            dk_s[r, :] = jnp.zeros((16, dk_s.shape[1]), F32)
            dv_s[r, :] = jnp.zeros((16, dv_s.shape[1]), F32)

        def order(r):
            row = lax.broadcasted_iota(jnp.int32, (16, BK), 0)
            ahead_s[r, :] = lax.broadcasted_iota(jnp.int32, (16, BK), 1) - row - r.start

        by_rows(BQ, order)
        by_rows(w_s.shape[0], clear)
        by_rows(HEAD, clear_kv)

    @pl.when(i // per_half == core)
    def _():
        for copy in row_copies(x_own, g_own):
            copy.start()

    @pl.when(i // per_half != core)
    def _():
        for copy in row_copies(x_oth, g_oth):
            copy.start()

    def mixed(ref):
        parts = [ref[0, :, h * HEAD:(h + 1) * HEAD].reshape(BQ // MIX, 1, MIX, HEAD) for h in range(PAIR)]
        return jnp.concatenate(parts, axis=1).reshape(PAIR * BQ, HEAD)

    def apart(v, h):
        return v.reshape(BQ // MIX, PAIR, MIX, HEAD)[:, h].reshape(BQ, HEAD)

    q_mix, do_mix = mixed(q_ref), mixed(do_ref)
    q_s[...] = q_mix
    do_s[...] = do_mix
    qt_s[...] = q_mix.T
    dot_s[...] = do_mix.T
    qdoc = kdoc_ref[:, pl.ds(pl.multiple_of(chip_len + i * BQ, BQ), BQ)]
    qd_s[...] = jnp.broadcast_to(qdoc, (HEAD, BQ)).T
    m_s[...] = jnp.full(m_s.shape, NEG_BIG, F32)
    lo = lo_ref[i]
    n_blocks = nb_ref[i]
    lanes = BK // HEAD

    def fold(v, op):
        out = v[:, :HEAD]
        for n in range(1, lanes):
            out = op(out, v[:, n * HEAD:(n + 1) * HEAD])
        return out

    def spread(v):
        return jnp.concatenate([v] * lanes, axis=1)

    def offset(b):
        return pl.multiple_of(lo + b * BK, ALIGN)

    def scores(b, carry):
        off = offset(b)
        s = dot_nt(q_s[...], kv_s[pl.ds(off, BK), :HEAD])
        limit = chip_len + i * BQ - off
        key_doc = kdoc_ref[:, pl.ds(off, BK)]
        for c in range(BQ // MIX):
            here = slice(c * MIX, (c + 1) * MIX)
            keep = (ahead_s[here, :] <= limit) & (key_doc == spread(qd_s[here, :]))
            shift = jnp.where(keep, 0.0, NEG_BIG)
            for h in range(PAIR):
                rows = slice((c * PAIR + h) * MIX, (c * PAIR + h + 1) * MIX)
                sh = s[rows, :] * (SCALE * LOG2E) + shift
                s_s[b, rows, :] = sh
                m_s[rows, :] = jnp.maximum(m_s[rows, :], fold(sh, jnp.maximum))
        return carry

    arrive(0, 4)
    lax.fori_loop(0, n_blocks, scores, 0)
    l_s[...] = jnp.zeros(l_s.shape, F32)
    d_s[...] = jnp.zeros(d_s.shape, F32)
    m_s[...] = jnp.broadcast_to(jnp.max(m_s[...], axis=1, keepdims=True), m_s.shape)

    def weights(b, carry):
        dp = dot_nt(do_s[...], kv_s[pl.ds(offset(b), BK), HEAD:])
        e = jnp.exp2(s_s[b] - spread(m_s[...]))
        s_s[b] = e
        dp_s[b] = dp
        l_s[...] += fold(e, jnp.add)
        d_s[...] += fold(e * dp, jnp.add)
        return carry

    arrive(4, 6)
    lax.fori_loop(0, n_blocks, weights, 0)
    ctx_s[...] = jnp.zeros(ctx_s.shape, F32)
    dq_s[...] = jnp.zeros(dq_s.shape, F32)
    inv = 1.0 / jnp.sum(l_s[...], axis=1, keepdims=True)
    delta = jnp.sum(d_s[...], axis=1, keepdims=True) * inv
    l_s[...] = jnp.broadcast_to(inv, l_s.shape)
    d_s[...] = jnp.broadcast_to(delta, d_s.shape)

    def grads(b, carry):
        off = offset(b)
        p = s_s[b] * spread(l_s[...])
        pb = p.astype(BF)
        ds = (p * (dp_s[b] - spread(d_s[...])) * SCALE).astype(BF)
        ctx_s[...] += dot_nn(pb, kv_s[pl.ds(off, BK), HEAD:])
        dq_s[...] += dot_nn(ds, kv_s[pl.ds(off, BK), :HEAD])
        dv_s[:, pl.ds(off, BK)] += dot_nn(dot_s[...], pb)
        dk_s[:, pl.ds(off, BK)] += dot_nn(qt_s[...], ds)
        return carry

    lax.fori_loop(0, n_blocks, grads, 0)
    last = pl.num_programs(0) - 1

    def out_copies():
        return (
            pltpu.make_async_copy(before_s.at[pl.ds(0, 2 * HEAD), :], up_ref, out_sem.at[0]),
            pltpu.make_async_copy(before_s.at[pl.ds(2 * HEAD, 2 * HEAD), :], here_ref, out_sem.at[1]),
        )

    @pl.when(i == last)
    def _():
        if not first:
            for copy in before_copies():
                copy.wait()

        def narrow_kv(r, carry):
            rows = span(r, 16)
            for n, acc in enumerate((dk_s, dv_s)):
                for side in range(2):
                    at = pl.ds(pl.multiple_of((n + 2 * side) * HEAD + r * 16, 16), 16)
                    total = acc[rows, side * chip_len:(side + 1) * chip_len]
                    if not first:
                        total = total + before_s[at, :].astype(F32)
                    before_s[at, :] = total.astype(BF)
            return carry

        lax.fori_loop(0, HEAD // 16, narrow_kv, 0)
        for copy in out_copies():
            copy.start()

    cos_t, sin_t = spread_table(tab_s[span(i, BQ), :])
    ctx_all, dq_all = ctx_s[...].astype(BF), dq_s[...].astype(BF).astype(F32)
    for h in range(PAIR):
        cols = slice(h * HEAD, (h + 1) * HEAD)
        ctx = apart(ctx_all, h)
        act_ref[0, :, cols] = ctx
        at_s[WIDE + h * HEAD:WIDE + (h + 1) * HEAD, :] = ctx.T
        dq = apart(dq_all, h)
        dq = (dq * cos_t - swap_halves(dq) * sin_t).astype(BF)
        act_ref[1, :, cols] = dq
        at_s[h * HEAD:(h + 1) * HEAD, :] = dq.T
    step = 4 * HEAD
    for copy in row_copies(x_own, g_own):
        copy.wait()

    def product(c):
        cols = span(c, step)
        for lhs, rows_ref in ((slice(0, WIDE), x_s), (slice(WIDE, 2 * WIDE), g_s)):
            w_s[lhs, cols] += dot_nn(at_s[lhs, :], rows_ref[:, cols])
        return cols

    def products(c, carry):
        product(c)
        return carry

    def part_copy(c):
        cols = span(c, step)
        return pltpu.make_async_copy(x_s.at[:, cols], part_ref.at[:, cols], part_sem.at[c])

    def last_products(c, carry):
        cols = product(c)
        x_s[:, cols] = w_s[:, cols].astype(BF)
        part_copy(c).start()
        return carry

    n_products = x_s.shape[1] // step

    @pl.when(i < last)
    def _():
        lax.fori_loop(0, n_products, products, 0)

    @pl.when(i == last)
    def _():
        lax.fori_loop(0, n_products, last_products, 0)
        for c in range(n_products):
            part_copy(c).wait()
        for copy in out_copies():
            copy.wait()


def attention(chunk, core, lo, n_blocks, q, dctx, kdoc, tabs, kv_prev, kv_chip, xs, gs, before):
    first = before is None
    chip_len = q.shape[1]
    width = xs[0].shape[1]
    assert 2 * WIDE == BQ == 4 * HEAD and width == chip_len
    padded = 2 * chip_len + BK
    max_blocks = 2 * chip_len // BK
    rows = PAIR * BQ
    full = lambda shape: pl.BlockSpec(shape, lambda i, *s: (0,) * len(shape))
    pairs = chip_len * chip_len * PAIR
    return pl.pallas_call(
        functools.partial(attn_kernel, first),
        grid_spec=pltpu.PrefetchScalarGridSpec(
            num_scalar_prefetch=3,
            grid=(chip_len // BQ,),
            in_specs=[
                pl.BlockSpec((1, BQ, WIDE), lambda i, *s: (chunk, i, 0)),
                pl.BlockSpec((1, BQ, WIDE), lambda i, *s: (chunk, i, 0)),
                full((1, padded)),
            ] + [pl.BlockSpec(memory_space=pl.ANY)] * 12,
            out_specs=[
                pl.BlockSpec((2, BQ, WIDE), lambda i, *s: (0, i, 0)),
                pl.BlockSpec(memory_space=pl.ANY),
                pl.BlockSpec(memory_space=pl.ANY),
                pl.BlockSpec(memory_space=pl.ANY),
            ],
            scratch_shapes=[
                pltpu.VMEM((padded, 2 * HEAD), BF),
                pltpu.VMEM((max_blocks, rows, BK), F32),
                pltpu.VMEM((max_blocks, rows, BK), F32),
                pltpu.VMEM((rows, HEAD), F32),
                pltpu.VMEM((rows, HEAD), F32),
                pltpu.VMEM((rows, HEAD), F32),
                pltpu.VMEM((BQ, HEAD), jnp.int32),
                pltpu.VMEM((BQ, BK), jnp.int32),
                pltpu.VMEM((rows, HEAD), F32),
                pltpu.VMEM((rows, HEAD), F32),
                pltpu.VMEM((rows, HEAD), BF),
                pltpu.VMEM((rows, HEAD), BF),
                pltpu.VMEM((HEAD, rows), BF),
                pltpu.VMEM((HEAD, rows), BF),
                pltpu.VMEM((chip_len, HEAD), F32),
                pltpu.VMEM((HEAD, padded), F32),
                pltpu.VMEM((HEAD, padded), F32),
                pltpu.VMEM((BQ, width), BF),
                pltpu.VMEM((BQ, width), BF),
                pltpu.VMEM((2 * WIDE, BQ), BF),
                pltpu.VMEM((2 * WIDE, width), F32),
                pltpu.VMEM((4 * HEAD, chip_len), BF),
                pltpu.SemaphoreType.DMA((6,)),
                pltpu.SemaphoreType.DMA((2,)),
                pltpu.SemaphoreType.DMA((4,)),
                pltpu.SemaphoreType.DMA((width // (4 * HEAD),)),
            ],
        ),
        out_shape=[
            jax.ShapeDtypeStruct((2, chip_len, WIDE), BF),
            jax.ShapeDtypeStruct((2 * WIDE, width), BF),
            jax.ShapeDtypeStruct((2 * HEAD, chip_len), BF),
            jax.ShapeDtypeStruct((2 * HEAD, chip_len), BF),
        ],
        compiler_params=params(),
        cost_estimate=cost(pairs * HEAD * 2 * 8, 12 * 1024 * 1024, pairs),
        name="attention",
    )(core, lo, n_blocks, q, dctx, kdoc, *tabs, *kv_prev, *kv_chip, *xs, *gs, *(gs if first else before))


def kv_finish_kernel(s_ref, near_ref, far_ref, tab_own, tab_oth, out_ref, outt_ref, tab_s):
    tokens = tab_own.shape[0]
    step = out_ref.shape[0]

    @pl.when(pl.program_id(0) == 0)
    def _():
        tab_s[span(s_ref[0], tokens), :] = tab_own[...]
        tab_s[span(1 - s_ref[0], tokens), :] = tab_oth[...]

    total = near_ref[...].astype(F32) + far_ref[...].astype(F32)
    cos_t, sin_t = spread_table(tab_s[span(pl.program_id(0), step), :])
    dk = total[:HEAD].astype(BF).astype(F32).T
    dk = (dk * cos_t - swap_halves(dk) * sin_t).astype(BF)
    dvt = total[HEAD:].astype(BF)
    out_ref[:, :HEAD] = dk
    out_ref[:, HEAD:] = dvt.T
    outt_ref[:HEAD, :] = dk.T
    outt_ref[HEAD:, :] = dvt


def kv_finish(core, near, far, tab_own, tab_oth):
    tokens = tab_own.shape[0]
    chip_len = 2 * tokens
    step = 512
    return pl.pallas_call(
        kv_finish_kernel,
        grid_spec=pltpu.PrefetchScalarGridSpec(
            num_scalar_prefetch=1,
            grid=(chip_len // step,),
            in_specs=[
                pl.BlockSpec((2 * HEAD, step), lambda t, s: (0, t)),
                pl.BlockSpec((2 * HEAD, step), lambda t, s: (0, t)),
                pl.BlockSpec((tokens, HEAD), lambda t, s: (0, 0)),
                pl.BlockSpec((tokens, HEAD), lambda t, s: (0, 0)),
            ],
            out_specs=[
                pl.BlockSpec((step, 2 * HEAD), lambda t, s: (t, 0)),
                pl.BlockSpec((2 * HEAD, step), lambda t, s: (0, t)),
            ],
            scratch_shapes=[pltpu.VMEM((chip_len, HEAD), F32)],
        ),
        out_shape=[
            jax.ShapeDtypeStruct((chip_len, 2 * HEAD), BF),
            jax.ShapeDtypeStruct((2 * HEAD, chip_len), BF),
        ],
        compiler_params=params(),
        cost_estimate=cost(chip_len * HEAD * 64, chip_len * HEAD * 16),
        name="kv_finish",
    )(core, near, far, tab_own, tab_oth)


def kvgrad_kernel(s_ref, dkvt_ref, x_own, x_oth, out_ref):
    tokens = x_own.shape[0]
    own, oth = span(s_ref[0], tokens), span(1 - s_ref[0], tokens)
    out_ref[...] = (dot_nn(dkvt_ref[:, own], x_own[...]) + dot_nn(dkvt_ref[:, oth], x_oth[...])).astype(BF)


def kvgrad(core, dkvt, x_own, x_oth):
    tokens, width = x_own.shape
    step = 512
    piece = pl.BlockSpec((tokens, step), lambda n, s: (0, n))
    return pl.pallas_call(
        kvgrad_kernel,
        grid_spec=pltpu.PrefetchScalarGridSpec(
            num_scalar_prefetch=1,
            grid=(width // step,),
            in_specs=[pl.BlockSpec((2 * HEAD, 2 * tokens), lambda n, s: (0, 0)), piece, piece],
            out_specs=pl.BlockSpec((2 * HEAD, step), lambda n, s: (0, n)),
        ),
        out_shape=jax.ShapeDtypeStruct((2 * HEAD, width), BF),
        compiler_params=params(),
        cost_estimate=cost(4 * tokens * width * 2 * HEAD, 4 * tokens * width),
        name="kvgrad",
    )(core, dkvt, x_own, x_oth)


def kv_combine_kernel(s_ref, a_ref, b_ref, *rest):
    gk_ref, gv_ref = rest[-2:]
    total = a_ref[...].astype(F32) + b_ref[...].astype(F32)
    gk_ref[...] = total[:HEAD, :].T
    gv_ref[...] = total[HEAD:, :].T


def kv_combine(own, core, parts, prev):
    rows, width = parts[0].shape
    step = 1024
    out = jax.ShapeDtypeStruct((width, rows), F32)
    extra = [] if prev is None else list(prev)
    return pl.pallas_call(
        kv_combine_kernel,
        grid_spec=pltpu.PrefetchScalarGridSpec(
            num_scalar_prefetch=1,
            grid=(width // step,),
            in_specs=[pl.BlockSpec((rows, step), lambda n, s: (0, n))] * 2
            + [pl.BlockSpec(memory_space=pl.ANY)] * len(extra),
            out_specs=[pl.BlockSpec((step, HEAD), lambda n, s: (n, s[0] if own else 1 - s[0]))] * 2,
        ),
        out_shape=[out, out],
        input_output_aliases={} if prev is None else {3: 0, 4: 1},
        compiler_params=params(),
        cost_estimate=cost(8 * width * rows * 16, 8 * width * rows),
        name="kv_combine",
    )(core, *parts, *extra)


def combine_kernel(s_ref, a_ref, b_ref, c_ref, d_ref, *rest):
    gq_ref, go_ref = rest[-2:]

    def put(u_ref, v_ref):
        def part(c, carry):
            cols = span(c, 256)
            gq_ref[cols, :] = (u_ref[0, :, cols].astype(F32) + v_ref[0, :, cols].astype(F32)).T
            go_ref[:, cols] = u_ref[1, :, cols].astype(F32) + v_ref[1, :, cols].astype(F32)
            return carry

        lax.fori_loop(0, u_ref.shape[2] // 256, part, 0)

    @pl.when(pl.program_id(0) == 0)
    def _():
        put(a_ref, b_ref)

    @pl.when(pl.program_id(0) == 1)
    def _():
        put(c_ref, d_ref)


def combine(core, chunk, n_chunks, parts, prev):
    width = parts[0].shape[2]
    step = 1024
    last = width // step - 1
    near = pl.BlockSpec((2, WIDE, step), lambda w, r, s: (0, 0, r + w * (last - r)))
    far = pl.BlockSpec((2, WIDE, step), lambda w, r, s: (0, 0, r * w))

    def place(w, s):
        return (s[0] + w - 2 * s[0] * w) * n_chunks + chunk

    shape = jax.ShapeDtypeStruct((width, 2 * n_chunks * WIDE), F32)
    shape_o = jax.ShapeDtypeStruct((2 * n_chunks * WIDE, width), F32)
    extra = [] if prev is None else list(prev)
    return pl.pallas_call(
        combine_kernel,
        grid_spec=pltpu.PrefetchScalarGridSpec(
            num_scalar_prefetch=1,
            grid=(2, width // step),
            in_specs=[near, near, far, far] + [pl.BlockSpec(memory_space=pl.ANY)] * len(extra),
            out_specs=[
                pl.BlockSpec((step, WIDE), lambda w, r, s: (r, place(w, s))),
                pl.BlockSpec((WIDE, step), lambda w, r, s: (place(w, s), r)),
            ],
        ),
        out_shape=[shape, shape_o],
        input_output_aliases={} if prev is None else {5: 0, 6: 1},
        compiler_params=params(),
        cost_estimate=cost(16 * width * WIDE * 64, 32 * width * WIDE),
        name="combine",
    )(core, *parts, *extra)


def fill_heads(core, own_refs, oth_refs, lhs):
    n = len(own_refs)
    for j in range(n):
        lhs[:, pl.ds(pl.multiple_of((core * n + j) * WIDE, WIDE), WIDE)] = own_refs[j][0]
        lhs[:, pl.ds(pl.multiple_of(((1 - core) * n + j) * WIDE, WIDE), WIDE)] = oth_refs[j][0]


def attn_out_kernel(n, s_ref, *refs):
    own_refs, oth_refs = refs[:n], refs[n:2 * n]
    wo_ref, out_ref, lhs = refs[2 * n:]

    @pl.when(pl.program_id(0) == 0)
    def _():
        fill_heads(s_ref[0], own_refs, oth_refs, lhs)

    out_ref[...] = dot_nn(lhs[...], wo_ref[...]).astype(BF)


def attn_out(core, own, oth, w_o):
    n = len(own)
    tokens = own[0].shape[1] // 2
    heads, width = w_o.shape
    step = 512
    return pl.pallas_call(
        functools.partial(attn_out_kernel, n),
        grid_spec=pltpu.PrefetchScalarGridSpec(
            num_scalar_prefetch=1,
            grid=(width // step,),
            in_specs=[pl.BlockSpec((1, tokens, WIDE), lambda k, s: (0, s[0], 0))] * (2 * n)
            + [pl.BlockSpec((heads, step), lambda k, s: (0, k))],
            out_specs=pl.BlockSpec((tokens, step), lambda k, s: (0, k)),
            scratch_shapes=[pltpu.VMEM((tokens, heads), BF)],
        ),
        out_shape=jax.ShapeDtypeStruct((tokens, width), BF),
        compiler_params=params(),
        cost_estimate=cost(2 * tokens * heads * width, 2 * heads * width + 4 * tokens * width),
        name="attn_out",
    )(core, *own, *oth, w_o)


def hidden_kernel(n, s_ref, *refs):
    own_refs, oth_refs = refs[:n], refs[n:2 * n]
    kv_own, kv_oth, wq_ref, wk_ref, wv_ref, out_ref, lhs, klhs, vlhs = refs[2 * n:]
    core = s_ref[0]

    @pl.when(pl.program_id(0) == 0)
    def _():
        fill_heads(core, own_refs, oth_refs, lhs)
        for place, ref in ((core, kv_own), (1 - core, kv_oth)):
            where = pl.ds(pl.multiple_of(place * HEAD, HEAD), HEAD)
            klhs[:, where] = ref[:, :HEAD]
            vlhs[:, where] = ref[:, HEAD:]

    out_ref[...] = (
        dot_nt(lhs[...], wq_ref[...]) + dot_nt(klhs[...], wk_ref[...]) + dot_nt(vlhs[...], wv_ref[...])
    ).astype(BF)


def grad_hidden(core, own, oth, kv_own, kv_oth, w_q, w_k, w_v):
    n = len(own)
    tokens = own[0].shape[1] // 2
    width, heads = w_q.shape
    kv_cols = w_k.shape[1]
    step = 512
    return pl.pallas_call(
        functools.partial(hidden_kernel, n),
        grid_spec=pltpu.PrefetchScalarGridSpec(
            num_scalar_prefetch=1,
            grid=(width // step,),
            in_specs=[pl.BlockSpec((1, tokens, WIDE), lambda k, s: (1, s[0], 0))] * (2 * n)
            + [pl.BlockSpec((tokens, 2 * HEAD), lambda k, s: (s[0], 0))] * 2
            + [
                pl.BlockSpec((step, heads), lambda k, s: (k, 0)),
                pl.BlockSpec((step, kv_cols), lambda k, s: (k, 0)),
                pl.BlockSpec((step, kv_cols), lambda k, s: (k, 0)),
            ],
            out_specs=pl.BlockSpec((tokens, step), lambda k, s: (0, k)),
            scratch_shapes=[
                pltpu.VMEM((tokens, heads), BF),
                pltpu.VMEM((tokens, kv_cols), BF),
                pltpu.VMEM((tokens, kv_cols), BF),
            ],
        ),
        out_shape=jax.ShapeDtypeStruct((tokens, width), BF),
        compiler_params=params(),
        cost_estimate=cost(2 * tokens * (heads + 2 * kv_cols) * width, 2 * heads * width + 4 * tokens * width),
        name="grad_hidden",
    )(core, *own, *oth, kv_own, kv_oth, w_q, w_k, w_v)


def solution(mesh):
    n_dev = mesh.shape["sp"]
    n_chunks = 4
    near_perm = [(d, d ^ 1) for d in range(n_dev)]
    far_perm = [(d, d ^ 2) for d in range(n_dev)]
    down_perm = [(0, 2), (1, 3)]
    up_perm = [(2, 0), (3, 1)]

    def near(v):
        return lax.ppermute(v, "sp", near_perm)

    def far(v):
        return lax.ppermute(v, "sp", far_perm)

    def device_step(hidden, grad_out, positions, doc_ids, w_q, w_k, w_v, w_o):
        tokens = hidden.shape[0]
        chip_len = 2 * tokens
        assert n_chunks == w_q.shape[1] // (2 * WIDE)
        place = lax.axis_index("sp")
        core_id, chip_id = place & 1, place >> 1
        core = core_id.astype(jnp.int32)[None]

        doc_oth = near(doc_ids)
        doc_far = far(doc_ids)
        doc_far_oth = lax.ppermute(doc_ids, "sp", [(d, d ^ 3) for d in range(n_dev)])
        x_oth = near(hidden)
        g_oth = near(grad_out)
        tab_own = rope_table(positions)
        tab_oth = near(tab_own)
        kv_own, q = qkv_proj(True, core, hidden, w_q, w_k, w_v, tab_own, None)
        kvp_own = lax.ppermute(kv_own, "sp", down_perm)

        def in_order(own, oth):
            return jnp.where(core_id == 0, jnp.concatenate([own, oth]), jnp.concatenate([oth, own]))

        doc_chip, doc_far = in_order(doc_ids, doc_oth), in_order(doc_far, doc_far_oth)
        kv_oth, q = qkv_proj(False, core, x_oth, w_q, w_k, w_v, tab_oth, q)
        kvp_oth = lax.ppermute(kv_oth, "sp", down_perm)
        dctx = dctx_proj(core, grad_out, g_oth, w_o)

        heads_doc = doc_chip[::BQ]
        lo = jnp.sum(doc_chip[None, :] < heads_doc[:, None], axis=1, dtype=jnp.int32)
        lo_far = jnp.sum(doc_far[None, :] < heads_doc[:, None], axis=1, dtype=jnp.int32)
        lo = lo + jnp.where(chip_id == 0, chip_len, lo_far)
        lo = (lo >> (ALIGN.bit_length() - 1)) << (ALIGN.bit_length() - 1)
        end = chip_len + BQ * (1 + jnp.arange(chip_len // BQ, dtype=jnp.int32))
        n_blocks = (end - lo + BK - 1) >> (BK.bit_length() - 1)
        kdoc = jnp.concatenate([doc_far, doc_chip, jnp.zeros((BK,), jnp.int32)])[None, :]

        acts, acts_oth, dkv_sum, sums = [], [], None, None
        for j in range(n_chunks):
            act, part, dkv_up, dkv_here = attention(
                j, core, lo, n_blocks, q, dctx, kdoc, (tab_own, tab_oth), (kvp_own, kvp_oth), (kv_own, kv_oth),
                (hidden, x_oth), (grad_out, g_oth), dkv_sum,
            )
            part = part.reshape(2, WIDE, -1)
            acts.append(act)
            dkv_sum = (dkv_up, dkv_here)
            if j == n_chunks - 1:
                dkv_far = lax.ppermute(dkv_up, "sp", up_perm)
            acts_oth.append(near(act))
            part_far = far(part)
            part_near = near(part)
            part_far_near = near(part_far)
            sums = combine(core, j, n_chunks, (part, part_far, part_near, part_far_near), sums)
        grad_wq, grad_wo = sums

        dkv, dkvt = kv_finish(core, dkv_here, dkv_far, tab_own, tab_oth)
        dkv_oth = near(dkv)
        kv_part = kvgrad(core, dkvt, hidden, x_oth)
        kv_part_far = far(kv_part)
        kv_part_near = near(kv_part)
        kv_part_far_near = near(kv_part_far)
        kv_sums = kv_combine(True, core, (kv_part, kv_part_far), None)
        grad_wk, grad_wv = kv_combine(False, core, (kv_part_near, kv_part_far_near), kv_sums)
        out = attn_out(core, acts, acts_oth, w_o)
        g_hidden = grad_hidden(core, acts, acts_oth, dkv, dkv_oth, w_q, w_k, w_v)
        return out, g_hidden, grad_wq, grad_wk, grad_wv, grad_wo

    tok_spec = P(("dp", "sp"), None)
    vec_spec = P(("dp", "sp"))
    rep_spec = P(None, None)
    part_spec = P("dp", None)


    return jax.shard_map(
        device_step,
        mesh=mesh,
        in_specs=(tok_spec, tok_spec, vec_spec, vec_spec, rep_spec, rep_spec, rep_spec, rep_spec),
        out_specs=(tok_spec, tok_spec, part_spec, part_spec, part_spec, part_spec),
        check_vma=False,
    )
```
